32 devices in a mesh: ty: 4 (over y, x), tx: 8 (over z, core).
Axes of the slice: x: 2, y: 2, z: 4, core: 2. Of those that a mesh axis runs over, the one named last changes fastest.
Arguments:
- sky: bfloat16 [2048, 4096], P('ty', 'tx'), may hold values from -6 to 6
- point_count: int32 [4, 8], P('ty', 'tx'), may hold values from 0 to 4, as said below
- point_offset: int32 [4, 8, 4, 2], P('ty', 'tx'), may hold values from 0 to 511
- beam_width: bfloat16 [4, 8, 4], P('ty', 'tx'), may hold values from 128 to 340
- uv_bins: int32 [4, 8, 4, 2, 2], P('ty', 'tx'), may hold values from 0 to 7
- uv_count: int32 [4, 8, 4], P('ty', 'tx'), may hold values from 1 to 2
- uv_weight: bfloat16 [4, 8, 4, 2, 128, 128], P('ty', 'tx'), may hold values from 1 to 8
Outputs:
- curvature: float32 [2048, 4096], P('ty', 'tx')
The draws below stay inside these ranges and needn't reach their ends.
Inputs may be any that keep to these rules, and one draw needn't show every extreme that they name: `point_count`: each tile holds at most 4 pointings, and the tiles of columns 2i and 2i + 1 of one row hold at most 4 together; in every draw some such pair holds exactly 4, all on one of its tiles. `point_offset`: entries of slots at or beyond a tile's count are ignored. `uv_bins`: entries of uv slots at or beyond a pointing's uv_count are ignored.
All inputs are finite; a program needn't handle non-finite values.
Results may differ from the reference program's by a relative error of at most 0.0085.
Values may be sent and summed in bfloat16 or wider, within the bound.
A program may use at most 128 MiB of HBM per device.

```python
import math
import jax
import jax.numpy as jnp
from jax import lax

TILE = 512
UVB = 128
UVSLOT = 2
SLOTS = 4
UVBLK = 8
GRID_Y = 4
GRID_X = 8
SKY_Y = 2048
SKY_X = 4096


def draw_point_count(key, part):
    key_total, key_first, key_where, key_side = jax.random.split(jax.random.fold_in(key, 11), 4)
    pairs = GRID_X // 2
    totals = jax.random.randint(key_total, (GRID_Y, pairs), 2, SLOTS + 1)
    first = jax.random.randint(key_first, (GRID_Y, pairs), 0, totals + 1)
    chosen = jax.random.randint(key_where, (), 0, GRID_Y * pairs)
    side = jax.random.randint(key_side, (), 0, 2)
    flat = jnp.arange(GRID_Y * pairs, dtype=jnp.int32).reshape(GRID_Y, pairs)
    hit = flat == chosen
    totals = jnp.where(hit, SLOTS, totals)
    first = jnp.where(hit, side * SLOTS, first)
    second = totals - first
    return jnp.stack([first, second], axis=-1).reshape(GRID_Y, GRID_X).astype(jnp.int32)


def set_ends(entries, stream_key, smallest, high):
    extent = entries.shape
    spot = [jax.random.randint(jax.random.fold_in(stream_key, axis), (), 0, extent[axis]) for axis in range(len(extent))]
    entries = entries.at[tuple(spot)].set(smallest)
    longest = extent.index(max(extent))
    spot[longest] = (spot[longest] + 1) % extent[longest]
    return entries.at[tuple(spot)].set(high)


def level_of(rng, shape, shards, low, largest):
    level, own = 1.0, jax.random.fold_in(rng, 6)
    for dim, shards_of in shards:
        heights = jnp.exp(jax.random.uniform(jax.random.fold_in(own, dim), (shards_of,), jnp.float32, low / len(shards), largest / len(shards)))
        level = level * jnp.repeat(heights, shape[dim] // shards_of).reshape([-1 if axis == dim else 1 for axis in range(len(shape))])
    return level


def normal_values(rng, extent, scale, limit, cuts=(), kind=jnp.bfloat16):
    values = jax.random.normal(rng, extent, jnp.float32) * scale
    if len(cuts) > 0:
        values = level_of(rng, extent, cuts, -0.22, 0.18) * values
    return jnp.clip(values, min=-limit, max=limit).astype(kind)


def setup_inputs(seed: int = 0) -> dict:
    keys = jax.random.split(jax.random.key(seed), 8)
    sky = normal_values(keys[0], (SKY_Y, SKY_X), 1.0, 6.0, ((0, 4), (1, 8)))
    point_count = draw_point_count(jax.random.fold_in(keys[7], 71), 0)
    point_offset = set_ends(jax.random.randint(keys[2], (GRID_Y, GRID_X, SLOTS, 2), 0, TILE), jax.random.fold_in(keys[2], 1), 0, TILE - 1).astype(jnp.int32)
    beam_width = jnp.clip(jnp.exp(math.log(340.0) - 0.97691535 * jax.random.uniform(keys[3], (GRID_Y, GRID_X, SLOTS), jnp.float32) ** level_of(keys[3], (GRID_Y, GRID_X, SLOTS), ((0, 4), (1, 8)), -0.2, 0.2)), 128.0, 340.0).astype(jnp.bfloat16)
    uv_bins = set_ends(jax.random.randint(keys[4], (GRID_Y, GRID_X, SLOTS, UVSLOT, 2), 0, UVBLK), jax.random.fold_in(keys[4], 1), 0, UVBLK - 1).astype(jnp.int32)
    uv_count = set_ends(jax.random.randint(keys[5], (GRID_Y, GRID_X, SLOTS), 1, UVSLOT + 1), jax.random.fold_in(keys[5], 1), 1, UVSLOT).astype(jnp.int32)
    uv_weight = jnp.clip(jnp.exp(math.log(8.0) - 2.0794415 * jax.random.uniform(keys[6], (GRID_Y, GRID_X, SLOTS, UVSLOT, UVB, UVB), jnp.float32) ** level_of(keys[6], (GRID_Y, GRID_X, SLOTS, UVSLOT, UVB, UVB), ((0, 4), (1, 8)), -0.2, 0.2)), 1.0, 8.0).astype(jnp.bfloat16)
    return {"sky": sky, "point_count": point_count, "point_offset": point_offset, "beam_width": beam_width, "uv_bins": uv_bins, "uv_count": uv_count, "uv_weight": uv_weight}


def dft_tables(blocks, block_size, length):
    rows = blocks[:, None] * block_size + jnp.arange(block_size, dtype=jnp.int32)[None, :]
    pixels = jnp.arange(length, dtype=jnp.int32)
    phase = rows[:, :, None] * pixels[None, None, :] % length
    angle = phase.astype(jnp.float32) * (2.0 * math.pi / length)
    factor = 1.0 / math.sqrt(length)
    return ((jnp.cos(angle) * factor).astype(jnp.bfloat16), (jnp.sin(angle) * factor).astype(jnp.bfloat16))

def beam_map(width, length):
    offset = jnp.arange(length, dtype=jnp.float32) - length // 2
    square = offset * offset
    radius = square[:, None] + square[None, :]
    spread = width.astype(jnp.float32)
    return jnp.exp(-radius / (2.0 * spread * spread))

def pointing_image(beamed, width, uv_pair, used, weight_tiles):
    slots_uv = weight_tiles.shape[0]
    block_size = weight_tiles.shape[1]
    length = beamed.shape[0]
    row_cos, row_sin = dft_tables(uv_pair[:, 0], block_size, length)
    col_cos, col_sin = dft_tables(uv_pair[:, 1], block_size, length)
    row_tables = jnp.stack([row_cos, row_sin], axis=1).reshape(slots_uv * 2 * block_size, length)
    col_tables = jnp.stack([jnp.concatenate([col_cos, col_sin], axis=1), jnp.concatenate([-col_sin, col_cos], axis=1)], axis=1)
    first = jnp.dot(row_tables, beamed, preferred_element_type=jnp.float32).astype(jnp.bfloat16)
    first = first.reshape(slots_uv, 2, block_size, length)
    visible = jnp.einsum('kcin,kcbn->kib', first.astype(jnp.float32), col_tables.astype(jnp.float32))
    used_mask = (jnp.arange(slots_uv, dtype=jnp.int32) < used).astype(jnp.float32)
    weighted = weight_tiles.astype(jnp.float32) * used_mask[:, None, None]
    scaled = (visible * jnp.concatenate([weighted, weighted], axis=2)).astype(jnp.bfloat16)
    spread = jnp.einsum('kib,kcbn->kcin', scaled.astype(jnp.float32), col_tables.astype(jnp.float32))
    spread = spread.astype(jnp.bfloat16).reshape(slots_uv * 2 * block_size, length)
    back = lax.dot_general(row_tables, spread, (((0,), (0,)), ((), ())), preferred_element_type=jnp.float32)
    return (beam_map(width, length) * back).astype(jnp.bfloat16)

def reference(sky, point_count, point_offset, beam_width, uv_bins, uv_count, uv_weight):
    grid_rows, grid_cols = point_count.shape
    slots = point_offset.shape[2]
    tile_size = TILE
    patch_size = 2 * TILE
    padded = jnp.pad(sky, tile_size)
    pairs = grid_cols // 2
    shape = (grid_rows, pairs, slots)
    row_ids = jnp.broadcast_to(jnp.arange(grid_rows, dtype=jnp.int32)[:, None, None], shape)
    pair_ids = jnp.broadcast_to(jnp.arange(pairs, dtype=jnp.int32)[None, :, None], shape)
    combined = jnp.broadcast_to(jnp.arange(slots, dtype=jnp.int32)[None, None, :], shape)
    even_count = point_count[:, 0::2][:, :, None]
    odd_count = point_count[:, 1::2][:, :, None]
    from_odd = (combined >= even_count).astype(jnp.int32)
    columns = 2 * pair_ids + from_odd
    slot_ids = jnp.clip(combined - from_odd * even_count, 0, slots - 1)
    live_ids = combined < even_count + odd_count

    def place(total, item):
        row, col, slot, live = item
        offset = point_offset[row, col, slot]
        top = (row * tile_size + offset[0]).astype(jnp.int32)
        left = (col * tile_size + offset[1]).astype(jnp.int32)
        window = lax.dynamic_slice(padded, (top, left), (patch_size, patch_size))
        width = beam_width[row, col, slot]
        beamed = (beam_map(width, patch_size) * window.astype(jnp.float32)).astype(jnp.bfloat16)
        image = pointing_image(beamed, width, uv_bins[row, col, slot], uv_count[row, col, slot], uv_weight[row, col, slot])
        image = jnp.where(live, image.astype(jnp.float32), jnp.zeros((), jnp.float32))
        current = lax.dynamic_slice(total, (top, left), (patch_size, patch_size))
        return (lax.dynamic_update_slice(total, current + image, (top, left)), None)
    start = jnp.zeros(padded.shape, jnp.float32)
    items = (row_ids.reshape(-1), columns.reshape(-1), slot_ids.reshape(-1), live_ids.reshape(-1))
    total, unused = lax.scan(place, start, items)
    return total[tile_size:-tile_size, tile_size:-tile_size]
```

```python
import functools
import math

import jax
import jax.numpy as jnp
import numpy as np
from jax import lax
from jax.experimental import pallas as pl
from jax.experimental.pallas import tpu as pltpu
from jax.sharding import PartitionSpec as P

F32 = jnp.float32
BF16 = jnp.bfloat16
I32 = jnp.int32
FINE = 32
CHUNK = 256
FIELDS = 8
MESH = pl.DeviceIdType.MESH


def seed_tables(length, fine):
    pixels = np.arange(length, dtype=np.int64)
    rows = np.concatenate([np.arange(fine), fine * np.arange(length // fine)])
    angle = (rows[:, None] * pixels[None, :] % length) * (2.0 * math.pi / length)
    scale = np.where(np.arange(rows.shape[0]) < fine, 1.0 / math.sqrt(length), 1.0)[:, None]
    return (np.cos(angle) * scale).astype(np.float32), (np.sin(angle) * scale).astype(np.float32)


def wide(column, width):
    return jnp.concatenate([column] * (width // column.shape[1]), axis=1)


def kernel(
    meta_ref, cosines_ref, sines_ref, sky_ref, weight_ref, out_ref,
    meta_got, meta_all, outer_ref, inner_ref, weight_got, row_tab, flip_tab, col_tab,
    rows_ref, flip_ref, cols_ref, beamed_ref, first_ref, spread_ref, gx_ref, gy_ref,
    part_send, part_mine, part_got, vis_own, vis_send, vis_got,
    scaled_own, scaled_par, acc_outer, acc_inner, edge_send, edge_got, inner_got,
    meta_sems, sky_sems, weight_sems, part_sems, vis_sems, scaled_sems, par_sems, last_sems,
):
    size = sky_ref.shape[0]
    length = 2 * size
    slots, slots_uv, block = weight_ref.shape[0], weight_ref.shape[1], weight_ref.shape[2]
    half_slots = slots // 2
    ty, tx = lax.axis_index("ty"), lax.axis_index("tx")
    ny, nx = lax.axis_size("ty"), lax.axis_size("tx")
    core = tx % 2
    partner = tx + 1 - 2 * core
    beyond = tx - 1 + 2 * core
    has_up, has_down = ty > 0, ty < ny - 1
    has_beyond = jnp.logical_and(beyond >= 0, beyond < nx)
    has_row = (has_up, has_down)
    row_half = pl.multiple_of((ty % 2) * size, size)
    col_half = pl.multiple_of((1 - core) * size, size)
    to_partner = {"tx": partner}
    to_beyond = {"tx": beyond}
    to_row = ({"ty": ty - 1}, {"ty": ty + 1})
    to_cross = ({"ty": ty - 1, "tx": partner}, {"ty": ty + 1, "tx": partner})

    def remote(src, dst, sems, at, target):
        return pltpu.make_async_remote_copy(
            src_ref=src,
            dst_ref=dst,
            send_sem=sems.at[(0,) + at],
            recv_sem=sems.at[(1,) + at],
            device_id=target,
            device_id_type=MESH,
        )

    def meta_copy(slot, target):
        return remote(meta_ref, meta_got[slot], meta_sems, (slot,), target)

    def meta_partner():
        return meta_copy(0, to_partner)

    def meta_send(side):
        return meta_copy(2 - side, to_row[side]), meta_copy(4 - side, to_cross[side])

    def meta_take(side):
        return meta_copy(1 + side, to_row[side]), meta_copy(3 + side, to_cross[side])

    def sky_partner():
        return remote(sky_ref, inner_ref, sky_sems, (0,), to_partner)

    def sky_beyond():
        return remote(sky_ref, outer_ref, sky_sems, (1,), to_beyond)

    def weight_copy():
        return remote(weight_ref, weight_got, weight_sems, (0,), to_partner)

    def part_copy(d, jj):
        return remote(part_send.at[d, jj], part_got.at[d, jj], part_sems, (d, jj), to_partner)

    def vis_copy(side, slot, jj):
        return remote(vis_send.at[side, jj], vis_got.at[slot, jj], vis_sems, (slot, jj), to_row[side])

    def scaled_copy(side, slot, jj):
        return remote(
            scaled_own.at[1, jj], scaled_own.at[2 * slot, jj], scaled_sems, (slot, jj), to_row[side]
        )

    def par_copy(d, jj):
        return remote(scaled_own.at[d, jj], scaled_par.at[d, jj], par_sems, (d, jj), to_partner)

    def last_edge():
        return remote(edge_send, edge_got, last_sems, (0,), to_beyond)

    def last_inner():
        return remote(acc_inner, inner_got, last_sems, (1,), to_partner)

    for side in range(2):

        @pl.when(jnp.logical_not(has_row[side]))
        def _(side=side):
            vis_got[side] = jnp.zeros(vis_got.shape[1:], BF16)

    @pl.when(jnp.logical_not(has_beyond))
    def _():
        outer_ref[...] = jnp.zeros_like(outer_ref)
        edge_got[...] = jnp.zeros_like(edge_got)

    barrier = pltpu.get_barrier_semaphore()
    pl.semaphore_signal(barrier, inc=1, device_id=to_partner, device_id_type=MESH)

    @pl.when(has_beyond)
    def _():
        pl.semaphore_signal(barrier, inc=1, device_id=to_beyond, device_id_type=MESH)

    for side in range(2):

        @pl.when(has_row[side])
        def _(side=side):
            pl.semaphore_signal(barrier, inc=1, device_id=to_row[side], device_id_type=MESH)
            pl.semaphore_signal(barrier, inc=1, device_id=to_cross[side], device_id_type=MESH)

    pl.semaphore_wait(
        barrier,
        1 + has_beyond.astype(I32) + 2 * has_up.astype(I32) + 2 * has_down.astype(I32),
    )

    @pl.when(has_beyond)
    def _():
        sky_beyond().start()

    meta_partner().start()
    for side in range(2):

        @pl.when(has_row[side])
        def _(side=side):
            for copy in meta_send(side):
                copy.start()

    sky_partner().start()
    weight_copy().start()

    per_block = block // FINE

    def table(j, carry):
        blk, at = j // per_block, pl.ds(pl.multiple_of((j % per_block) * FINE, FINE), FINE)
        for tab, half in ((row_tab, row_half), (col_tab, col_half)):
            lanes = pl.ds(half, size)
            c, s = cosines_ref[pl.ds(FINE + j, 1), lanes], sines_ref[pl.ds(FINE + j, 1), lanes]
            fc, fs = cosines_ref[:FINE, lanes], sines_ref[:FINE, lanes]
            tab[blk, 0, at, :] = (fc * c - fs * s).astype(BF16)
            tab[blk, 1, at, :] = (fs * c + fc * s).astype(BF16)
        return carry

    lax.fori_loop(0, length // FINE, table, 0)

    def flipped(j, carry):
        row = (ty % 2) * (size // FINE) + j
        c, s = cosines_ref[pl.ds(FINE + row, 1), :], sines_ref[pl.ds(FINE + row, 1), :]
        fc, fs = cosines_ref[:FINE, :], sines_ref[:FINE, :]
        at = pl.ds(pl.multiple_of(j * FINE, FINE), FINE)
        cos, sin = (fc * c - fs * s).astype(BF16), (fs * c + fc * s).astype(BF16)
        for blk in range(length // block):
            flip_tab[blk, 0, at, :] = cos[:, blk * block : (blk + 1) * block]
            flip_tab[blk, 1, at, :] = sin[:, blk * block : (blk + 1) * block]
        return carry

    lax.fori_loop(0, size // FINE, flipped, 0)

    meta_partner().wait()
    for side in range(2):

        @pl.when(has_row[side])
        def _(side=side):
            for copy in meta_take(side):
                copy.wait_recv()

        @pl.when(jnp.logical_not(has_row[side]))
        def _(side=side):
            for slot in (1 + side, 3 + side):
                for s in range(slots + 1):
                    for f in range(FIELDS):
                        meta_got[slot][s, f] = 0

    sources = ((meta_got[1], meta_got[3]), (meta_ref, meta_got[0]), (meta_got[2], meta_got[4]))
    even_here = core == 0

    def gather(s, carry):
        for d, (same, other) in enumerate(sources):
            for f in range(FIELDS):
                a, b = same[s, f], other[s, f]
                meta_all[d, 0, s, f] = jnp.where(even_here, a, b)
                meta_all[d, 1, s, f] = jnp.where(even_here, b, a)
        return carry

    lax.fori_loop(0, slots + 1, gather, 0)

    def pointing(d, j):
        even, odd = meta_all[d, 0, slots, 0], meta_all[d, 1, slots, 0]
        from_odd = (j >= even).astype(I32)
        slot = jnp.clip(j - from_odd * even, 0, slots - 1)
        live = j < even + odd
        return from_odd, slot, live

    def bins(d, from_odd, slot, k, which):
        b = meta_all[d, from_odd, slot, 3 + 2 * k + which]
        return jnp.clip(b, 0, length // block - 1)

    def gaussian(shape, axis, shift, decay, live):
        away = lax.broadcasted_iota(I32, shape, axis) + shift
        inside = jnp.logical_and(away >= -size, away < size)
        inside = jnp.logical_and(inside, live)
        away = away.astype(F32)
        if axis == 0:
            fold = away.reshape(shape[0] // 8, 8, shape[1])
            value = jnp.exp(-(fold * fold) * decay[None]).reshape(shape)
        else:
            value = jnp.exp(-(away * away) * wide(decay, shape[1]))
        return jnp.where(inside, value, jnp.zeros(shape, F32))

    def beams(d, from_odd, slot, live):
        oy, ox = meta_all[d, from_odd, slot, 0], meta_all[d, from_odd, slot, 1]
        width = jnp.full((8, 128), meta_all[d, from_odd, slot, 2], I32).astype(F32)
        decay = 1.0 / (2.0 * width * width)
        gy_ref[...] = gaussian((size, 128), 0, (1 - d) * size - oy, decay, live)
        outer_at, inner_at = 3 * core - 1, 1 - core
        gx_ref[0] = gaussian((8, size), 1, (outer_at - from_odd) * size - ox, decay, live)
        gx_ref[1] = gaussian((8, size), 1, (inner_at - from_odd) * size - ox, decay, live)

    def column_tables(d, from_odd, slot):
        for k in range(slots_uv):
            at = bins(d, from_odd, slot, k, 1)
            cols_ref[(2 * k) * block : (2 * k + 1) * block, :] = col_tab[at, 0]
            cols_ref[(2 * k + 1) * block : (2 * k + 2) * block, :] = col_tab[at, 1]

    def forward(d, j, result_ref):
        from_odd, slot, live = pointing(d, j)
        beams(d, from_odd, slot, live)
        column_tables(d, from_odd, slot)
        for k in range(slots_uv):
            at = bins(d, from_odd, slot, k, 0)
            rows_ref[(2 * k) * block : (2 * k + 1) * block, :] = row_tab[at, 0]
            rows_ref[(2 * k + 1) * block : (2 * k + 2) * block, :] = row_tab[at, 1]
        for at in range(0, size, CHUNK):
            cols = slice(at, at + CHUNK)
            value = gx_ref[0, 0:1, cols] * outer_ref[:, cols].astype(F32)
            value = value + gx_ref[1, 0:1, cols] * inner_ref[:, cols].astype(F32)
            beamed_ref[:, cols] = (wide(gy_ref[...], CHUNK) * value).astype(BF16)
        for at in range(0, size, CHUNK):
            cols = slice(at, at + CHUNK)
            first_ref[:, cols] = jnp.dot(
                rows_ref[...], beamed_ref[:, cols], preferred_element_type=F32
            ).astype(BF16)
        for k in range(slots_uv):
            rows = slice(2 * k * block, (2 * k + 2) * block)
            both = lax.dot_general(
                first_ref[rows, :], cols_ref[rows, :], (((1,), (1,)), ((), ())),
                preferred_element_type=F32,
            )
            result_ref[k, :, :block] = both[:block, :block] - both[block:, block:]
            result_ref[k, :, block:] = both[:block, block:] + both[block:, :block]

    def adjoint(d, j, scaled_ref):
        from_odd, slot, live = pointing(d, j)
        beams(d, from_odd, slot, live)
        column_tables(d, from_odd, slot)
        for k in range(slots_uv):
            at = bins(d, from_odd, slot, k, 0)
            flip_ref[:, (2 * k) * block : (2 * k + 1) * block] = flip_tab[at, 0]
            flip_ref[:, (2 * k + 1) * block : (2 * k + 2) * block] = flip_tab[at, 1]
        for k in range(slots_uv):
            rows = slice(2 * k * block, (2 * k + 2) * block)
            value = scaled_ref[k]
            real, turned = value[:, :block], value[:, block:]
            square = jnp.concatenate(
                [value, jnp.concatenate([turned, -real], axis=1)], axis=0
            )
            spread_ref[rows, :] = jnp.dot(
                square, cols_ref[rows, :], preferred_element_type=F32
            ).astype(BF16)
        for at in range(0, size, CHUNK):
            cols = slice(at, at + CHUNK)
            back = jnp.dot(flip_ref[...], spread_ref[:, cols], preferred_element_type=F32)
            back = wide(gy_ref[...], CHUNK) * back
            acc_outer[:, cols] += gx_ref[0, 0:1, cols] * back
            acc_inner[:, cols] += gx_ref[1, 0:1, cols] * back

    mine, theirs = half_slots * core, half_slots * (1 - core)

    @pl.when(has_beyond)
    def _():
        sky_beyond().wait_recv()

    sky_partner().wait_recv()

    def forward_step(s, carry):
        inside = s // (2 * half_slots)
        d = 2 * (s % 2) * (1 - inside) + inside
        jj = (s // 2) * (1 - inside) + (s - 2 * half_slots) * inside

        def role(i, carry):
            @pl.when(i == 0)
            def _():
                forward(d, theirs + jj, part_send.at[d, jj])
                part_copy(d, jj).start()

            @pl.when(i == 1)
            def _():
                forward(d, mine + jj, part_mine.at[d, jj])

            return carry

        lax.fori_loop(0, 2, role, 0)
        part_copy(d, jj).wait_recv()
        total = part_mine[d, jj] + part_got[d, jj]
        for side in range(2):

            @pl.when(jnp.logical_and(d == 2 * side, has_row[side]))
            def _(side=side):
                vis_send[side, jj] = total.astype(BF16)
                vis_copy(side, 1 - side, jj).start()

        @pl.when(d == 1)
        def _():
            vis_own[jj] = total

        return carry

    lax.fori_loop(0, 3 * half_slots, forward_step, 0)

    acc_outer[...] = jnp.zeros_like(acc_outer)
    acc_inner[...] = jnp.zeros_like(acc_inner)
    weight_copy().wait_recv()

    def adjoint_mine(d, jj):
        adjoint(d, mine + jj, scaled_own.at[d, jj])

    def adjoint_theirs(d, jj):
        par_copy(d, jj).wait_recv()
        adjoint(d, theirs + jj, scaled_par.at[d, jj])

    def own_step(jj, carry):
        from_odd, slot, live = pointing(1, mine + jj)
        used = meta_all[1, from_odd, slot, 3 + 2 * slots_uv]
        here = from_odd == core
        for side in range(2):

            @pl.when(has_row[side])
            def _(side=side):
                vis_copy(1 - side, side, jj).wait_recv()

        for k in range(slots_uv):
            weight = jnp.where(here, weight_ref[slot, k], weight_got[slot, k]).astype(F32)
            weight = weight * jnp.where(k < used, 1.0, 0.0).astype(F32)
            total = vis_own[jj, k] + vis_got[0, jj, k].astype(F32) + vis_got[1, jj, k].astype(F32)
            scaled_own[1, jj, k] = (total * wide(weight, 2 * block)).astype(BF16)
        for side in range(2):

            @pl.when(has_row[side])
            def _(side=side):
                scaled_copy(side, 1 - side, jj).start()

        par_copy(1, jj).start()
        adjoint_mine(1, jj)
        adjoint_theirs(1, jj)
        return carry

    lax.fori_loop(0, half_slots, own_step, 0)

    def other_step(jj, carry):
        for side in range(2):

            @pl.when(has_row[side])
            def _(side=side):
                scaled_copy(1 - side, side, jj).wait_recv()
                par_copy(2 * side, jj).start()

        for side in range(2):

            @pl.when(has_row[side])
            def _(side=side):
                adjoint_mine(2 * side, jj)

        for side in range(2):

            @pl.when(has_row[side])
            def _(side=side):
                adjoint_theirs(2 * side, jj)

        return carry

    lax.fori_loop(0, half_slots, other_step, 0)

    @pl.when(has_beyond)
    def _():
        edge_send[...] = acc_outer[...].astype(BF16)
        last_edge().start()

    last_inner().start()

    sky_partner().wait_send()
    weight_copy().wait_send()

    @pl.when(has_beyond)
    def _():
        sky_beyond().wait_send()

    for side in range(2):

        @pl.when(has_row[side])
        def _(side=side):
            for copy in meta_send(side):
                copy.wait_send()
            for jj in range(half_slots):
                vis_copy(side, 1 - side, jj).wait_send()
                scaled_copy(side, 1 - side, jj).wait_send()
                par_copy(2 * side, jj).wait_send()

    for jj in range(half_slots):
        par_copy(1, jj).wait_send()
        for d in range(3):
            part_copy(d, jj).wait_send()

    last_inner().wait()

    @pl.when(has_beyond)
    def _():
        last_edge().wait()

    out_ref[...] = inner_got[...] + edge_got[...].astype(F32)


def shards(sky, point_count, point_offset, beam_width, uv_bins, uv_count, uv_weight):
    size = sky.shape[0]
    length = 2 * size
    slots, slots_uv, block = uv_weight.shape[2], uv_weight.shape[3], uv_weight.shape[4]
    half_slots = slots // 2
    depth = 2 * slots_uv * block
    cosines, sines = seed_tables(length, FINE)
    rows = jnp.concatenate(
        [
            point_offset.reshape(slots, 2),
            beam_width.reshape(slots, 1).astype(I32),
            uv_bins.reshape(slots, 2 * slots_uv),
            uv_count.reshape(slots, 1),
        ],
        axis=1,
    )
    count = jnp.broadcast_to(point_count.reshape(1, 1), (1, FIELDS))
    meta = jnp.concatenate([rows, count], axis=0)
    weight = uv_weight.reshape(slots, slots_uv, block, block)

    dma = pltpu.SemaphoreType.DMA
    meta_shape = (slots + 1, FIELDS)
    tile = pltpu.VMEM((size, size), BF16)
    plane = pltpu.VMEM((size, size), F32)
    patch = (slots_uv, block, 2 * block)
    return pl.pallas_call(
        kernel,
        out_shape=jax.ShapeDtypeStruct((size, size), F32),
        in_specs=[pl.BlockSpec(memory_space=pltpu.SMEM)]
        + [pl.BlockSpec(memory_space=pltpu.VMEM)] * 4,
        out_specs=pl.BlockSpec(memory_space=pltpu.VMEM),
        scratch_shapes=[
            tuple([pltpu.SMEM(meta_shape, I32)] * 5),
            pltpu.SMEM((3, 2) + meta_shape, I32),
            tile,
            tile,
            pltpu.VMEM(weight.shape, BF16),
            pltpu.VMEM((length // block, 2, block, size), BF16),
            pltpu.VMEM((length // block, 2, size, block), BF16),
            pltpu.VMEM((length // block, 2, block, size), BF16),
            pltpu.VMEM((depth, size), BF16),
            pltpu.VMEM((size, depth), BF16),
            pltpu.VMEM((depth, size), BF16),
            tile,
            pltpu.VMEM((depth, size), BF16),
            pltpu.VMEM((depth, size), BF16),
            pltpu.VMEM((2, 8, size), F32),
            pltpu.VMEM((size, 128), F32),
            pltpu.VMEM((3, half_slots) + patch, F32),
            pltpu.VMEM((3, half_slots) + patch, F32),
            pltpu.VMEM((3, half_slots) + patch, F32),
            pltpu.VMEM((half_slots,) + patch, F32),
            pltpu.VMEM((2, half_slots) + patch, BF16),
            pltpu.VMEM((2, half_slots) + patch, BF16),
            pltpu.VMEM((3, half_slots) + patch, BF16),
            pltpu.VMEM((3, half_slots) + patch, BF16),
            plane,
            plane,
            tile,
            tile,
            plane,
            dma((2, 5)),
            dma((2, 2)),
            dma((2, 1)),
            dma((2, 3, half_slots)),
            dma((2, 2, half_slots)),
            dma((2, 2, half_slots)),
            dma((2, 3, half_slots)),
            dma((2, 2)),
        ],
        compiler_params=pltpu.CompilerParams(
            vmem_limit_bytes=56 * 1024 * 1024, collective_id=0, has_side_effects=True
        ),
    )(meta, cosines, sines, sky, weight)


def solution(mesh):
    in_specs = (
        P("ty", "tx"),
        P("ty", "tx"),
        P("ty", "tx", None, None),
        P("ty", "tx", None),
        P("ty", "tx", None, None, None),
        P("ty", "tx", None),
        P("ty", "tx", None, None, None, None),
    )
    out_specs = P("ty", "tx")
    return jax.shard_map(shards, mesh=mesh, in_specs=in_specs, out_specs=out_specs, check_vma=False)
```

```python
import functools
import math

import jax
import jax.numpy as jnp
import numpy as np
from jax import lax
from jax.experimental import pallas as pl
from jax.experimental.pallas import tpu as pltpu
from jax.sharding import PartitionSpec as P

F32 = jnp.float32
BF16 = jnp.bfloat16
I32 = jnp.int32
FINE = 32
CHUNK = 256
BANDS = 4
FIELDS = 8
MESH = pl.DeviceIdType.MESH


def seed_tables(length, fine):
    pixels = np.arange(length, dtype=np.int64)
    rows = np.concatenate([np.arange(fine), fine * np.arange(length // fine)])
    angle = (rows[:, None] * pixels[None, :] % length) * (2.0 * math.pi / length)
    scale = np.where(np.arange(rows.shape[0]) < fine, 1.0 / math.sqrt(length), 1.0)[:, None]
    return (np.cos(angle) * scale).astype(np.float32), (np.sin(angle) * scale).astype(np.float32)


def wide(column, width):
    return jnp.concatenate([column] * (width // column.shape[1]), axis=1)


def kernel(
    count_in, offset_in, width_in, bins_in, used_in, cosines_in, sines_in, sky_in, weight_in,
    inner_got, edge_got,
    meta_ref, meta_got, meta_all, sky_ref, outer_ref, inner_ref, weight_ref, weight_got,
    cosines_ref, sines_ref, row_tab, flip_tab, col_tab,
    rows_ref, flip_ref, cols_ref, beamed_ref, first_ref, spread_ref, gx_ref, gy_ref,
    part_send, part_mine, part_got, vis_own, vis_send, vis_got,
    scaled_own, scaled_par, acc_outer, acc_inner, edge_send,
    local_sems, meta_sems, sky_sems, weight_sems, part_sems, vis_sems, scaled_sems, par_sems, last_sems,
):
    size = sky_ref.shape[0]
    length = 2 * size
    slots, slots_uv, block = weight_ref.shape[0], weight_ref.shape[1], weight_ref.shape[2]
    half_slots = slots // 2
    ty, tx = lax.axis_index("ty"), lax.axis_index("tx")
    ny, nx = lax.axis_size("ty"), lax.axis_size("tx")
    core = tx % 2
    partner = tx + 1 - 2 * core
    beyond = tx - 1 + 2 * core
    has_up, has_down = ty > 0, ty < ny - 1
    has_beyond = jnp.logical_and(beyond >= 0, beyond < nx)
    has_row = (has_up, has_down)
    row_half = pl.multiple_of((ty % 2) * size, size)
    col_half = pl.multiple_of((1 - core) * size, size)
    to_partner = {"tx": partner}
    to_beyond = {"tx": beyond}
    to_row = ({"ty": ty - 1}, {"ty": ty + 1})
    to_cross = ({"ty": ty - 1, "tx": partner}, {"ty": ty + 1, "tx": partner})

    local = [
        pltpu.make_async_copy(source, target, local_sems.at[i])
        for i, (source, target) in enumerate(
            (
                (sky_in, sky_ref),
                (cosines_in, cosines_ref),
                (sines_in, sines_ref),
                (weight_in, weight_ref),
            )
        )
    ]

    def remote(src, dst, sems, at, target):
        return pltpu.make_async_remote_copy(
            src_ref=src,
            dst_ref=dst,
            send_sem=sems.at[(0,) + at],
            recv_sem=sems.at[(1,) + at],
            device_id=target,
            device_id_type=MESH,
        )

    def meta_copy(slot, target):
        return remote(meta_ref, meta_got[slot], meta_sems, (slot,), target)

    def meta_partner():
        return meta_copy(0, to_partner)

    def meta_send(side):
        return meta_copy(2 - side, to_row[side]), meta_copy(4 - side, to_cross[side])

    def meta_take(side):
        return meta_copy(1 + side, to_row[side]), meta_copy(3 + side, to_cross[side])

    def sky_partner():
        return remote(sky_ref, inner_ref, sky_sems, (0,), to_partner)

    def sky_beyond():
        return remote(sky_ref, outer_ref, sky_sems, (1,), to_beyond)

    def weight_copy():
        return remote(weight_ref, weight_got, weight_sems, (0,), to_partner)

    def part_copy(d, jj):
        return remote(part_send.at[d, jj], part_got.at[d, jj], part_sems, (d, jj), to_partner)

    def vis_copy(side, slot, jj):
        return remote(vis_send.at[side, jj], vis_got.at[slot, jj], vis_sems, (slot, jj), to_row[side])

    def scaled_copy(side, slot, jj):
        return remote(
            scaled_own.at[1, jj], scaled_own.at[2 * slot, jj], scaled_sems, (slot, jj), to_row[side]
        )

    def par_copy(d, jj):
        return remote(scaled_own.at[d, jj], scaled_par.at[d, jj], par_sems, (d, jj), to_partner)

    def last_edge():
        return remote(edge_send, edge_got, last_sems, (0,), to_beyond)

    def last_inner():
        return remote(acc_inner, inner_got, last_sems, (1,), to_partner)

    barrier = pltpu.get_barrier_semaphore()
    pl.semaphore_signal(barrier, inc=1, device_id=to_partner, device_id_type=MESH)

    @pl.when(has_beyond)
    def _():
        pl.semaphore_signal(barrier, inc=1, device_id=to_beyond, device_id_type=MESH)

    for side in range(2):

        @pl.when(has_row[side])
        def _(side=side):
            pl.semaphore_signal(barrier, inc=1, device_id=to_row[side], device_id_type=MESH)
            pl.semaphore_signal(barrier, inc=1, device_id=to_cross[side], device_id_type=MESH)

    for copy in local:
        copy.start()

    meta_ref[slots, 0] = count_in[0, 0]
    for s in range(slots):
        meta_ref[s, 0] = offset_in[0, s]
        meta_ref[s, 1] = offset_in[1, s]
        meta_ref[s, 2] = width_in[0, s]
        for k in range(slots_uv):
            for which in range(2):
                meta_ref[s, 3 + 2 * k + which] = bins_in[k, which, s]
        meta_ref[s, 3 + 2 * slots_uv] = used_in[0, s]

    for side in range(2):

        @pl.when(jnp.logical_not(has_row[side]))
        def _(side=side):
            vis_got[side] = jnp.zeros(vis_got.shape[1:], BF16)

    @pl.when(jnp.logical_not(has_beyond))
    def _():
        outer_ref[...] = jnp.zeros_like(outer_ref)
        edge_got[...] = jnp.zeros_like(edge_got)

    acc_outer[...] = jnp.zeros_like(acc_outer)
    acc_inner[...] = jnp.zeros_like(acc_inner)

    local[0].wait()
    pl.semaphore_wait(
        barrier,
        1 + has_beyond.astype(I32) + 2 * has_up.astype(I32) + 2 * has_down.astype(I32),
    )

    @pl.when(has_beyond)
    def _():
        sky_beyond().start()

    sky_partner().start()
    meta_partner().start()
    for side in range(2):

        @pl.when(has_row[side])
        def _(side=side):
            for copy in meta_send(side):
                copy.start()

    for copy in local[1:]:
        copy.wait()
    weight_copy().start()

    per_block = block // FINE

    def table(j, carry):
        blk, at = j // per_block, pl.ds(pl.multiple_of((j % per_block) * FINE, FINE), FINE)
        for tab, half in ((row_tab, row_half), (col_tab, col_half)):
            lanes = pl.ds(half, size)
            c, s = cosines_ref[pl.ds(FINE + j, 1), lanes], sines_ref[pl.ds(FINE + j, 1), lanes]
            fc, fs = cosines_ref[:FINE, lanes], sines_ref[:FINE, lanes]
            tab[blk, 0, at, :] = (fc * c - fs * s).astype(BF16)
            tab[blk, 1, at, :] = (fs * c + fc * s).astype(BF16)
        return carry

    lax.fori_loop(0, length // FINE, table, 0)

    def flipped(j, carry):
        row = (ty % 2) * (size // FINE) + j
        c, s = cosines_ref[pl.ds(FINE + row, 1), :], sines_ref[pl.ds(FINE + row, 1), :]
        fc, fs = cosines_ref[:FINE, :], sines_ref[:FINE, :]
        at = pl.ds(pl.multiple_of(j * FINE, FINE), FINE)
        cos, sin = (fc * c - fs * s).astype(BF16), (fs * c + fc * s).astype(BF16)
        for blk in range(length // block):
            flip_tab[blk, 0, at, :] = cos[:, blk * block : (blk + 1) * block]
            flip_tab[blk, 1, at, :] = sin[:, blk * block : (blk + 1) * block]
        return carry

    lax.fori_loop(0, size // FINE, flipped, 0)

    meta_partner().wait()
    for side in range(2):

        @pl.when(has_row[side])
        def _(side=side):
            for copy in meta_take(side):
                copy.wait_recv()

        @pl.when(jnp.logical_not(has_row[side]))
        def _(side=side):
            for slot in (1 + side, 3 + side):
                meta_got[slot][slots, 0] = 0
                for s in range(slots):
                    for f in range(FIELDS):
                        meta_got[slot][s, f] = 0

    sources = ((meta_got[1], meta_got[3]), (meta_ref, meta_got[0]), (meta_got[2], meta_got[4]))
    even_here = core == 0

    def gather(s, f):
        for d, (same, other) in enumerate(sources):
            a, b = same[s, f], other[s, f]
            meta_all[d, 0, s, f] = jnp.where(even_here, a, b)
            meta_all[d, 1, s, f] = jnp.where(even_here, b, a)

    def gather_slot(s, carry):
        for f in range(FIELDS):
            gather(s, f)
        return carry

    lax.fori_loop(0, slots, gather_slot, 0)
    gather(slots, 0)

    def pointing(d, j):
        even, odd = meta_all[d, 0, slots, 0], meta_all[d, 1, slots, 0]
        from_odd = (j >= even).astype(I32)
        slot = jnp.clip(j - from_odd * even, 0, slots - 1)
        live = j < even + odd
        return from_odd, slot, live

    def bins(d, from_odd, slot, k, which):
        b = meta_all[d, from_odd, slot, 3 + 2 * k + which]
        return jnp.clip(b, 0, length // block - 1)

    def gaussian(shape, axis, shift, decay, live):
        away = lax.broadcasted_iota(I32, shape, axis) + shift
        inside = jnp.logical_and(away >= -size, away < size)
        inside = jnp.logical_and(inside, live)
        away = away.astype(F32)
        if axis == 0:
            fold = away.reshape(shape[0] // 8, 8, shape[1])
            value = jnp.exp(-(fold * fold) * decay[None]).reshape(shape)
        else:
            value = jnp.exp(-(away * away) * wide(decay, shape[1]))
        return jnp.where(inside, value, jnp.zeros(shape, F32))

    def beams(d, from_odd, slot, live):
        oy, ox = meta_all[d, from_odd, slot, 0], meta_all[d, from_odd, slot, 1]
        width = jnp.full((8, 128), meta_all[d, from_odd, slot, 2], I32).astype(F32)
        decay = 1.0 / (2.0 * width * width)
        gy_ref[...] = gaussian((size, 128), 0, (1 - d) * size - oy, decay, live)
        outer_at, inner_at = 3 * core - 1, 1 - core
        gx_ref[0] = gaussian((8, size), 1, (outer_at - from_odd) * size - ox, decay, live)
        gx_ref[1] = gaussian((8, size), 1, (inner_at - from_odd) * size - ox, decay, live)

    def column_tables(d, from_odd, slot):
        for k in range(slots_uv):
            at = bins(d, from_odd, slot, k, 1)
            cols_ref[(2 * k) * block : (2 * k + 1) * block, :] = col_tab[at, 0]
            cols_ref[(2 * k + 1) * block : (2 * k + 2) * block, :] = col_tab[at, 1]

    def forward(d, j, result_ref):
        from_odd, slot, live = pointing(d, j)
        beams(d, from_odd, slot, live)
        column_tables(d, from_odd, slot)
        for k in range(slots_uv):
            at = bins(d, from_odd, slot, k, 0)
            rows_ref[(2 * k) * block : (2 * k + 1) * block, :] = row_tab[at, 0]
            rows_ref[(2 * k + 1) * block : (2 * k + 2) * block, :] = row_tab[at, 1]
        for at in range(0, size, CHUNK):
            cols = slice(at, at + CHUNK)
            value = gx_ref[0, 0:1, cols] * outer_ref[:, cols].astype(F32)
            value = value + gx_ref[1, 0:1, cols] * inner_ref[:, cols].astype(F32)
            beamed_ref[:, cols] = (wide(gy_ref[...], CHUNK) * value).astype(BF16)
        for at in range(0, size, CHUNK):
            cols = slice(at, at + CHUNK)
            first_ref[:, cols] = jnp.dot(
                rows_ref[...], beamed_ref[:, cols], preferred_element_type=F32
            ).astype(BF16)
        for k in range(slots_uv):
            rows = slice(2 * k * block, (2 * k + 2) * block)
            both = lax.dot_general(
                first_ref[rows, :], cols_ref[rows, :], (((1,), (1,)), ((), ())),
                preferred_element_type=F32,
            )
            result_ref[k, :, :block] = both[:block, :block] - both[block:, block:]
            result_ref[k, :, block:] = both[:block, block:] + both[block:, :block]

    def adjoint(d, j, scaled_ref):
        from_odd, slot, live = pointing(d, j)
        beams(d, from_odd, slot, live)
        column_tables(d, from_odd, slot)
        for k in range(slots_uv):
            at = bins(d, from_odd, slot, k, 0)
            flip_ref[:, (2 * k) * block : (2 * k + 1) * block] = flip_tab[at, 0]
            flip_ref[:, (2 * k + 1) * block : (2 * k + 2) * block] = flip_tab[at, 1]
        for k in range(slots_uv):
            rows = slice(2 * k * block, (2 * k + 2) * block)
            value = scaled_ref[k]
            real, turned = value[:, :block], value[:, block:]
            square = jnp.concatenate(
                [value, jnp.concatenate([turned, -real], axis=1)], axis=0
            )
            spread_ref[rows, :] = jnp.dot(
                square, cols_ref[rows, :], preferred_element_type=F32
            ).astype(BF16)
        for at in range(0, size, CHUNK):
            cols = slice(at, at + CHUNK)
            back = jnp.dot(flip_ref[...], spread_ref[:, cols], preferred_element_type=F32)
            back = wide(gy_ref[...], CHUNK) * back
            acc_outer[:, cols] += gx_ref[0, 0:1, cols] * back
            acc_inner[:, cols] += gx_ref[1, 0:1, cols] * back

    mine, theirs = half_slots * core, half_slots * (1 - core)

    @pl.when(has_beyond)
    def _():
        sky_beyond().wait_recv()

    sky_partner().wait_recv()

    def member(g, i):
        own = g // half_slots
        d = 2 * i * (1 - own) + own
        jj = g * (1 - own) + i * own
        return d, jj

    def forward_group(g, carry):
        def give(i, carry):
            d, jj = member(g, i)
            forward(d, theirs + jj, part_send.at[d, jj])
            part_copy(d, jj).start()
            return carry

        def take(i, carry):
            d, jj = member(g, i)
            forward(d, mine + jj, part_mine)
            part_copy(d, jj).wait_recv()
            total = part_mine[...] + part_got[d, jj]
            for side in range(2):

                @pl.when(jnp.logical_and(d == 2 * side, has_row[side]))
                def _(side=side):
                    vis_send[side, jj] = total.astype(BF16)
                    vis_copy(side, 1 - side, jj).start()

            @pl.when(d == 1)
            def _():
                vis_own[jj] = total

            return carry

        lax.fori_loop(0, 2, give, 0)
        lax.fori_loop(0, 2, take, 0)
        return carry

    lax.fori_loop(0, half_slots + 1, forward_group, 0)

    weight_copy().wait_recv()

    def adjoint_mine(d, jj):
        adjoint(d, mine + jj, scaled_own.at[d, jj])

    def adjoint_theirs(d, jj):
        par_copy(d, jj).wait_recv()
        adjoint(d, theirs + jj, scaled_par.at[d, jj])

    def own_step(jj, carry):
        from_odd, slot, live = pointing(1, mine + jj)
        used = meta_all[1, from_odd, slot, 3 + 2 * slots_uv]
        here = from_odd == core
        for side in range(2):

            @pl.when(has_row[side])
            def _(side=side):
                vis_copy(1 - side, side, jj).wait_recv()

        for k in range(slots_uv):
            weight = jnp.where(here, weight_ref[slot, k], weight_got[slot, k]).astype(F32)
            weight = weight * jnp.where(k < used, 1.0, 0.0).astype(F32)
            total = vis_own[jj, k] + vis_got[0, jj, k].astype(F32) + vis_got[1, jj, k].astype(F32)
            scaled_own[1, jj, k] = (total * wide(weight, 2 * block)).astype(BF16)
        for side in range(2):

            @pl.when(has_row[side])
            def _(side=side):
                scaled_copy(side, 1 - side, jj).start()

        par_copy(1, jj).start()
        adjoint_mine(1, jj)
        adjoint_theirs(1, jj)
        return carry

    lax.fori_loop(0, half_slots, own_step, 0)

    def other_step(jj, carry):
        for side in range(2):

            @pl.when(has_row[side])
            def _(side=side):
                scaled_copy(1 - side, side, jj).wait_recv()
                par_copy(2 * side, jj).start()

        for side in range(2):

            @pl.when(has_row[side])
            def _(side=side):
                adjoint_mine(2 * side, jj)

        for side in range(2):

            @pl.when(has_row[side])
            def _(side=side):
                adjoint_theirs(2 * side, jj)

        return carry

    lax.fori_loop(0, half_slots, other_step, 0)

    @pl.when(has_beyond)
    def _():
        edge_send[...] = acc_outer[...].astype(BF16)
        last_edge().start()

    last_inner().start()

    sky_partner().wait_send()
    weight_copy().wait_send()

    @pl.when(has_beyond)
    def _():
        sky_beyond().wait_send()

    for side in range(2):

        @pl.when(has_row[side])
        def _(side=side):
            for copy in meta_send(side):
                copy.wait_send()
            for jj in range(half_slots):
                vis_copy(side, 1 - side, jj).wait_send()
                scaled_copy(side, 1 - side, jj).wait_send()
                par_copy(2 * side, jj).wait_send()

    for jj in range(half_slots):
        par_copy(1, jj).wait_send()
        for d in range(3):
            part_copy(d, jj).wait_send()

    last_inner().wait()

    @pl.when(has_beyond)
    def _():
        last_edge().wait()


def add_kernel(inner_ref, edge_ref, out_hbm, out_ref, sems):
    band = out_ref.shape[0] // BANDS
    copies = []
    for i in range(BANDS):
        rows = slice(i * band, (i + 1) * band)
        out_ref[rows, :] = inner_ref[rows, :] + edge_ref[rows, :].astype(F32)
        copies.append(pltpu.make_async_copy(out_ref.at[rows], out_hbm.at[rows], sems.at[i]))
        copies[-1].start()
    for copy in copies:
        copy.wait()


def shards(sky, point_count, point_offset, beam_width, uv_bins, uv_count, uv_weight):
    size = sky.shape[0]
    length = 2 * size
    slots, slots_uv, block = uv_weight.shape[2], uv_weight.shape[3], uv_weight.shape[4]
    half_slots = slots // 2
    depth = 2 * slots_uv * block
    cosines, sines = seed_tables(length, FINE)
    count = point_count.reshape(1, 1)
    offset = jnp.transpose(point_offset, (0, 1, 3, 2)).reshape(2, slots)
    width = beam_width.astype(I32).reshape(1, slots)
    bins = jnp.transpose(uv_bins, (0, 1, 3, 4, 2)).reshape(slots_uv, 2, slots)
    used = uv_count.reshape(1, slots)
    weight = uv_weight.reshape(slots, slots_uv, block, block)

    dma = pltpu.SemaphoreType.DMA
    meta_shape = (slots + 1, FIELDS)
    tile = pltpu.VMEM((size, size), BF16)
    plane = pltpu.VMEM((size, size), F32)
    patch = (slots_uv, block, 2 * block)
    vmem = pl.BlockSpec(memory_space=pltpu.VMEM)
    inner, edge = pl.pallas_call(
        kernel,
        out_shape=(jax.ShapeDtypeStruct((size, size), F32), jax.ShapeDtypeStruct((size, size), BF16)),
        in_specs=[pl.BlockSpec(memory_space=pltpu.SMEM)] * 5
        + [pl.BlockSpec(memory_space=pl.ANY)] * 4,
        out_specs=(vmem, vmem),
        scratch_shapes=[
            pltpu.SMEM(meta_shape, I32),
            tuple([pltpu.SMEM(meta_shape, I32)] * 5),
            pltpu.SMEM((3, 2) + meta_shape, I32),
            tile,
            tile,
            tile,
            pltpu.VMEM(weight.shape, BF16),
            pltpu.VMEM(weight.shape, BF16),
            pltpu.VMEM(cosines.shape, F32),
            pltpu.VMEM(sines.shape, F32),
            pltpu.VMEM((length // block, 2, block, size), BF16),
            pltpu.VMEM((length // block, 2, size, block), BF16),
            pltpu.VMEM((length // block, 2, block, size), BF16),
            pltpu.VMEM((depth, size), BF16),
            pltpu.VMEM((size, depth), BF16),
            pltpu.VMEM((depth, size), BF16),
            tile,
            pltpu.VMEM((depth, size), BF16),
            pltpu.VMEM((depth, size), BF16),
            pltpu.VMEM((2, 8, size), F32),
            pltpu.VMEM((size, 128), F32),
            pltpu.VMEM((3, half_slots) + patch, F32),
            pltpu.VMEM(patch, F32),
            pltpu.VMEM((3, half_slots) + patch, F32),
            pltpu.VMEM((half_slots,) + patch, F32),
            pltpu.VMEM((2, half_slots) + patch, BF16),
            pltpu.VMEM((2, half_slots) + patch, BF16),
            pltpu.VMEM((3, half_slots) + patch, BF16),
            pltpu.VMEM((3, half_slots) + patch, BF16),
            plane,
            plane,
            tile,
            dma((4,)),
            dma((2, 5)),
            dma((2, 2)),
            dma((2, 1)),
            dma((2, 3, half_slots)),
            dma((2, 2, half_slots)),
            dma((2, 2, half_slots)),
            dma((2, 3, half_slots)),
            dma((2, 2)),
        ],
        compiler_params=pltpu.CompilerParams(
            vmem_limit_bytes=30 * 1024 * 1024, collective_id=0, has_side_effects=True
        ),
    )(count, offset, width, bins, used, cosines, sines, sky, weight)
    return pl.pallas_call(
        add_kernel,
        out_shape=jax.ShapeDtypeStruct((size, size), F32),
        in_specs=[vmem, vmem],
        out_specs=pl.BlockSpec(memory_space=pl.ANY),
        scratch_shapes=[plane, dma((BANDS,))],
        compiler_params=pltpu.CompilerParams(vmem_limit_bytes=8 * 1024 * 1024),
        cost_estimate=pl.CostEstimate(flops=size * size, bytes_accessed=10 * size * size, transcendentals=0),
    )(inner, edge)


def solution(mesh):
    in_specs = (
        P("ty", "tx"),
        P("ty", "tx"),
        P("ty", "tx", None, None),
        P("ty", "tx", None),
        P("ty", "tx", None, None, None),
        P("ty", "tx", None),
        P("ty", "tx", None, None, None, None),
    )
    out_specs = P("ty", "tx")
    return jax.shard_map(shards, mesh=mesh, in_specs=in_specs, out_specs=out_specs, check_vma=False)
```

```python
import functools
import math

import jax
import jax.numpy as jnp
import numpy as np
from jax import lax
from jax.experimental import pallas as pl
from jax.experimental.pallas import tpu as pltpu
from jax.sharding import PartitionSpec as P

F32 = jnp.float32
BF16 = jnp.bfloat16
I32 = jnp.int32
FINE = 32
CHUNK = 256
BANDS = 4
FIELDS = 8
MESH = pl.DeviceIdType.MESH


def seed_tables(length, fine):
    pixels = np.arange(length, dtype=np.int64)
    rows = np.concatenate([np.arange(fine), fine * np.arange(length // fine)])
    angle = (rows[:, None] * pixels[None, :] % length) * (2.0 * math.pi / length)
    scale = np.where(np.arange(rows.shape[0]) < fine, 1.0 / math.sqrt(length), 1.0)[:, None]
    return np.stack([np.cos(angle) * scale, np.sin(angle) * scale]).astype(np.float32)


def wide(column, width):
    return jnp.concatenate([column] * (width // column.shape[1]), axis=1)


def kernel(
    count_in, offset_in, width_in, bins_in, used_in, seeds_in, sky_in, weight_in,
    inner_got, edge_got,
    meta_ref, meta_got, meta_all, sky_ref, outer_ref, inner_ref, weight_ref, weight_got,
    seeds_ref, row_tab, flip_tab, col_tab,
    rows_ref, flip_ref, cols_ref, beamed_ref, first_ref, spread_ref, gx_ref, gy_ref,
    part_send, part_got, totals, raw_send, raw_got, sum_send, sum_got,
    scaled_own, scaled_par, acc_outer, acc_inner, edge_send,
    local_sems, meta_sems, sky_sems, weight_sems, part_sems, raw_sems, sum_sems, scaled_sems,
    onward_sems, par_sems, last_sems,
):
    size = sky_ref.shape[0]
    length = 2 * size
    slots, slots_uv, block = weight_ref.shape[0], weight_ref.shape[1], weight_ref.shape[2]
    half_slots = slots // 2
    ty, tx = lax.axis_index("ty"), lax.axis_index("tx")
    ny, nx = lax.axis_size("ty"), lax.axis_size("tx")
    core = tx % 2
    partner = tx + 1 - 2 * core
    beyond = tx - 1 + 2 * core
    has_up, has_down = ty > 0, ty < ny - 1
    has_beyond = jnp.logical_and(beyond >= 0, beyond < nx)
    has_row = (has_up, has_down)
    row_half = pl.multiple_of((ty % 2) * size, size)
    col_half = pl.multiple_of((1 - core) * size, size)
    to_partner = {"tx": partner}
    to_beyond = {"tx": beyond}
    to_row = ({"ty": ty - 1}, {"ty": ty + 1})
    to_cross = ({"ty": ty - 1, "tx": partner}, {"ty": ty + 1, "tx": partner})
    odd_row = ty % 2
    d_far, d_mate = 2 * odd_row, 2 * (1 - odd_row)
    giving, fed = ty - 2 + 4 * odd_row, ty + 2 - 4 * odd_row
    has_far = jnp.logical_and(giving >= 0, giving < ny)
    has_fed = jnp.logical_and(fed >= 0, fed < ny)
    to_mate, to_giving, to_fed = {"ty": ty + 1 - 2 * odd_row}, {"ty": giving}, {"ty": fed}

    local = [
        pltpu.make_async_copy(source, target, local_sems.at[i])
        for i, (source, target) in enumerate(
            (
                (sky_in, sky_ref),
                (seeds_in, seeds_ref),
                (weight_in, weight_ref),
            )
        )
    ]

    def remote(src, dst, sems, at, target):
        return pltpu.make_async_remote_copy(
            src_ref=src,
            dst_ref=dst,
            send_sem=sems.at[(0,) + at],
            recv_sem=sems.at[(1,) + at],
            device_id=target,
            device_id_type=MESH,
        )

    def meta_copy(slot, target):
        return remote(meta_ref, meta_got[slot], meta_sems, (slot,), target)

    def meta_partner():
        return meta_copy(0, to_partner)

    def meta_send(side):
        return meta_copy(2 - side, to_row[side]), meta_copy(4 - side, to_cross[side])

    def meta_take(side):
        return meta_copy(1 + side, to_row[side]), meta_copy(3 + side, to_cross[side])

    def sky_partner():
        return remote(sky_ref, inner_ref, sky_sems, (0,), to_partner)

    def sky_beyond():
        return remote(sky_ref, outer_ref, sky_sems, (1,), to_beyond)

    def weight_copy():
        return remote(weight_ref, weight_got, weight_sems, (0,), to_partner)

    def part_copy(g, jj):
        return remote(part_send.at[g, jj], part_got.at[g, jj], part_sems, (g, jj), to_partner)

    def raw_copy(target, jj, k):
        return remote(raw_send.at[jj, k], raw_got.at[jj, k], raw_sems, (jj, k), target)

    def sum_copy(jj, k):
        return remote(sum_send.at[jj, k], sum_got.at[jj, k], sum_sems, (jj, k), to_mate)

    def scaled_copy(jj, k):
        return remote(
            scaled_own.at[2, jj, k], scaled_own.at[1, jj, k], scaled_sems, (jj, k), to_mate
        )

    def onward_copy(target, jj, k):
        return remote(
            scaled_own.at[1, jj, k], scaled_own.at[0, jj, k], onward_sems, (jj, k), target
        )

    def par_copy(g, jj):
        return remote(scaled_own.at[g, jj], scaled_par.at[g, jj], par_sems, (g, jj), to_partner)

    def last_edge():
        return remote(edge_send, edge_got, last_sems, (0,), to_beyond)

    def last_inner():
        return remote(acc_inner, inner_got, last_sems, (1,), to_partner)

    barrier = pltpu.get_barrier_semaphore()
    pl.semaphore_signal(barrier, inc=1, device_id=to_partner, device_id_type=MESH)

    @pl.when(has_beyond)
    def _():
        pl.semaphore_signal(barrier, inc=1, device_id=to_beyond, device_id_type=MESH)

    for side in range(2):

        @pl.when(has_row[side])
        def _(side=side):
            pl.semaphore_signal(barrier, inc=1, device_id=to_row[side], device_id_type=MESH)
            pl.semaphore_signal(barrier, inc=1, device_id=to_cross[side], device_id_type=MESH)

    for has, target in ((has_far, to_giving), (has_fed, to_fed)):

        @pl.when(has)
        def _(target=target):
            pl.semaphore_signal(barrier, inc=1, device_id=target, device_id_type=MESH)

    for copy in local:
        copy.start()

    meta_ref[slots, 0] = count_in[0, 0]
    for s in range(slots):
        meta_ref[s, 0] = offset_in[0, s]
        meta_ref[s, 1] = offset_in[1, s]
        meta_ref[s, 2] = width_in[0, s]
        for k in range(slots_uv):
            for which in range(2):
                meta_ref[s, 3 + 2 * k + which] = bins_in[k, which, s]
        meta_ref[s, 3 + 2 * slots_uv] = used_in[0, s]

    @pl.when(jnp.logical_not(has_fed))
    def _():
        raw_got[...] = jnp.zeros_like(raw_got)

    @pl.when(jnp.logical_not(has_beyond))
    def _():
        outer_ref[...] = jnp.zeros_like(outer_ref)
        edge_got[...] = jnp.zeros_like(edge_got)

    acc_outer[...] = jnp.zeros_like(acc_outer)
    acc_inner[...] = jnp.zeros_like(acc_inner)

    local[0].wait()
    pl.semaphore_wait(
        barrier,
        1 + has_beyond.astype(I32) + 2 * has_up.astype(I32) + 2 * has_down.astype(I32)
        + has_far.astype(I32) + has_fed.astype(I32),
    )

    @pl.when(has_beyond)
    def _():
        sky_beyond().start()

    sky_partner().start()
    meta_partner().start()
    for side in range(2):

        @pl.when(has_row[side])
        def _(side=side):
            for copy in meta_send(side):
                copy.start()

    for copy in local[1:]:
        copy.wait()
    weight_copy().start()

    per_block = block // FINE

    def table(j, carry):
        blk, at = j // per_block, pl.ds(pl.multiple_of((j % per_block) * FINE, FINE), FINE)
        for tab, half in ((row_tab, row_half), (col_tab, col_half)):
            lanes = pl.ds(half, size)
            c, s = seeds_ref[0, pl.ds(FINE + j, 1), lanes], seeds_ref[1, pl.ds(FINE + j, 1), lanes]
            fc, fs = seeds_ref[0, :FINE, lanes], seeds_ref[1, :FINE, lanes]
            tab[blk, 0, at, :] = (fc * c - fs * s).astype(BF16)
            tab[blk, 1, at, :] = (fs * c + fc * s).astype(BF16)
        return carry

    lax.fori_loop(0, length // FINE, table, 0)

    def flipped(j, carry):
        row = (ty % 2) * (size // FINE) + j
        c, s = seeds_ref[0, pl.ds(FINE + row, 1), :], seeds_ref[1, pl.ds(FINE + row, 1), :]
        fc, fs = seeds_ref[0, :FINE, :], seeds_ref[1, :FINE, :]
        at = pl.ds(pl.multiple_of(j * FINE, FINE), FINE)
        cos, sin = (fc * c - fs * s).astype(BF16), (fs * c + fc * s).astype(BF16)
        for blk in range(length // block):
            flip_tab[blk, 0, at, :] = cos[:, blk * block : (blk + 1) * block]
            flip_tab[blk, 1, at, :] = sin[:, blk * block : (blk + 1) * block]
        return carry

    lax.fori_loop(0, size // FINE, flipped, 0)

    meta_partner().wait()
    for side in range(2):

        @pl.when(has_row[side])
        def _(side=side):
            for copy in meta_take(side):
                copy.wait_recv()

        @pl.when(jnp.logical_not(has_row[side]))
        def _(side=side):
            for slot in (1 + side, 3 + side):
                meta_got[slot][slots, 0] = 0
                for s in range(slots):
                    for f in range(FIELDS):
                        meta_got[slot][s, f] = 0

    sources = ((meta_got[1], meta_got[3]), (meta_ref, meta_got[0]), (meta_got[2], meta_got[4]))
    even_here = core == 0

    def gather(s, f):
        for d, (same, other) in enumerate(sources):
            a, b = same[s, f], other[s, f]
            meta_all[d, 0, s, f] = jnp.where(even_here, a, b)
            meta_all[d, 1, s, f] = jnp.where(even_here, b, a)

    def gather_slot(s, carry):
        for f in range(FIELDS):
            gather(s, f)
        return carry

    lax.fori_loop(0, slots, gather_slot, 0)
    gather(slots, 0)

    def pointing(d, j):
        even, odd = meta_all[d, 0, slots, 0], meta_all[d, 1, slots, 0]
        from_odd = (j >= even).astype(I32)
        slot = jnp.clip(j - from_odd * even, 0, slots - 1)
        live = j < even + odd
        return from_odd, slot, live

    def bins(d, from_odd, slot, k, which):
        b = meta_all[d, from_odd, slot, 3 + 2 * k + which]
        return jnp.clip(b, 0, length // block - 1)

    def gaussian(shape, axis, shift, decay, live):
        away = lax.broadcasted_iota(I32, shape, axis) + shift
        inside = jnp.logical_and(away >= -size, away < size)
        inside = jnp.logical_and(inside, live)
        away = away.astype(F32)
        if axis == 0:
            fold = away.reshape(shape[0] // 8, 8, shape[1])
            value = jnp.exp(-(fold * fold) * decay[None]).reshape(shape)
        else:
            value = jnp.exp(-(away * away) * wide(decay, shape[1]))
        return jnp.where(inside, value, jnp.zeros(shape, F32))

    def beams(d, from_odd, slot, live):
        oy, ox = meta_all[d, from_odd, slot, 0], meta_all[d, from_odd, slot, 1]
        width = jnp.full((8, 128), meta_all[d, from_odd, slot, 2], I32).astype(F32)
        decay = 1.0 / (2.0 * width * width)
        gy_ref[...] = gaussian((size, 128), 0, (1 - d) * size - oy, decay, live)
        outer_at, inner_at = 3 * core - 1, 1 - core
        gx_ref[0] = gaussian((8, size), 1, (outer_at - from_odd) * size - ox, decay, live)
        gx_ref[1] = gaussian((8, size), 1, (inner_at - from_odd) * size - ox, decay, live)

    def column_tables(d, from_odd, slot):
        for k in range(slots_uv):
            at = bins(d, from_odd, slot, k, 1)
            cols_ref[(2 * k) * block : (2 * k + 1) * block, :] = col_tab[at, 0]
            cols_ref[(2 * k + 1) * block : (2 * k + 2) * block, :] = col_tab[at, 1]

    def forward(d, j, result_ref):
        from_odd, slot, live = pointing(d, j)
        beams(d, from_odd, slot, live)
        column_tables(d, from_odd, slot)
        for k in range(slots_uv):
            at = bins(d, from_odd, slot, k, 0)
            rows_ref[(2 * k) * block : (2 * k + 1) * block, :] = row_tab[at, 0]
            rows_ref[(2 * k + 1) * block : (2 * k + 2) * block, :] = row_tab[at, 1]
        for at in range(0, size, CHUNK):
            cols = slice(at, at + CHUNK)
            value = gx_ref[0, 0:1, cols] * outer_ref[:, cols].astype(F32)
            value = value + gx_ref[1, 0:1, cols] * inner_ref[:, cols].astype(F32)
            beamed_ref[:, cols] = (wide(gy_ref[...], CHUNK) * value).astype(BF16)
        for at in range(0, size, CHUNK):
            cols = slice(at, at + CHUNK)
            first_ref[:, cols] = jnp.dot(
                rows_ref[...], beamed_ref[:, cols], preferred_element_type=F32
            ).astype(BF16)
        for k in range(slots_uv):
            rows = slice(2 * k * block, (2 * k + 2) * block)
            both = lax.dot_general(
                first_ref[rows, :], cols_ref[rows, :], (((1,), (1,)), ((), ())),
                preferred_element_type=F32,
            )
            result_ref[k, :, :block] = both[:block, :block] - both[block:, block:]
            result_ref[k, :, block:] = both[:block, block:] + both[block:, :block]

    def adjoint(d, j, scaled_ref):
        from_odd, slot, live = pointing(d, j)
        beams(d, from_odd, slot, live)
        column_tables(d, from_odd, slot)
        for k in range(slots_uv):
            at = bins(d, from_odd, slot, k, 0)
            flip_ref[:, (2 * k) * block : (2 * k + 1) * block] = flip_tab[at, 0]
            flip_ref[:, (2 * k + 1) * block : (2 * k + 2) * block] = flip_tab[at, 1]
        for k in range(slots_uv):
            rows = slice(2 * k * block, (2 * k + 2) * block)
            value = scaled_ref[k]
            real, turned = value[:, :block], value[:, block:]
            square = jnp.concatenate(
                [value, jnp.concatenate([turned, -real], axis=1)], axis=0
            )
            spread_ref[rows, :] = jnp.dot(
                square, cols_ref[rows, :], preferred_element_type=F32
            ).astype(BF16)
        for at in range(0, size, CHUNK):
            cols = slice(at, at + CHUNK)
            back = jnp.dot(flip_ref[...], spread_ref[:, cols], preferred_element_type=F32)
            back = wide(gy_ref[...], CHUNK) * back
            acc_outer[:, cols] += gx_ref[0, 0:1, cols] * back
            acc_inner[:, cols] += gx_ref[1, 0:1, cols] * back

    mine, theirs = half_slots * core, half_slots * (1 - core)

    @pl.when(has_beyond)
    def _():
        sky_beyond().wait_recv()

    sky_partner().wait_recv()

    def give(g, d):
        def step(jj, carry):
            forward(d, theirs + jj, part_send.at[g, jj])
            part_copy(g, jj).start()
            return carry

        lax.fori_loop(0, half_slots, step, 0)

    def take(g, d, after):
        def step(jj, carry):
            forward(d, mine + jj, totals.at[g, jj])
            part_copy(g, jj).wait_recv()
            after(jj)
            return carry

        lax.fori_loop(0, half_slots, step, 0)

    def give_far(jj):
        for k in range(slots_uv):
            raw_send[jj, k] = (totals[0, jj, k] + part_got[0, jj, k]).astype(BF16)
            raw_copy(to_giving, jj, k).start()

    def keep(g):
        def add(jj):
            totals[g, jj] = totals[g, jj] + part_got[g, jj]

        return add

    @pl.when(has_far)
    def _():
        give(0, d_far)
        take(0, d_far, give_far)

    give(1, d_mate)
    take(1, d_mate, keep(1))
    give(2, 1)
    take(2, 1, keep(2))

    for jj in range(half_slots):
        for k in range(slots_uv):

            @pl.when(has_fed)
            def _(jj=jj, k=k):
                raw_copy(to_fed, jj, k).wait_recv()

            sum_send[jj, k] = (totals[1, jj, k] + raw_got[jj, k].astype(F32)).astype(BF16)
            sum_copy(jj, k).start()

    weight_copy().wait_recv()
    for jj in range(half_slots):
        from_odd, slot, live = pointing(1, mine + jj)
        used = meta_all[1, from_odd, slot, 3 + 2 * slots_uv]
        here = from_odd == core
        for k in range(slots_uv):
            weight = jnp.where(here, weight_ref[slot, k], weight_got[slot, k]).astype(F32)
            weight = weight * jnp.where(k < used, 1.0, 0.0).astype(F32)
            sum_copy(jj, k).wait_recv()
            total = totals[2, jj, k] + sum_got[jj, k].astype(F32)
            scaled_own[2, jj, k] = (total * wide(weight, 2 * block)).astype(BF16)
            scaled_copy(jj, k).start()
        par_copy(2, jj).start()

    def adjoint_group(g, d):
        def step_mine(jj, carry):
            adjoint(d, mine + jj, scaled_own.at[g, jj])
            return carry

        def step_theirs(jj, carry):
            par_copy(g, jj).wait_recv()
            adjoint(d, theirs + jj, scaled_par.at[g, jj])
            return carry

        return step_mine, step_theirs

    for step in adjoint_group(2, 1):
        lax.fori_loop(0, half_slots, step, 0)

    for jj in range(half_slots):
        for k in range(slots_uv):
            scaled_copy(jj, k).wait_recv()

            @pl.when(has_fed)
            def _(jj=jj, k=k):
                onward_copy(to_fed, jj, k).start()

        par_copy(1, jj).start()

    for step in adjoint_group(1, d_mate):
        lax.fori_loop(0, half_slots, step, 0)

    @pl.when(has_far)
    def _():
        step_mine, step_theirs = adjoint_group(0, d_far)

        def step(jj, carry):
            for k in range(slots_uv):
                onward_copy(to_giving, jj, k).wait_recv()
            par_copy(0, jj).start()
            return step_mine(jj, carry)

        lax.fori_loop(0, half_slots, step, 0)
        lax.fori_loop(0, half_slots, step_theirs, 0)

    @pl.when(has_beyond)
    def _():
        edge_send[...] = acc_outer[...].astype(BF16)
        last_edge().start()

    last_inner().start()

    sky_partner().wait_send()
    weight_copy().wait_send()

    @pl.when(has_beyond)
    def _():
        sky_beyond().wait_send()

    for side in range(2):

        @pl.when(has_row[side])
        def _(side=side):
            for copy in meta_send(side):
                copy.wait_send()

    for jj in range(half_slots):
        for g in (1, 2):
            part_copy(g, jj).wait_send()
            par_copy(g, jj).wait_send()
        for k in range(slots_uv):
            sum_copy(jj, k).wait_send()
            scaled_copy(jj, k).wait_send()

            @pl.when(has_fed)
            def _(jj=jj, k=k):
                onward_copy(to_fed, jj, k).wait_send()

        @pl.when(has_far)
        def _(jj=jj):
            part_copy(0, jj).wait_send()
            par_copy(0, jj).wait_send()
            for k in range(slots_uv):
                raw_copy(to_giving, jj, k).wait_send()

    last_inner().wait()

    @pl.when(has_beyond)
    def _():
        last_edge().wait()


def add_kernel(inner_ref, edge_ref, out_hbm, out_ref, sems):
    band = out_ref.shape[0] // BANDS
    copies = []
    for i in range(BANDS):
        rows = slice(i * band, (i + 1) * band)
        out_ref[rows, :] = inner_ref[rows, :] + edge_ref[rows, :].astype(F32)
        copies.append(pltpu.make_async_copy(out_ref.at[rows], out_hbm.at[rows], sems.at[i]))
        copies[-1].start()
    for copy in copies:
        copy.wait()


def shards(sky, point_count, point_offset, beam_width, uv_bins, uv_count, uv_weight):
    size = sky.shape[0]
    length = 2 * size
    slots, slots_uv, block = uv_weight.shape[2], uv_weight.shape[3], uv_weight.shape[4]
    half_slots = slots // 2
    depth = 2 * slots_uv * block
    seeds = seed_tables(length, FINE)
    count = point_count.reshape(1, 1)
    offset = jnp.transpose(point_offset, (0, 1, 3, 2)).reshape(2, slots)
    width = beam_width.astype(I32).reshape(1, slots)
    bins = jnp.transpose(uv_bins, (0, 1, 3, 4, 2)).reshape(slots_uv, 2, slots)
    used = uv_count.reshape(1, slots)
    weight = uv_weight.reshape(slots, slots_uv, block, block)

    dma = pltpu.SemaphoreType.DMA
    meta_shape = (slots + 1, FIELDS)
    tile = pltpu.VMEM((size, size), BF16)
    plane = pltpu.VMEM((size, size), F32)
    patch = (slots_uv, block, 2 * block)
    vmem = pl.BlockSpec(memory_space=pltpu.VMEM)
    inner, edge = pl.pallas_call(
        kernel,
        out_shape=(jax.ShapeDtypeStruct((size, size), F32), jax.ShapeDtypeStruct((size, size), BF16)),
        in_specs=[pl.BlockSpec(memory_space=pltpu.SMEM)] * 5
        + [pl.BlockSpec(memory_space=pl.ANY)] * 3,
        out_specs=(vmem, vmem),
        scratch_shapes=[
            pltpu.SMEM(meta_shape, I32),
            tuple([pltpu.SMEM(meta_shape, I32)] * 5),
            pltpu.SMEM((3, 2) + meta_shape, I32),
            tile,
            tile,
            tile,
            pltpu.VMEM(weight.shape, BF16),
            pltpu.VMEM(weight.shape, BF16),
            pltpu.VMEM(seeds.shape, F32),
            pltpu.VMEM((length // block, 2, block, size), BF16),
            pltpu.VMEM((length // block, 2, size, block), BF16),
            pltpu.VMEM((length // block, 2, block, size), BF16),
            pltpu.VMEM((depth, size), BF16),
            pltpu.VMEM((size, depth), BF16),
            pltpu.VMEM((depth, size), BF16),
            tile,
            pltpu.VMEM((depth, size), BF16),
            pltpu.VMEM((depth, size), BF16),
            pltpu.VMEM((2, 8, size), F32),
            pltpu.VMEM((size, 128), F32),
            pltpu.VMEM((3, half_slots) + patch, F32),
            pltpu.VMEM((3, half_slots) + patch, F32),
            pltpu.VMEM((3, half_slots) + patch, F32),
            pltpu.VMEM((half_slots,) + patch, BF16),
            pltpu.VMEM((half_slots,) + patch, BF16),
            pltpu.VMEM((half_slots,) + patch, BF16),
            pltpu.VMEM((half_slots,) + patch, BF16),
            pltpu.VMEM((3, half_slots) + patch, BF16),
            pltpu.VMEM((3, half_slots) + patch, BF16),
            plane,
            plane,
            tile,
            dma((3,)),
            dma((2, 5)),
            dma((2, 2)),
            dma((2, 1)),
            dma((2, 3, half_slots)),
            dma((2, half_slots, slots_uv)),
            dma((2, half_slots, slots_uv)),
            dma((2, half_slots, slots_uv)),
            dma((2, half_slots, slots_uv)),
            dma((2, 3, half_slots)),
            dma((2, 2)),
        ],
        compiler_params=pltpu.CompilerParams(
            vmem_limit_bytes=int(56 * 1024 * 1024), collective_id=0, has_side_effects=True
        ),
    )(count, offset, width, bins, used, seeds, sky, weight)
    return pl.pallas_call(
        add_kernel,
        out_shape=jax.ShapeDtypeStruct((size, size), F32),
        in_specs=[vmem, vmem],
        out_specs=pl.BlockSpec(memory_space=pl.ANY),
        scratch_shapes=[plane, dma((BANDS,))],
        compiler_params=pltpu.CompilerParams(vmem_limit_bytes=8 * 1024 * 1024),
        cost_estimate=pl.CostEstimate(flops=size * size, bytes_accessed=10 * size * size, transcendentals=0),
    )(inner, edge)


def solution(mesh):
    in_specs = (
        P("ty", "tx"),
        P("ty", "tx"),
        P("ty", "tx", None, None),
        P("ty", "tx", None),
        P("ty", "tx", None, None, None),
        P("ty", "tx", None),
        P("ty", "tx", None, None, None, None),
    )
    out_specs = P("ty", "tx")
    return jax.shard_map(shards, mesh=mesh, in_specs=in_specs, out_specs=out_specs, check_vma=False)
```

```python
import functools
import math

import jax
import jax.numpy as jnp
import numpy as np
from jax import lax
from jax.experimental import pallas as pl
from jax.experimental.pallas import tpu as pltpu
from jax.sharding import PartitionSpec as P

F32 = jnp.float32
BF16 = jnp.bfloat16
I32 = jnp.int32
FINE = 32
CHUNK = 256
BANDS = 4
FIELDS = 8
MESH = pl.DeviceIdType.MESH


def seed_tables(length, fine):
    pixels = np.arange(length, dtype=np.int64)
    rows = np.concatenate([np.arange(fine), fine * np.arange(length // fine)])
    angle = (rows[:, None] * pixels[None, :] % length) * (2.0 * math.pi / length)
    scale = np.where(np.arange(rows.shape[0]) < fine, 1.0 / math.sqrt(length), 1.0)[:, None]
    return np.stack([np.cos(angle) * scale, np.sin(angle) * scale]).astype(np.float32)


def wide(column, width):
    return jnp.concatenate([column] * (width // column.shape[1]), axis=1)


def kernel(
    count_in, offset_in, width_in, bins_in, used_in, seeds_in, sky_in, weight_in,
    inner_got, edge_got,
    meta_ref, meta_got, meta_all, sky_ref, outer_ref, inner_ref, weight_ref, weight_got,
    seeds_ref, row_tab, flip_tab, col_tab,
    beamed_ref, first_ref, spread_ref, gx_ref, gy_ref,
    part_send, part_got, totals, raw_send, raw_got, sum_send, sum_got,
    scaled_own, scaled_par, acc_outer, acc_inner, edge_send,
    local_sems, meta_sems, sky_sems, weight_sems, part_sems, raw_sems, sum_sems, scaled_sems,
    onward_sems, par_sems, last_sems,
):
    size = sky_ref.shape[0]
    length = 2 * size
    slots, slots_uv, block = weight_ref.shape[0], weight_ref.shape[1], weight_ref.shape[2]
    half_slots = slots // 2
    ty, tx = lax.axis_index("ty"), lax.axis_index("tx")
    ny, nx = lax.axis_size("ty"), lax.axis_size("tx")
    core = tx % 2
    partner = tx + 1 - 2 * core
    beyond = tx - 1 + 2 * core
    has_up, has_down = ty > 0, ty < ny - 1
    has_beyond = jnp.logical_and(beyond >= 0, beyond < nx)
    has_row = (has_up, has_down)
    row_half = pl.multiple_of((ty % 2) * size, size)
    col_half = pl.multiple_of((1 - core) * size, size)
    to_partner = {"tx": partner}
    to_beyond = {"tx": beyond}
    to_row = ({"ty": ty - 1}, {"ty": ty + 1})
    to_cross = ({"ty": ty - 1, "tx": partner}, {"ty": ty + 1, "tx": partner})
    odd_row = ty % 2
    d_far, d_mate = 2 * odd_row, 2 * (1 - odd_row)
    giving, fed = ty - 2 + 4 * odd_row, ty + 2 - 4 * odd_row
    has_far = jnp.logical_and(giving >= 0, giving < ny)
    has_fed = jnp.logical_and(fed >= 0, fed < ny)
    to_mate, to_giving, to_fed = {"ty": ty + 1 - 2 * odd_row}, {"ty": giving}, {"ty": fed}

    local = [
        pltpu.make_async_copy(source, target, local_sems.at[i])
        for i, (source, target) in enumerate(
            (
                (sky_in, sky_ref),
                (seeds_in, seeds_ref),
                (weight_in, weight_ref),
            )
        )
    ]

    def remote(src, dst, sems, at, target):
        return pltpu.make_async_remote_copy(
            src_ref=src,
            dst_ref=dst,
            send_sem=sems.at[(0,) + at],
            recv_sem=sems.at[(1,) + at],
            device_id=target,
            device_id_type=MESH,
        )

    def meta_copy(slot, target):
        return remote(meta_ref, meta_got[slot], meta_sems, (slot,), target)

    def meta_partner():
        return meta_copy(0, to_partner)

    def meta_send(side):
        return meta_copy(2 - side, to_row[side]), meta_copy(4 - side, to_cross[side])

    def meta_take(side):
        return meta_copy(1 + side, to_row[side]), meta_copy(3 + side, to_cross[side])

    def sky_partner():
        return remote(sky_ref, inner_ref, sky_sems, (0,), to_partner)

    def sky_beyond():
        return remote(sky_ref, outer_ref, sky_sems, (1,), to_beyond)

    def weight_copy():
        return remote(weight_ref, weight_got, weight_sems, (0,), to_partner)

    def part_copy(g, jj):
        return remote(part_send.at[g, jj], part_got.at[g, jj], part_sems, (g, jj), to_partner)

    def raw_copy(target, jj, k):
        return remote(raw_send.at[jj, k], raw_got.at[jj, k], raw_sems, (jj, k), target)

    def sum_copy(jj, k):
        return remote(sum_send.at[jj, k], sum_got.at[jj, k], sum_sems, (jj, k), to_mate)

    def scaled_copy(jj, k):
        return remote(
            scaled_own.at[2, jj, k], scaled_own.at[1, jj, k], scaled_sems, (jj, k), to_mate
        )

    def onward_copy(target, jj, k):
        return remote(
            scaled_own.at[1, jj, k], scaled_own.at[0, jj, k], onward_sems, (jj, k), target
        )

    def par_copy(g, jj):
        return remote(scaled_own.at[g, jj], scaled_par.at[g, jj], par_sems, (g, jj), to_partner)

    def last_edge():
        return remote(edge_send, edge_got, last_sems, (0,), to_beyond)

    def last_inner():
        return remote(acc_inner, inner_got, last_sems, (1,), to_partner)

    barrier = pltpu.get_barrier_semaphore()
    pl.semaphore_signal(barrier, inc=1, device_id=to_partner, device_id_type=MESH)

    @pl.when(has_beyond)
    def _():
        pl.semaphore_signal(barrier, inc=1, device_id=to_beyond, device_id_type=MESH)

    for side in range(2):

        @pl.when(has_row[side])
        def _(side=side):
            pl.semaphore_signal(barrier, inc=1, device_id=to_row[side], device_id_type=MESH)
            pl.semaphore_signal(barrier, inc=1, device_id=to_cross[side], device_id_type=MESH)

    for has, target in ((has_far, to_giving), (has_fed, to_fed)):

        @pl.when(has)
        def _(target=target):
            pl.semaphore_signal(barrier, inc=1, device_id=target, device_id_type=MESH)

    for copy in local:
        copy.start()

    meta_ref[slots, 0] = count_in[0, 0]
    for s in range(slots):
        meta_ref[s, 0] = offset_in[0, s]
        meta_ref[s, 1] = offset_in[1, s]
        meta_ref[s, 2] = width_in[0, s]
        for k in range(slots_uv):
            for which in range(2):
                meta_ref[s, 3 + 2 * k + which] = bins_in[k, which, s]
        meta_ref[s, 3 + 2 * slots_uv] = used_in[0, s]

    @pl.when(jnp.logical_not(has_beyond))
    def _():
        outer_ref[...] = jnp.zeros_like(outer_ref)
        edge_got[...] = jnp.zeros_like(edge_got)

    acc_outer[...] = jnp.zeros_like(acc_outer)
    acc_inner[...] = jnp.zeros_like(acc_inner)

    with jax.named_scope("barrier"):
        local[0].wait()
        pl.semaphore_wait(
            barrier,
            1 + has_beyond.astype(I32) + 2 * has_up.astype(I32) + 2 * has_down.astype(I32)
            + has_far.astype(I32) + has_fed.astype(I32),
        )

    @pl.when(has_beyond)
    def _():
        sky_beyond().start()

    sky_partner().start()
    meta_partner().start()
    for side in range(2):

        @pl.when(has_row[side])
        def _(side=side):
            for copy in meta_send(side):
                copy.start()

    for copy in local[1:]:
        copy.wait()
    weight_copy().start()

    per_block = block // FINE

    def table(j, carry):
        blk, at = j // per_block, pl.ds(pl.multiple_of((j % per_block) * FINE, FINE), FINE)
        for tab, half in ((row_tab, row_half), (col_tab, col_half)):
            lanes = pl.ds(half, size)
            c, s = seeds_ref[0, pl.ds(FINE + j, 1), lanes], seeds_ref[1, pl.ds(FINE + j, 1), lanes]
            fc, fs = seeds_ref[0, :FINE, lanes], seeds_ref[1, :FINE, lanes]
            tab[blk, at, :] = (fc * c - fs * s).astype(BF16)
            tab[blk, pl.ds(pl.multiple_of(block + (j % per_block) * FINE, FINE), FINE), :] = (fs * c + fc * s).astype(BF16)
        return carry

    with jax.named_scope("tables"):
        lax.fori_loop(0, length // FINE, table, 0)

    def flipped(j, carry):
        row = (ty % 2) * (size // FINE) + j
        c, s = seeds_ref[0, pl.ds(FINE + row, 1), :], seeds_ref[1, pl.ds(FINE + row, 1), :]
        fc, fs = seeds_ref[0, :FINE, :], seeds_ref[1, :FINE, :]
        at = pl.ds(pl.multiple_of(j * FINE, FINE), FINE)
        cos, sin = (fc * c - fs * s).astype(BF16), (fs * c + fc * s).astype(BF16)
        for blk in range(length // block):
            flip_tab[blk, at, :block] = cos[:, blk * block : (blk + 1) * block]
            flip_tab[blk, at, block:] = sin[:, blk * block : (blk + 1) * block]
        return carry

    with jax.named_scope("flips"):
        lax.fori_loop(0, size // FINE, flipped, 0)

    with jax.named_scope("meta"):
        meta_partner().wait()
        for side in range(2):

            @pl.when(has_row[side])
            def _(side=side):
                for copy in meta_take(side):
                    copy.wait_recv()

            @pl.when(jnp.logical_not(has_row[side]))
            def _(side=side):
                for slot in (1 + side, 3 + side):
                    meta_got[slot][slots, 0] = 0
                    for s in range(slots):
                        for f in range(FIELDS):
                            meta_got[slot][s, f] = 0

    sources = ((meta_got[1], meta_got[3]), (meta_ref, meta_got[0]), (meta_got[2], meta_got[4]))
    even_here = core == 0

    def gather(s, f):
        for d, (same, other) in enumerate(sources):
            a, b = same[s, f], other[s, f]
            meta_all[d, 0, s, f] = jnp.where(even_here, a, b)
            meta_all[d, 1, s, f] = jnp.where(even_here, b, a)

    def gather_slot(s, carry):
        for f in range(FIELDS):
            gather(s, f)
        return carry

    lax.fori_loop(0, slots, gather_slot, 0)
    gather(slots, 0)

    def pointing(d, j):
        even, odd = meta_all[d, 0, slots, 0], meta_all[d, 1, slots, 0]
        from_odd = (j >= even).astype(I32)
        slot = jnp.clip(j - from_odd * even, 0, slots - 1)
        live = j < even + odd
        return from_odd, slot, live

    def bins(d, from_odd, slot, k, which):
        b = meta_all[d, from_odd, slot, 3 + 2 * k + which]
        return jnp.clip(b, 0, length // block - 1)

    def gaussian(shape, axis, shift, decay, live):
        away = lax.broadcasted_iota(I32, shape, axis) + shift
        inside = jnp.logical_and(away >= -size, away < size)
        inside = jnp.logical_and(inside, live)
        away = away.astype(F32)
        if axis == 0:
            fold = away.reshape(shape[0] // 8, 8, shape[1])
            value = jnp.exp(-(fold * fold) * decay[None]).reshape(shape)
        else:
            value = jnp.exp(-(away * away) * wide(decay, shape[1]))
        return jnp.where(inside, value, jnp.zeros(shape, F32))

    def beams(i, carry):
        d, j = i // slots, i % slots
        from_odd, slot, live = pointing(d, j)
        oy, ox = meta_all[d, from_odd, slot, 0], meta_all[d, from_odd, slot, 1]
        width = jnp.full((8, 128), meta_all[d, from_odd, slot, 2], I32).astype(F32)
        decay = 1.0 / (2.0 * width * width)
        gy_ref[d, j] = gaussian((size, 128), 0, (1 - d) * size - oy, decay, live)
        outer_at, inner_at = 3 * core - 1, 1 - core
        gx_ref[d, j, 0] = gaussian((8, size), 1, (outer_at - from_odd) * size - ox, decay, live)
        gx_ref[d, j, 1] = gaussian((8, size), 1, (inner_at - from_odd) * size - ox, decay, live)
        return carry

    with jax.named_scope("beams"):
        lax.fori_loop(0, 3 * slots, beams, 0)

    def column_table(d, from_odd, slot, k):
        return col_tab[bins(d, from_odd, slot, k, 1)]

    def forward(d, j, result_ref):
        from_odd, slot, live = pointing(d, j)
        rows = jnp.concatenate(
            [row_tab[bins(d, from_odd, slot, k, 0)] for k in range(slots_uv)], axis=0
        )
        gy = wide(gy_ref[d, j], CHUNK)
        for at in range(0, size, CHUNK):
            cols = slice(at, at + CHUNK)
            value = gx_ref[d, j, 0, 0:1, cols] * outer_ref[:, cols].astype(F32)
            value = value + gx_ref[d, j, 1, 0:1, cols] * inner_ref[:, cols].astype(F32)
            beamed_ref[:, cols] = (gy * value).astype(BF16)
        for at in range(0, size, CHUNK):
            cols = slice(at, at + CHUNK)
            first_ref[:, cols] = jnp.dot(
                rows, beamed_ref[:, cols], preferred_element_type=F32
            ).astype(BF16)
        for k in range(slots_uv):
            both = lax.dot_general(
                first_ref[2 * k * block : (2 * k + 2) * block, :],
                column_table(d, from_odd, slot, k),
                (((1,), (1,)), ((), ())),
                preferred_element_type=F32,
            )
            result_ref[k, :, :block] = both[:block, :block] - both[block:, block:]
            result_ref[k, :, block:] = both[:block, block:] + both[block:, :block]

    def adjoint(d, j, scaled_ref):
        from_odd, slot, live = pointing(d, j)
        rows = jnp.concatenate(
            [flip_tab[bins(d, from_odd, slot, k, 0)] for k in range(slots_uv)], axis=1
        )
        gy = wide(gy_ref[d, j], CHUNK)
        for k in range(slots_uv):
            value = scaled_ref[k]
            real, turned = value[:, :block], value[:, block:]
            square = jnp.concatenate(
                [value, jnp.concatenate([turned, -real], axis=1)], axis=0
            )
            spread_ref[2 * k * block : (2 * k + 2) * block, :] = jnp.dot(
                square, column_table(d, from_odd, slot, k), preferred_element_type=F32
            ).astype(BF16)
        for at in range(0, size, CHUNK):
            cols = slice(at, at + CHUNK)
            back = gy * jnp.dot(rows, spread_ref[:, cols], preferred_element_type=F32)
            acc_outer[:, cols] += gx_ref[d, j, 0, 0:1, cols] * back
            acc_inner[:, cols] += gx_ref[d, j, 1, 0:1, cols] * back

    mine, theirs = half_slots * core, half_slots * (1 - core)

    with jax.named_scope("sky"):
        @pl.when(has_beyond)
        def _():
            sky_beyond().wait_recv()

        sky_partner().wait_recv()

    def give(g, d):
        def step(jj, carry):
            forward(d, theirs + jj, part_send.at[g, jj])
            part_copy(g, jj).start()
            return carry

        with jax.named_scope(f"give{g}"):
            lax.fori_loop(0, half_slots, step, 0)

    def take(g, d, after):
        def step(jj, carry):
            forward(d, mine + jj, totals.at[g, jj])
            part_copy(g, jj).wait_recv()
            after(jj)
            return carry

        with jax.named_scope(f"take{g}"):
            lax.fori_loop(0, half_slots, step, 0)

    def give_far(jj):
        for k in range(slots_uv):
            raw_send[jj, k] = (totals[0, jj, k] + part_got[0, jj, k]).astype(BF16)
            raw_copy(to_giving, jj, k).start()

    def keep(g):
        def add(jj):
            totals[g, jj] = totals[g, jj] + part_got[g, jj]

        return add

    @pl.when(has_far)
    def _():
        give(0, d_far)
        take(0, d_far, give_far)

    def pass_one(jj, k, fed_too):
        value = totals[1, jj, k]
        if fed_too:
            value = value + raw_got[jj, k].astype(F32)
        sum_send[jj, k] = value.astype(BF16)
        sum_copy(jj, k).start()

    def give_mate(jj):
        totals[1, jj] = totals[1, jj] + part_got[1, jj]

        @pl.when(jnp.logical_not(has_fed))
        def _():
            for k in range(slots_uv):
                pass_one(jj, k, False)

    give(1, d_mate)
    take(1, d_mate, give_mate)
    give(2, 1)
    take(2, 1, keep(2))

    with jax.named_scope("pass_sums"):

        @pl.when(has_fed)
        def _():
            for jj in range(half_slots):
                for k in range(slots_uv):
                    raw_copy(to_fed, jj, k).wait_recv()
                    pass_one(jj, k, True)

    with jax.named_scope("scale"):
        weight_copy().wait_recv()
        for jj in range(half_slots):
            from_odd, slot, live = pointing(1, mine + jj)
            used = meta_all[1, from_odd, slot, 3 + 2 * slots_uv]
            here = from_odd == core
            for k in range(slots_uv):
                weight = jnp.where(here, weight_ref[slot, k], weight_got[slot, k]).astype(F32)
                weight = weight * jnp.where(k < used, 1.0, 0.0).astype(F32)
                sum_copy(jj, k).wait_recv()
                total = totals[2, jj, k] + sum_got[jj, k].astype(F32)
                scaled_own[2, jj, k] = (total * wide(weight, 2 * block)).astype(BF16)
                scaled_copy(jj, k).start()
            par_copy(2, jj).start()

    def adjoint_group(g, d):
        def step_mine(jj, carry):
            adjoint(d, mine + jj, scaled_own.at[g, jj])
            return carry

        def step_theirs(jj, carry):
            par_copy(g, jj).wait_recv()
            adjoint(d, theirs + jj, scaled_par.at[g, jj])
            return carry

        return step_mine, step_theirs

    with jax.named_scope("adj_own"):
        for step in adjoint_group(2, 1):
            lax.fori_loop(0, half_slots, step, 0)

    with jax.named_scope("pass_scaled"):
        for jj in range(half_slots):
            for k in range(slots_uv):
                scaled_copy(jj, k).wait_recv()

                @pl.when(has_fed)
                def _(jj=jj, k=k):
                    onward_copy(to_fed, jj, k).start()

            par_copy(1, jj).start()

    with jax.named_scope("adj_mate"):
        for step in adjoint_group(1, d_mate):
            lax.fori_loop(0, half_slots, step, 0)

    with jax.named_scope("adj_far"):
        @pl.when(has_far)
        def _():
            step_mine, step_theirs = adjoint_group(0, d_far)

            def step(jj, carry):
                for k in range(slots_uv):
                    onward_copy(to_giving, jj, k).wait_recv()
                par_copy(0, jj).start()
                return step_mine(jj, carry)

            lax.fori_loop(0, half_slots, step, 0)
            lax.fori_loop(0, half_slots, step_theirs, 0)

    @pl.when(has_beyond)
    def _():
        edge_send[...] = acc_outer[...].astype(BF16)
        last_edge().start()

    last_inner().start()

    sky_partner().wait_send()
    weight_copy().wait_send()

    @pl.when(has_beyond)
    def _():
        sky_beyond().wait_send()

    for side in range(2):

        @pl.when(has_row[side])
        def _(side=side):
            for copy in meta_send(side):
                copy.wait_send()

    for jj in range(half_slots):
        for g in (1, 2):
            part_copy(g, jj).wait_send()
            par_copy(g, jj).wait_send()
        for k in range(slots_uv):
            sum_copy(jj, k).wait_send()
            scaled_copy(jj, k).wait_send()

            @pl.when(has_fed)
            def _(jj=jj, k=k):
                onward_copy(to_fed, jj, k).wait_send()

        @pl.when(has_far)
        def _(jj=jj):
            part_copy(0, jj).wait_send()
            par_copy(0, jj).wait_send()
            for k in range(slots_uv):
                raw_copy(to_giving, jj, k).wait_send()

    with jax.named_scope("last"):
        last_inner().wait()

        @pl.when(has_beyond)
        def _():
            last_edge().wait()


def add_kernel(inner_ref, edge_ref, out_hbm, out_ref, sems):
    band = out_ref.shape[0] // BANDS
    copies = []
    for i in range(BANDS):
        rows = slice(i * band, (i + 1) * band)
        out_ref[rows, :] = inner_ref[rows, :] + edge_ref[rows, :].astype(F32)
        copies.append(pltpu.make_async_copy(out_ref.at[rows], out_hbm.at[rows], sems.at[i]))
        copies[-1].start()
    for copy in copies:
        copy.wait()


def shards(sky, point_count, point_offset, beam_width, uv_bins, uv_count, uv_weight):
    size = sky.shape[0]
    length = 2 * size
    slots, slots_uv, block = uv_weight.shape[2], uv_weight.shape[3], uv_weight.shape[4]
    half_slots = slots // 2
    depth = 2 * slots_uv * block
    seeds = seed_tables(length, FINE)
    count = point_count.reshape(1, 1)
    offset = jnp.transpose(point_offset, (0, 1, 3, 2)).reshape(2, slots)
    width = beam_width.astype(I32).reshape(1, slots)
    bins = jnp.transpose(uv_bins, (0, 1, 3, 4, 2)).reshape(slots_uv, 2, slots)
    used = uv_count.reshape(1, slots)
    weight = uv_weight.reshape(slots, slots_uv, block, block)

    dma = pltpu.SemaphoreType.DMA
    meta_shape = (slots + 1, FIELDS)
    tile = pltpu.VMEM((size, size), BF16)
    plane = pltpu.VMEM((size, size), F32)
    patch = (slots_uv, block, 2 * block)
    vmem = pl.BlockSpec(memory_space=pltpu.VMEM)
    inner, edge = pl.pallas_call(
        kernel,
        out_shape=(jax.ShapeDtypeStruct((size, size), F32), jax.ShapeDtypeStruct((size, size), BF16)),
        in_specs=[pl.BlockSpec(memory_space=pltpu.SMEM)] * 5
        + [pl.BlockSpec(memory_space=pl.ANY)] * 3,
        out_specs=(vmem, vmem),
        scratch_shapes=[
            pltpu.SMEM(meta_shape, I32),
            tuple([pltpu.SMEM(meta_shape, I32)] * 5),
            pltpu.SMEM((3, 2) + meta_shape, I32),
            tile,
            tile,
            tile,
            pltpu.VMEM(weight.shape, BF16),
            pltpu.VMEM(weight.shape, BF16),
            pltpu.VMEM(seeds.shape, F32),
            pltpu.VMEM((length // block, 2 * block, size), BF16),
            pltpu.VMEM((length // block, size, 2 * block), BF16),
            pltpu.VMEM((length // block, 2 * block, size), BF16),
            tile,
            pltpu.VMEM((depth, size), BF16),
            pltpu.VMEM((depth, size), BF16),
            pltpu.VMEM((3, slots, 2, 8, size), F32),
            pltpu.VMEM((3, slots, size, 128), F32),
            pltpu.VMEM((3, half_slots) + patch, F32),
            pltpu.VMEM((3, half_slots) + patch, F32),
            pltpu.VMEM((3, half_slots) + patch, F32),
            pltpu.VMEM((half_slots,) + patch, BF16),
            pltpu.VMEM((half_slots,) + patch, BF16),
            pltpu.VMEM((half_slots,) + patch, BF16),
            pltpu.VMEM((half_slots,) + patch, BF16),
            pltpu.VMEM((3, half_slots) + patch, BF16),
            pltpu.VMEM((3, half_slots) + patch, BF16),
            plane,
            plane,
            tile,
            dma((3,)),
            dma((2, 5)),
            dma((2, 2)),
            dma((2, 1)),
            dma((2, 3, half_slots)),
            dma((2, half_slots, slots_uv)),
            dma((2, half_slots, slots_uv)),
            dma((2, half_slots, slots_uv)),
            dma((2, half_slots, slots_uv)),
            dma((2, 3, half_slots)),
            dma((2, 2)),
        ],
        compiler_params=pltpu.CompilerParams(
            vmem_limit_bytes=int(56 * 1024 * 1024), collective_id=0, has_side_effects=True
        ),
    )(count, offset, width, bins, used, seeds, sky, weight)
    return pl.pallas_call(
        add_kernel,
        out_shape=jax.ShapeDtypeStruct((size, size), F32),
        in_specs=[vmem, vmem],
        out_specs=pl.BlockSpec(memory_space=pl.ANY),
        scratch_shapes=[plane, dma((BANDS,))],
        compiler_params=pltpu.CompilerParams(vmem_limit_bytes=8 * 1024 * 1024),
        cost_estimate=pl.CostEstimate(flops=size * size, bytes_accessed=10 * size * size, transcendentals=0),
    )(inner, edge)


def solution(mesh):
    in_specs = (
        P("ty", "tx"),
        P("ty", "tx"),
        P("ty", "tx", None, None),
        P("ty", "tx", None),
        P("ty", "tx", None, None, None),
        P("ty", "tx", None),
        P("ty", "tx", None, None, None, None),
    )
    out_specs = P("ty", "tx")
    return jax.shard_map(shards, mesh=mesh, in_specs=in_specs, out_specs=out_specs, check_vma=False)
```

```python
import functools
import math

import jax
import jax.numpy as jnp
import numpy as np
from jax import lax
from jax.experimental import pallas as pl
from jax.experimental.pallas import tpu as pltpu
from jax.sharding import PartitionSpec as P

F32 = jnp.float32
BF16 = jnp.bfloat16
I32 = jnp.int32
FINE = 32
CHUNK = 256
BANDS = 4
FIELDS = 8
MESH = pl.DeviceIdType.MESH


def seed_tables(length, fine):
    pixels = np.arange(length, dtype=np.int64)
    rows = np.concatenate([np.arange(fine), fine * np.arange(length // fine)])
    angle = (rows[:, None] * pixels[None, :] % length) * (2.0 * math.pi / length)
    scale = np.where(np.arange(rows.shape[0]) < fine, 1.0 / math.sqrt(length), 1.0)[:, None]
    return np.stack([np.cos(angle) * scale, np.sin(angle) * scale]).astype(np.float32)


def wide(column, width):
    return jnp.concatenate([column] * (width // column.shape[1]), axis=1)


def kernel(
    count_in, offset_in, width_in, bins_in, used_in, seeds_in, sky_in, weight_in,
    inner_got, edge_got,
    meta_ref, meta_got, meta_all, sky_ref, outer_ref, inner_ref, weight_ref, weight_got,
    seeds_ref, row_tab, flip_tab, col_tab,
    beamed_ref, first_ref, spread_ref, gx_ref, gy_ref,
    early, part_send, part_got, totals, raw_send, raw_got, sum_send, sum_got,
    scaled_own, scaled_par, acc_outer, acc_inner, edge_send, inner_send,
    local_sems, meta_sems, sky_sems, weight_sems, part_sems, raw_sems, sum_sems, scaled_sems,
    onward_sems, par_sems, last_sems,
):
    size = sky_ref.shape[0]
    length = 2 * size
    slots, slots_uv, block = weight_ref.shape[0], weight_ref.shape[1], weight_ref.shape[2]
    half_slots = slots // 2
    ty, tx = lax.axis_index("ty"), lax.axis_index("tx")
    ny, nx = lax.axis_size("ty"), lax.axis_size("tx")
    core = tx % 2
    partner = tx + 1 - 2 * core
    beyond = tx - 1 + 2 * core
    has_up, has_down = ty > 0, ty < ny - 1
    has_beyond = jnp.logical_and(beyond >= 0, beyond < nx)
    has_row = (has_up, has_down)
    row_half = pl.multiple_of((ty % 2) * size, size)
    col_half = pl.multiple_of((1 - core) * size, size)
    to_partner = {"tx": partner}
    to_beyond = {"tx": beyond}
    to_row = ({"ty": ty - 1}, {"ty": ty + 1})
    to_cross = ({"ty": ty - 1, "tx": partner}, {"ty": ty + 1, "tx": partner})
    odd_row = ty % 2
    d_far, d_mate = 2 * odd_row, 2 * (1 - odd_row)
    giving, fed = ty - 2 + 4 * odd_row, ty + 2 - 4 * odd_row
    has_far = jnp.logical_and(giving >= 0, giving < ny)
    has_fed = jnp.logical_and(fed >= 0, fed < ny)
    to_mate, to_giving, to_fed = {"ty": ty + 1 - 2 * odd_row}, {"ty": giving}, {"ty": fed}

    local = [
        pltpu.make_async_copy(source, target, local_sems.at[i])
        for i, (source, target) in enumerate(
            (
                (sky_in, sky_ref),
                (seeds_in, seeds_ref),
                (weight_in, weight_ref),
            )
        )
    ]

    def remote(src, dst, sems, at, target):
        return pltpu.make_async_remote_copy(
            src_ref=src,
            dst_ref=dst,
            send_sem=sems.at[(0,) + at],
            recv_sem=sems.at[(1,) + at],
            device_id=target,
            device_id_type=MESH,
        )

    def meta_copy(slot, target):
        return remote(meta_ref, meta_got[slot], meta_sems, (slot,), target)

    def meta_partner():
        return meta_copy(0, to_partner)

    def meta_send(side):
        return meta_copy(2 - side, to_row[side]), meta_copy(4 - side, to_cross[side])

    def meta_take(side):
        return meta_copy(1 + side, to_row[side]), meta_copy(3 + side, to_cross[side])

    def sky_partner():
        return remote(sky_ref, inner_ref, sky_sems, (0,), to_partner)

    def sky_beyond(part):
        cols = slice(part * CHUNK, (part + 1) * CHUNK)
        return remote(sky_ref.at[:, cols], outer_ref.at[:, cols], sky_sems, (1 + part,), to_beyond)

    def weight_copy():
        return remote(weight_ref, weight_got, weight_sems, (0,), to_partner)

    def part_copy(g, jj):
        return remote(part_send.at[g, jj], part_got.at[g, jj], part_sems, (g, jj), to_partner)

    def raw_copy(target, jj, k):
        return remote(raw_send.at[jj, k], raw_got.at[jj, k], raw_sems, (jj, k), target)

    def sum_copy(jj, k):
        return remote(sum_send.at[jj, k], sum_got.at[jj, k], sum_sems, (jj, k), to_mate)

    def scaled_copy(jj, k):
        return remote(
            scaled_own.at[2, jj, k], scaled_own.at[1, jj, k], scaled_sems, (jj, k), to_mate
        )

    def onward_copy(target, jj, k):
        return remote(
            scaled_own.at[1, jj, k], scaled_own.at[0, jj, k], onward_sems, (jj, k), target
        )

    def par_copy(g, jj):
        return remote(scaled_own.at[g, jj], scaled_par.at[g, jj], par_sems, (g, jj), to_partner)

    def last_edge():
        return remote(edge_send, edge_got, last_sems, (0,), to_beyond)

    def last_inner():
        return remote(inner_send, inner_got, last_sems, (1,), to_partner)

    def no_edge():
        return pltpu.make_async_copy(edge_send, edge_got, local_sems.at[len(local)])

    barrier = pltpu.get_barrier_semaphore()
    pl.semaphore_signal(barrier, inc=1, device_id=to_partner, device_id_type=MESH)

    @pl.when(has_beyond)
    def _():
        pl.semaphore_signal(barrier, inc=1, device_id=to_beyond, device_id_type=MESH)

    for side in range(2):

        @pl.when(has_row[side])
        def _(side=side):
            pl.semaphore_signal(barrier, inc=1, device_id=to_row[side], device_id_type=MESH)
            pl.semaphore_signal(barrier, inc=1, device_id=to_cross[side], device_id_type=MESH)

    for has, target in ((has_far, to_giving), (has_fed, to_fed)):

        @pl.when(has)
        def _(target=target):
            pl.semaphore_signal(barrier, inc=1, device_id=target, device_id_type=MESH)

    for copy in local:
        copy.start()

    lane = lax.broadcasted_iota(I32, (1, slots), 1)
    widths = width_in[...].astype(F32)
    meta_ref[slots, 0] = count_in[0, 0]
    for s in range(slots):
        meta_ref[s, 0] = offset_in[0, s]
        meta_ref[s, 1] = offset_in[1, s]
        meta_ref[s, 2] = jnp.sum(jnp.where(lane == s, widths, 0.0)).astype(I32)
        for k in range(slots_uv):
            for which in range(2):
                meta_ref[s, 3 + 2 * k + which] = bins_in[k, which, s]
        meta_ref[s, 3 + 2 * slots_uv] = used_in[0, s]

    @pl.when(jnp.logical_not(has_beyond))
    def _():
        outer_ref[...] = jnp.zeros_like(outer_ref)
        edge_send[...] = jnp.zeros_like(edge_send)

    with jax.named_scope("barrier"):
        local[0].wait()
        pl.semaphore_wait(
            barrier,
            1 + has_beyond.astype(I32) + 2 * has_up.astype(I32) + 2 * has_down.astype(I32)
            + has_far.astype(I32) + has_fed.astype(I32),
        )

    @pl.when(has_beyond)
    def _():
        for part in range(size // CHUNK):
            sky_beyond(part).start()

    sky_partner().start()
    meta_partner().start()
    for side in range(2):

        @pl.when(has_row[side])
        def _(side=side):
            for copy in meta_send(side):
                copy.start()

    for copy in local[1:]:
        copy.wait()

    acc_outer[...] = jnp.zeros_like(acc_outer)
    acc_inner[...] = jnp.zeros_like(acc_inner)

    per_block = block // FINE

    def table(j, carry):
        blk, at = j // per_block, pl.ds(pl.multiple_of((j % per_block) * FINE, FINE), FINE)
        for tab, half in ((row_tab, row_half), (col_tab, col_half)):
            lanes = pl.ds(half, size)
            c, s = seeds_ref[0, pl.ds(FINE + j, 1), lanes], seeds_ref[1, pl.ds(FINE + j, 1), lanes]
            fc, fs = seeds_ref[0, :FINE, lanes], seeds_ref[1, :FINE, lanes]
            tab[blk, at, :] = (fc * c - fs * s).astype(BF16)
            tab[blk, pl.ds(pl.multiple_of(block + (j % per_block) * FINE, FINE), FINE), :] = (fs * c + fc * s).astype(BF16)
        return carry

    with jax.named_scope("tables"):
        lax.fori_loop(0, length // FINE, table, 0)

    def flipped(j, carry):
        row = (ty % 2) * (size // FINE) + j
        c, s = seeds_ref[0, pl.ds(FINE + row, 1), :], seeds_ref[1, pl.ds(FINE + row, 1), :]
        fc, fs = seeds_ref[0, :FINE, :], seeds_ref[1, :FINE, :]
        at = pl.ds(pl.multiple_of(j * FINE, FINE), FINE)
        cos, sin = (fc * c - fs * s).astype(BF16), (fs * c + fc * s).astype(BF16)
        for blk in range(length // block):
            flip_tab[blk, at, :block] = cos[:, blk * block : (blk + 1) * block]
            flip_tab[blk, at, block:] = sin[:, blk * block : (blk + 1) * block]
        return carry

    with jax.named_scope("flips"):
        lax.fori_loop(0, size // FINE, flipped, 0)

    with jax.named_scope("meta"):
        meta_partner().wait()
        for side in range(2):

            @pl.when(has_row[side])
            def _(side=side):
                for copy in meta_take(side):
                    copy.wait_recv()

            @pl.when(jnp.logical_not(has_row[side]))
            def _(side=side):
                for slot in (1 + side, 3 + side):
                    meta_got[slot][slots, 0] = 0
                    for s in range(slots):
                        for f in range(FIELDS):
                            meta_got[slot][s, f] = 0

    sources = ((meta_got[1], meta_got[3]), (meta_ref, meta_got[0]), (meta_got[2], meta_got[4]))
    even_here = core == 0

    def gather(s, f):
        for d, (same, other) in enumerate(sources):
            a, b = same[s, f], other[s, f]
            meta_all[d, 0, s, f] = jnp.where(even_here, a, b)
            meta_all[d, 1, s, f] = jnp.where(even_here, b, a)

    def gather_slot(s, carry):
        for f in range(FIELDS):
            gather(s, f)
        return carry

    lax.fori_loop(0, slots, gather_slot, 0)
    gather(slots, 0)

    def pointing(d, j):
        even, odd = meta_all[d, 0, slots, 0], meta_all[d, 1, slots, 0]
        from_odd = (j >= even).astype(I32)
        slot = jnp.clip(j - from_odd * even, 0, slots - 1)
        live = j < even + odd
        return from_odd, slot, live

    def bins(d, from_odd, slot, k, which):
        b = meta_all[d, from_odd, slot, 3 + 2 * k + which]
        return jnp.clip(b, 0, length // block - 1)

    def gaussian(shape, axis, shift, decay, live):
        away = lax.broadcasted_iota(I32, shape, axis) + shift
        inside = jnp.logical_and(away >= -size, away < size)
        inside = jnp.logical_and(inside, live)
        away = away.astype(F32)
        if axis == 0:
            fold = away.reshape(shape[0] // 8, 8, shape[1])
            value = jnp.exp(-(fold * fold) * decay[None]).reshape(shape)
        else:
            value = jnp.exp(-(away * away) * wide(decay, shape[1]))
        return jnp.where(inside, value, jnp.zeros(shape, F32))

    def beams(i, carry):
        d, j = i // slots, i % slots
        from_odd, slot, live = pointing(d, j)
        oy, ox = meta_all[d, from_odd, slot, 0], meta_all[d, from_odd, slot, 1]
        width = jnp.full((8, 128), meta_all[d, from_odd, slot, 2], I32).astype(F32)
        decay = 1.0 / (2.0 * width * width)
        gy_ref[d, j] = gaussian((size, 128), 0, (1 - d) * size - oy, decay, live)
        outer_at, inner_at = 3 * core - 1, 1 - core
        gx_ref[d, j, 0] = gaussian((8, size), 1, (outer_at - from_odd) * size - ox, decay, live)
        gx_ref[d, j, 1] = gaussian((8, size), 1, (inner_at - from_odd) * size - ox, decay, live)
        return carry

    with jax.named_scope("beams"):
        lax.fori_loop(0, 3 * slots, beams, 0)

    def column_table(d, from_odd, slot, k):
        return col_tab[bins(d, from_odd, slot, k, 1)]

    def forward(d, j, result_ref, parts, before_ref=None):
        from_odd, slot, live = pointing(d, j)
        rows = jnp.concatenate(
            [row_tab[bins(d, from_odd, slot, k, 0)] for k in range(slots_uv)], axis=0
        )
        gy = wide(gy_ref[d, j], CHUNK)
        for part in parts:
            cols = slice(part * CHUNK, (part + 1) * CHUNK)
            value = gx_ref[d, j, 0, 0:1, cols] * outer_ref[:, cols].astype(F32)
            value = value + gx_ref[d, j, 1, 0:1, cols] * inner_ref[:, cols].astype(F32)
            beamed_ref[:, cols] = (gy * value).astype(BF16)
        for part in parts:
            cols = slice(part * CHUNK, (part + 1) * CHUNK)
            first_ref[:, cols] = jnp.dot(
                rows, beamed_ref[:, cols], preferred_element_type=F32
            ).astype(BF16)
        cols = slice(parts[0] * CHUNK, (parts[-1] + 1) * CHUNK)
        for k in range(slots_uv):
            both = lax.dot_general(
                first_ref[2 * k * block : (2 * k + 2) * block, cols],
                col_tab[bins(d, from_odd, slot, k, 1), :, cols],
                (((1,), (1,)), ((), ())),
                preferred_element_type=F32,
            )
            real = both[:block, :block] - both[block:, block:]
            turned = both[:block, block:] + both[block:, :block]
            if before_ref is not None:
                real, turned = real + before_ref[k, :, :block], turned + before_ref[k, :, block:]
            result_ref[k, :, :block] = real
            result_ref[k, :, block:] = turned

    def adjoint(d, j, scaled_ref):
        from_odd, slot, live = pointing(d, j)
        rows = jnp.concatenate(
            [flip_tab[bins(d, from_odd, slot, k, 0)] for k in range(slots_uv)], axis=1
        )
        gy = wide(gy_ref[d, j], CHUNK)
        for k in range(slots_uv):
            value = scaled_ref[k]
            real, turned = value[:, :block], value[:, block:]
            square = jnp.concatenate(
                [value, jnp.concatenate([turned, -real], axis=1)], axis=0
            )
            spread_ref[2 * k * block : (2 * k + 2) * block, :] = jnp.dot(
                square, column_table(d, from_odd, slot, k), preferred_element_type=F32
            ).astype(BF16)
        for at in range(0, size, CHUNK):
            cols = slice(at, at + CHUNK)
            back = gy * jnp.dot(rows, spread_ref[:, cols], preferred_element_type=F32)
            acc_outer[:, cols] += gx_ref[d, j, 0, 0:1, cols] * back
            acc_inner[:, cols] += gx_ref[d, j, 1, 0:1, cols] * back

    mine, theirs = half_slots * core, half_slots * (1 - core)

    parts = size // CHUNK

    def ahead(g, d):
        def step(j, carry):
            forward(d, j, early.at[g, j], range(parts - 1))
            return carry

        with jax.named_scope(f"ahead{g}"):
            lax.fori_loop(0, slots, step, 0)

    with jax.named_scope("sky0"):
        sky_partner().wait_recv()

        @pl.when(has_beyond)
        def _():
            for part in range(parts - 1):
                sky_beyond(part).wait_recv()

    @pl.when(has_far)
    def _():
        ahead(0, d_far)

    ahead(1, d_mate)

    with jax.named_scope("sky1"):

        @pl.when(has_beyond)
        def _():
            sky_beyond(parts - 1).wait_recv()

    weight_copy().start()

    def complete(g, d, j, result_ref):
        if g == 2:
            forward(d, j, result_ref, range(parts))
        else:
            forward(d, j, result_ref, range(parts - 1, parts), early.at[g, j])

    def give(g, d):
        def step(jj, carry):
            complete(g, d, theirs + jj, part_send.at[g, jj])
            part_copy(g, jj).start()
            return carry

        with jax.named_scope(f"give{g}"):
            lax.fori_loop(0, half_slots, step, 0)

    def take(g, d, after):
        def step(jj, carry):
            complete(g, d, mine + jj, totals.at[g, jj])
            part_copy(g, jj).wait_recv()
            after(jj)
            return carry

        with jax.named_scope(f"take{g}"):
            lax.fori_loop(0, half_slots, step, 0)

    def give_far(jj):
        for k in range(slots_uv):
            raw_send[jj, k] = (totals[0, jj, k] + part_got[0, jj, k]).astype(BF16)
            raw_copy(to_giving, jj, k).start()

    def keep(g):
        def add(jj):
            totals[g, jj] = totals[g, jj] + part_got[g, jj]

        return add

    @pl.when(has_far)
    def _():
        give(0, d_far)
        take(0, d_far, give_far)

    def pass_one(jj, k, fed_too):
        value = totals[1, jj, k]
        if fed_too:
            value = value + raw_got[jj, k].astype(F32)
        sum_send[jj, k] = value.astype(BF16)
        sum_copy(jj, k).start()

    def give_mate(jj):
        totals[1, jj] = totals[1, jj] + part_got[1, jj]

        @pl.when(jnp.logical_not(has_fed))
        def _():
            for k in range(slots_uv):
                pass_one(jj, k, False)

    give(1, d_mate)
    take(1, d_mate, give_mate)
    give(2, 1)
    take(2, 1, keep(2))

    with jax.named_scope("pass_sums"):

        @pl.when(has_fed)
        def _():
            for jj in range(half_slots):
                for k in range(slots_uv):
                    raw_copy(to_fed, jj, k).wait_recv()
                    pass_one(jj, k, True)

    def adjoint_mine(g, d, jj):
        adjoint(d, mine + jj, scaled_own.at[g, jj])

    def adjoint_theirs(g, d):
        def step(jj, carry):
            par_copy(g, jj).wait_recv()
            adjoint(d, theirs + jj, scaled_par.at[g, jj])
            return carry

        with jax.named_scope(f"theirs{g}"):
            lax.fori_loop(0, half_slots, step, 0)

    weight_copy().wait_recv()

    def scale_step(jj, carry):
        from_odd, slot, live = pointing(1, mine + jj)
        used = meta_all[1, from_odd, slot, 3 + 2 * slots_uv]
        here = from_odd == core
        for k in range(slots_uv):
            weight = jnp.where(here, weight_ref[slot, k], weight_got[slot, k]).astype(F32)
            weight = weight * jnp.where(k < used, 1.0, 0.0).astype(F32)
            sum_copy(jj, k).wait_recv()
            total = totals[2, jj, k] + sum_got[jj, k].astype(F32)
            scaled_own[2, jj, k] = (total * wide(weight, 2 * block)).astype(BF16)
            scaled_copy(jj, k).start()
        par_copy(2, jj).start()
        adjoint_mine(2, 1, jj)
        return carry

    with jax.named_scope("scale"):
        lax.fori_loop(0, half_slots, scale_step, 0)

    adjoint_theirs(2, 1)

    def mate_step(jj, carry):
        for k in range(slots_uv):
            scaled_copy(jj, k).wait_recv()

            @pl.when(has_fed)
            def _():
                onward_copy(to_fed, jj, k).start()

        par_copy(1, jj).start()
        adjoint_mine(1, d_mate, jj)
        return carry

    with jax.named_scope("mate"):
        lax.fori_loop(0, half_slots, mate_step, 0)

    adjoint_theirs(1, d_mate)

    def far_step(jj, carry):
        for k in range(slots_uv):
            onward_copy(to_giving, jj, k).wait_recv()
        par_copy(0, jj).start()
        adjoint_mine(0, d_far, jj)
        return carry

    @pl.when(has_far)
    def _():
        with jax.named_scope("far"):
            lax.fori_loop(0, half_slots, far_step, 0)
        adjoint_theirs(0, d_far)

    @pl.when(has_beyond)
    def _():
        edge_send[...] = acc_outer[...].astype(BF16)
        last_edge().start()

    inner_send[...] = acc_inner[...].astype(BF16)
    last_inner().start()

    @pl.when(jnp.logical_not(has_beyond))
    def _():
        no_edge().start()

    sky_partner().wait_send()
    weight_copy().wait_send()

    @pl.when(has_beyond)
    def _():
        for part in range(size // CHUNK):
            sky_beyond(part).wait_send()

    for side in range(2):

        @pl.when(has_row[side])
        def _(side=side):
            for copy in meta_send(side):
                copy.wait_send()

    for jj in range(half_slots):
        for g in (1, 2):
            part_copy(g, jj).wait_send()
            par_copy(g, jj).wait_send()
        for k in range(slots_uv):
            sum_copy(jj, k).wait_send()
            scaled_copy(jj, k).wait_send()

            @pl.when(has_fed)
            def _(jj=jj, k=k):
                onward_copy(to_fed, jj, k).wait_send()

        @pl.when(has_far)
        def _(jj=jj):
            part_copy(0, jj).wait_send()
            par_copy(0, jj).wait_send()
            for k in range(slots_uv):
                raw_copy(to_giving, jj, k).wait_send()

    with jax.named_scope("last"):
        last_inner().wait()

        @pl.when(has_beyond)
        def _():
            last_edge().wait()

        @pl.when(jnp.logical_not(has_beyond))
        def _():
            no_edge().wait()


def add_kernel(inner_hbm, edge_hbm, out_hbm, inner_ref, edge_ref, out_ref, sems):
    band = out_ref.shape[0] // BANDS
    bands = [slice(i * band, (i + 1) * band) for i in range(BANDS)]
    moves = [
        [
            pltpu.make_async_copy(inner_hbm.at[rows], inner_ref.at[rows], sems.at[0, i]),
            pltpu.make_async_copy(edge_hbm.at[rows], edge_ref.at[rows], sems.at[1, i]),
            pltpu.make_async_copy(out_ref.at[rows], out_hbm.at[rows], sems.at[2, i]),
        ]
        for i, rows in enumerate(bands)
    ]
    for inner, edge, out in moves:
        inner.start()
        edge.start()
    for rows, (inner, edge, out) in zip(bands, moves):
        inner.wait()
        edge.wait()
        out_ref[rows, :] = inner_ref[rows, :].astype(F32) + edge_ref[rows, :].astype(F32)
        out.start()
    for inner, edge, out in moves:
        out.wait()


def shards(sky, point_count, point_offset, beam_width, uv_bins, uv_count, uv_weight):
    size = sky.shape[0]
    length = 2 * size
    slots, slots_uv, block = uv_weight.shape[2], uv_weight.shape[3], uv_weight.shape[4]
    half_slots = slots // 2
    depth = 2 * slots_uv * block
    seeds = seed_tables(length, FINE)
    count = point_count.reshape(1, 1)
    offset = jnp.transpose(point_offset, (0, 1, 3, 2)).reshape(2, slots)
    width = beam_width.reshape(1, slots)
    bins = jnp.transpose(uv_bins, (0, 1, 3, 4, 2)).reshape(slots_uv, 2, slots)
    used = uv_count.reshape(1, slots)
    weight = uv_weight.reshape(slots, slots_uv, block, block)

    dma = pltpu.SemaphoreType.DMA
    meta_shape = (slots + 1, FIELDS)
    tile = pltpu.VMEM((size, size), BF16)
    plane = pltpu.VMEM((size, size), F32)
    patch = (slots_uv, block, 2 * block)
    smem, anywhere = pl.BlockSpec(memory_space=pltpu.SMEM), pl.BlockSpec(memory_space=pl.ANY)
    inner, edge = pl.pallas_call(
        kernel,
        out_shape=(jax.ShapeDtypeStruct((size, size), BF16),) * 2,
        in_specs=[smem, smem, pl.BlockSpec(memory_space=pltpu.VMEM), smem, smem] + [anywhere] * 3,
        out_specs=(anywhere, anywhere),
        scratch_shapes=[
            pltpu.SMEM(meta_shape, I32),
            tuple([pltpu.SMEM(meta_shape, I32)] * 5),
            pltpu.SMEM((3, 2) + meta_shape, I32),
            tile,
            tile,
            tile,
            pltpu.VMEM(weight.shape, BF16),
            pltpu.VMEM(weight.shape, BF16),
            pltpu.VMEM(seeds.shape, F32),
            pltpu.VMEM((length // block, 2 * block, size), BF16),
            pltpu.VMEM((length // block, size, 2 * block), BF16),
            pltpu.VMEM((length // block, 2 * block, size), BF16),
            tile,
            pltpu.VMEM((depth, size), BF16),
            pltpu.VMEM((depth, size), BF16),
            pltpu.VMEM((3, slots, 2, 8, size), F32),
            pltpu.VMEM((3, slots, size, 128), F32),
            pltpu.VMEM((2, slots) + patch, F32),
            pltpu.VMEM((3, half_slots) + patch, F32),
            pltpu.VMEM((3, half_slots) + patch, F32),
            pltpu.VMEM((3, half_slots) + patch, F32),
            pltpu.VMEM((half_slots,) + patch, BF16),
            pltpu.VMEM((half_slots,) + patch, BF16),
            pltpu.VMEM((half_slots,) + patch, BF16),
            pltpu.VMEM((half_slots,) + patch, BF16),
            pltpu.VMEM((3, half_slots) + patch, BF16),
            pltpu.VMEM((3, half_slots) + patch, BF16),
            plane,
            plane,
            tile,
            tile,
            dma((4,)),
            dma((2, 5)),
            dma((2, 1 + size // CHUNK)),
            dma((2, 1)),
            dma((2, 3, half_slots)),
            dma((2, half_slots, slots_uv)),
            dma((2, half_slots, slots_uv)),
            dma((2, half_slots, slots_uv)),
            dma((2, half_slots, slots_uv)),
            dma((2, 3, half_slots)),
            dma((2, 2)),
        ],
        compiler_params=pltpu.CompilerParams(
            vmem_limit_bytes=int(56 * 1024 * 1024), collective_id=0, has_side_effects=True
        ),
    )(count, offset, width, bins, used, seeds, sky, weight)
    return pl.pallas_call(
        add_kernel,
        out_shape=jax.ShapeDtypeStruct((size, size), F32),
        in_specs=[anywhere, anywhere],
        out_specs=anywhere,
        scratch_shapes=[tile, tile, plane, dma((3, BANDS))],
        compiler_params=pltpu.CompilerParams(vmem_limit_bytes=56 * 1024 * 1024),
        cost_estimate=pl.CostEstimate(flops=size * size, bytes_accessed=10 * size * size, transcendentals=0),
    )(inner, edge)


def solution(mesh):
    in_specs = (
        P("ty", "tx"),
        P("ty", "tx"),
        P("ty", "tx", None, None),
        P("ty", "tx", None),
        P("ty", "tx", None, None, None),
        P("ty", "tx", None),
        P("ty", "tx", None, None, None, None),
    )
    out_specs = P("ty", "tx")
    return jax.shard_map(shards, mesh=mesh, in_specs=in_specs, out_specs=out_specs, check_vma=False)
```

```python
import functools
import math

import jax
import jax.numpy as jnp
import numpy as np
from jax import lax
from jax.experimental import pallas as pl
from jax.experimental.pallas import tpu as pltpu
from jax.sharding import PartitionSpec as P

F32 = jnp.float32
BF16 = jnp.bfloat16
I32 = jnp.int32
FINE = 32
CHUNK = 256
BANDS = 4
FIELDS = 8
MESH = pl.DeviceIdType.MESH


def seed_tables(length, fine):
    pixels = np.arange(length, dtype=np.int64)
    rows = np.concatenate([np.arange(fine), fine * np.arange(length // fine)])
    angle = (rows[:, None] * pixels[None, :] % length) * (2.0 * math.pi / length)
    scale = np.where(np.arange(rows.shape[0]) < fine, 1.0 / math.sqrt(length), 1.0)[:, None]
    return np.stack([np.cos(angle) * scale, np.sin(angle) * scale]).astype(np.float32)


def wide(column, width):
    return jnp.concatenate([column] * (width // column.shape[1]), axis=1)


def kernel(
    count_in, offset_in, width_in, bins_in, used_in, seeds_in, sky_in, weight_in,
    inner_got, edge_got,
    meta_ref, meta_got, meta_all, sky_ref, outer_ref, inner_ref, weight_ref, weight_got,
    seeds_ref, row_tab, flip_tab, col_tab,
    beamed, first, spread, gx_ref, gy_ref,
    part_send, part_got, totals, raw_send, raw_got, sum_send, sum_got,
    scaled_own, scaled_par, acc_outer, acc_inner, edge_send, inner_send,
    local_sems, meta_sems, sky_sems, weight_sems, part_sems, raw_sems, sum_sems, scaled_sems,
    onward_sems, par_sems, last_sems,
):
    size = sky_ref.shape[0]
    length = 2 * size
    slots, slots_uv, block = weight_ref.shape[0], weight_ref.shape[1], weight_ref.shape[2]
    half_slots = slots // 2
    ty, tx = lax.axis_index("ty"), lax.axis_index("tx")
    ny, nx = lax.axis_size("ty"), lax.axis_size("tx")
    core = tx % 2
    partner = tx + 1 - 2 * core
    beyond = tx - 1 + 2 * core
    has_up, has_down = ty > 0, ty < ny - 1
    has_beyond = jnp.logical_and(beyond >= 0, beyond < nx)
    has_row = (has_up, has_down)
    row_half = pl.multiple_of((ty % 2) * size, size)
    col_half = pl.multiple_of((1 - core) * size, size)
    to_partner = {"tx": partner}
    to_beyond = {"tx": beyond}
    to_row = ({"ty": ty - 1}, {"ty": ty + 1})
    to_cross = ({"ty": ty - 1, "tx": partner}, {"ty": ty + 1, "tx": partner})
    odd_row = ty % 2
    d_far, d_mate = 2 * odd_row, 2 * (1 - odd_row)
    giving, fed = ty - 2 + 4 * odd_row, ty + 2 - 4 * odd_row
    has_far = jnp.logical_and(giving >= 0, giving < ny)
    has_fed = jnp.logical_and(fed >= 0, fed < ny)
    to_mate, to_giving, to_fed = {"ty": ty + 1 - 2 * odd_row}, {"ty": giving}, {"ty": fed}

    local = [
        pltpu.make_async_copy(source, target, local_sems.at[i])
        for i, (source, target) in enumerate(
            (
                (sky_in, sky_ref),
                (seeds_in, seeds_ref),
                (weight_in, weight_ref),
            )
        )
    ]

    def remote(src, dst, sems, at, target):
        return pltpu.make_async_remote_copy(
            src_ref=src,
            dst_ref=dst,
            send_sem=sems.at[(0,) + at],
            recv_sem=sems.at[(1,) + at],
            device_id=target,
            device_id_type=MESH,
        )

    def meta_copy(slot, target):
        return remote(meta_ref, meta_got[slot], meta_sems, (slot,), target)

    def meta_partner():
        return meta_copy(0, to_partner)

    def meta_send(side):
        return meta_copy(2 - side, to_row[side]), meta_copy(4 - side, to_cross[side])

    def meta_take(side):
        return meta_copy(1 + side, to_row[side]), meta_copy(3 + side, to_cross[side])

    def sky_partner():
        return remote(sky_ref, inner_ref, sky_sems, (0,), to_partner)

    def sky_beyond():
        return remote(sky_ref, outer_ref, sky_sems, (1,), to_beyond)

    def weight_copy():
        return remote(weight_ref, weight_got, weight_sems, (0,), to_partner)

    def part_copy(g, jj):
        return remote(part_send.at[g, jj], part_got.at[g, jj], part_sems, (g, jj), to_partner)

    def raw_copy(target, jj, k):
        return remote(raw_send.at[jj, k], raw_got.at[jj, k], raw_sems, (jj, k), target)

    def sum_copy(jj, k):
        return remote(sum_send.at[jj, k], sum_got.at[jj, k], sum_sems, (jj, k), to_mate)

    def scaled_copy(jj, k):
        return remote(
            scaled_own.at[2, jj, k], scaled_own.at[1, jj, k], scaled_sems, (jj, k), to_mate
        )

    def onward_copy(target, jj, k):
        return remote(
            scaled_own.at[1, jj, k], scaled_own.at[0, jj, k], onward_sems, (jj, k), target
        )

    def par_copy(g, jj, k):
        return remote(
            scaled_own.at[g, jj, k], scaled_par.at[g, jj, k], par_sems, (g, jj, k), to_partner
        )

    def last_edge():
        return remote(edge_send, edge_got, last_sems, (0,), to_beyond)

    def last_inner():
        return remote(inner_send, inner_got, last_sems, (1,), to_partner)

    def no_edge():
        return pltpu.make_async_copy(edge_send, edge_got, local_sems.at[len(local)])

    barrier = pltpu.get_barrier_semaphore()
    pl.semaphore_signal(barrier, inc=1, device_id=to_partner, device_id_type=MESH)

    @pl.when(has_beyond)
    def _():
        pl.semaphore_signal(barrier, inc=1, device_id=to_beyond, device_id_type=MESH)

    for side in range(2):

        @pl.when(has_row[side])
        def _(side=side):
            pl.semaphore_signal(barrier, inc=1, device_id=to_row[side], device_id_type=MESH)
            pl.semaphore_signal(barrier, inc=1, device_id=to_cross[side], device_id_type=MESH)

    for has, target in ((has_far, to_giving), (has_fed, to_fed)):

        @pl.when(has)
        def _(target=target):
            pl.semaphore_signal(barrier, inc=1, device_id=target, device_id_type=MESH)

    for copy in local:
        copy.start()

    lane = lax.broadcasted_iota(I32, (1, slots), 1)
    widths = width_in[...].astype(F32)
    meta_ref[slots, 0] = count_in[0, 0]
    for s in range(slots):
        meta_ref[s, 0] = offset_in[0, s]
        meta_ref[s, 1] = offset_in[1, s]
        meta_ref[s, 2] = jnp.sum(jnp.where(lane == s, widths, 0.0)).astype(I32)
        for k in range(slots_uv):
            for which in range(2):
                meta_ref[s, 3 + 2 * k + which] = bins_in[k, which, s]
        meta_ref[s, 3 + 2 * slots_uv] = used_in[0, s]

    @pl.when(jnp.logical_not(has_beyond))
    def _():
        outer_ref[...] = jnp.zeros_like(outer_ref)
        edge_send[...] = jnp.zeros_like(edge_send)

    with jax.named_scope("barrier"):
        local[0].wait()
        pl.semaphore_wait(
            barrier,
            1 + has_beyond.astype(I32) + 2 * has_up.astype(I32) + 2 * has_down.astype(I32)
            + has_far.astype(I32) + has_fed.astype(I32),
        )

    @pl.when(has_beyond)
    def _():
        sky_beyond().start()

    sky_partner().start()
    meta_partner().start()
    for side in range(2):

        @pl.when(has_row[side])
        def _(side=side):
            for copy in meta_send(side):
                copy.start()

    for copy in local[1:]:
        copy.wait()

    acc_outer[...] = jnp.zeros_like(acc_outer)
    acc_inner[...] = jnp.zeros_like(acc_inner)

    per_block = block // FINE

    def table(j, carry):
        blk, at = j // per_block, pl.ds(pl.multiple_of((j % per_block) * FINE, FINE), FINE)
        for tab, half in ((row_tab, row_half), (col_tab, col_half)):
            lanes = pl.ds(half, size)
            c, s = seeds_ref[0, pl.ds(FINE + j, 1), lanes], seeds_ref[1, pl.ds(FINE + j, 1), lanes]
            fc, fs = seeds_ref[0, :FINE, lanes], seeds_ref[1, :FINE, lanes]
            tab[blk, at, :] = (fc * c - fs * s).astype(BF16)
            tab[blk, pl.ds(pl.multiple_of(block + (j % per_block) * FINE, FINE), FINE), :] = (fs * c + fc * s).astype(BF16)
        return carry

    with jax.named_scope("tables"):
        lax.fori_loop(0, length // FINE, table, 0)

    def flipped(j, carry):
        row = (ty % 2) * (size // FINE) + j
        c, s = seeds_ref[0, pl.ds(FINE + row, 1), :], seeds_ref[1, pl.ds(FINE + row, 1), :]
        fc, fs = seeds_ref[0, :FINE, :], seeds_ref[1, :FINE, :]
        at = pl.ds(pl.multiple_of(j * FINE, FINE), FINE)
        cos, sin = (fc * c - fs * s).astype(BF16), (fs * c + fc * s).astype(BF16)
        for blk in range(length // block):
            flip_tab[blk, at, :block] = cos[:, blk * block : (blk + 1) * block]
            flip_tab[blk, at, block:] = sin[:, blk * block : (blk + 1) * block]
        return carry

    with jax.named_scope("flips"):
        lax.fori_loop(0, size // FINE, flipped, 0)

    with jax.named_scope("meta"):
        meta_partner().wait()
        for side in range(2):

            @pl.when(has_row[side])
            def _(side=side):
                for copy in meta_take(side):
                    copy.wait_recv()

            @pl.when(jnp.logical_not(has_row[side]))
            def _(side=side):
                for slot in (1 + side, 3 + side):
                    meta_got[slot][slots, 0] = 0
                    for s in range(slots):
                        for f in range(FIELDS):
                            meta_got[slot][s, f] = 0

    sources = ((meta_got[1], meta_got[3]), (meta_ref, meta_got[0]), (meta_got[2], meta_got[4]))
    even_here = core == 0

    def gather(s, f):
        for d, (same, other) in enumerate(sources):
            a, b = same[s, f], other[s, f]
            meta_all[d, 0, s, f] = jnp.where(even_here, a, b)
            meta_all[d, 1, s, f] = jnp.where(even_here, b, a)

    def gather_slot(s, carry):
        for f in range(FIELDS):
            gather(s, f)
        return carry

    lax.fori_loop(0, slots, gather_slot, 0)
    gather(slots, 0)

    def pointing(d, j):
        even, odd = meta_all[d, 0, slots, 0], meta_all[d, 1, slots, 0]
        from_odd = (j >= even).astype(I32)
        slot = jnp.clip(j - from_odd * even, 0, slots - 1)
        live = j < even + odd
        return from_odd, slot, live

    def bins(d, from_odd, slot, k, which):
        b = meta_all[d, from_odd, slot, 3 + 2 * k + which]
        return jnp.clip(b, 0, length // block - 1)

    def gaussian(shape, axis, shift, decay, live):
        away = lax.broadcasted_iota(I32, shape, axis) + shift
        inside = jnp.logical_and(away >= -size, away < size)
        inside = jnp.logical_and(inside, live)
        away = away.astype(F32)
        if axis == 0:
            fold = away.reshape(shape[0] // 8, 8, shape[1])
            value = jnp.exp(-(fold * fold) * decay[None]).reshape(shape)
        else:
            value = jnp.exp(-(away * away) * wide(decay, shape[1]))
        return jnp.where(inside, value, jnp.zeros(shape, F32))

    def beams(i, carry):
        d, j = i // slots, i % slots
        from_odd, slot, live = pointing(d, j)
        oy, ox = meta_all[d, from_odd, slot, 0], meta_all[d, from_odd, slot, 1]
        width = jnp.full((8, 128), meta_all[d, from_odd, slot, 2], I32).astype(F32)
        decay = 1.0 / (2.0 * width * width)
        gy_ref[d, j] = gaussian((size, 128), 0, (1 - d) * size - oy, decay, live)
        outer_at, inner_at = 3 * core - 1, 1 - core
        gx_ref[d, j, 0] = gaussian((8, size), 1, (outer_at - from_odd) * size - ox, decay, live)
        gx_ref[d, j, 1] = gaussian((8, size), 1, (inner_at - from_odd) * size - ox, decay, live)
        return carry

    with jax.named_scope("beams"):
        lax.fori_loop(0, 3 * slots, beams, 0)

    def column_table(d, from_odd, slot, k):
        return col_tab[bins(d, from_odd, slot, k, 1)]

    def prepare(d, j, beamed_ref):
        gy = wide(gy_ref[d, j], CHUNK)
        for at in range(0, size, CHUNK):
            cols = slice(at, at + CHUNK)
            value = gx_ref[d, j, 0, 0:1, cols] * outer_ref[:, cols].astype(F32)
            value = value + gx_ref[d, j, 1, 0:1, cols] * inner_ref[:, cols].astype(F32)
            beamed_ref[:, cols] = (gy * value).astype(BF16)

    def multiply(d, j, beamed_ref, first_ref, result_ref):
        from_odd, slot, live = pointing(d, j)
        rows = jnp.concatenate(
            [row_tab[bins(d, from_odd, slot, k, 0)] for k in range(slots_uv)], axis=0
        )
        for at in range(0, size, CHUNK):
            cols = slice(at, at + CHUNK)
            first_ref[:, cols] = jnp.dot(
                rows, beamed_ref[:, cols], preferred_element_type=F32
            ).astype(BF16)
        for k in range(slots_uv):
            both = lax.dot_general(
                first_ref[2 * k * block : (2 * k + 2) * block, :],
                col_tab[bins(d, from_odd, slot, k, 1)],
                (((1,), (1,)), ((), ())),
                preferred_element_type=F32,
            )
            real = both[:block, :block] - both[block:, block:]
            turned = both[:block, block:] + both[block:, :block]
            result_ref[k, :, :block] = real.astype(result_ref.dtype)
            result_ref[k, :, block:] = turned.astype(result_ref.dtype)

    def adjoint(d, j, scaled_ref, spread_ref):
        from_odd, slot, live = pointing(d, j)
        rows = jnp.concatenate(
            [flip_tab[bins(d, from_odd, slot, k, 0)] for k in range(slots_uv)], axis=1
        )
        gy = wide(gy_ref[d, j], CHUNK)
        for k in range(slots_uv):
            value = scaled_ref[k]
            real, turned = value[:, :block], value[:, block:]
            square = jnp.concatenate(
                [value, jnp.concatenate([turned, -real], axis=1)], axis=0
            )
            spread_ref[2 * k * block : (2 * k + 2) * block, :] = jnp.dot(
                square, column_table(d, from_odd, slot, k), preferred_element_type=F32
            ).astype(BF16)
        for at in range(0, size, CHUNK):
            cols = slice(at, at + CHUNK)
            back = gy * jnp.dot(rows, spread_ref[:, cols], preferred_element_type=F32)
            acc_outer[:, cols] += gx_ref[d, j, 0, 0:1, cols] * back
            acc_inner[:, cols] += gx_ref[d, j, 1, 0:1, cols] * back

    mine, theirs = half_slots * core, half_slots * (1 - core)

    with jax.named_scope("sky"):
        sky_partner().wait_recv()

        @pl.when(has_beyond)
        def _():
            sky_beyond().wait_recv()

    weight_copy().start()

    def pass_sum(jj, k, value):
        sum_send[jj, k] = value.astype(BF16)
        sum_copy(jj, k).start()

    def row_of(g):
        own = g // 2
        return 2 * (odd_row * (1 - g) + (1 - odd_row) * g) * (1 - own) + own

    order = [(theirs, jj) for jj in range(half_slots)] + [(mine, jj) for jj in range(half_slots)]

    def forward_group(g, carry):
        d, d_next = row_of(g), row_of(g + 1)
        for i, (base, jj) in enumerate(order):
            result = part_send.at[g, jj] if i < half_slots else totals.at[g, jj]
            multiply(d, base + jj, beamed[i % 2], first[i % 2], result)
            if i < half_slots:
                part_copy(g, jj).start()
            if i + 1 < len(order):
                prepare(d, order[i + 1][0] + order[i + 1][1], beamed[(i + 1) % 2])
            else:
                prepare(d_next, theirs, beamed[(i + 1) % 2])
        for jj in range(half_slots):
            part_copy(g, jj).wait_recv()
            for k in range(slots_uv):
                totals[g, jj, k] = totals[g, jj, k] + part_got[g, jj, k].astype(F32)

            @pl.when(g == 0)
            def _(jj=jj):
                for k in range(slots_uv):
                    raw_send[jj, k] = totals[0, jj, k].astype(BF16)
                    raw_copy(to_giving, jj, k).start()

            @pl.when(jnp.logical_and(g == 1, jnp.logical_not(has_fed)))
            def _(jj=jj):
                for k in range(slots_uv):
                    pass_sum(jj, k, totals[1, jj, k])

        return carry

    g_first = 1 - has_far.astype(I32)
    with jax.named_scope("forward"):
        prepare(row_of(g_first), theirs, beamed[0])
        lax.fori_loop(g_first, 3, forward_group, 0)

    with jax.named_scope("pass_sums"):

        @pl.when(has_fed)
        def _():
            for jj in range(half_slots):
                for k in range(slots_uv):
                    raw_copy(to_fed, jj, k).wait_recv()
                    pass_sum(jj, k, totals[1, jj, k] + raw_got[jj, k].astype(F32))

    def adjoint_mine(g, d, jj):
        adjoint(d, mine + jj, scaled_own.at[g, jj], spread[0])

    def adjoint_theirs(g, d):
        with jax.named_scope(f"theirs{g}"):
            for jj in range(half_slots):
                for k in range(slots_uv):
                    par_copy(g, jj, k).wait_recv()
            for jj in range(half_slots):
                adjoint(d, theirs + jj, scaled_par.at[g, jj], spread[jj % 2])

    weight_copy().wait_recv()

    def scale_step(jj, carry):
        from_odd, slot, live = pointing(1, mine + jj)
        used = meta_all[1, from_odd, slot, 3 + 2 * slots_uv]
        here = from_odd == core
        for k in range(slots_uv):
            weight = jnp.where(here, weight_ref[slot, k], weight_got[slot, k]).astype(F32)
            weight = weight * jnp.where(k < used, 1.0, 0.0).astype(F32)
            sum_copy(jj, k).wait_recv()
            total = totals[2, jj, k] + sum_got[jj, k].astype(F32)
            scaled_own[2, jj, k] = (total * wide(weight, 2 * block)).astype(BF16)
            par_copy(2, jj, k).start()
            scaled_copy(jj, k).start()
        adjoint_mine(2, 1, jj)
        return carry

    with jax.named_scope("scale"):
        lax.fori_loop(0, half_slots, scale_step, 0)

    adjoint_theirs(2, 1)

    def mate_step(jj, carry):
        for k in range(slots_uv):
            scaled_copy(jj, k).wait_recv()
            par_copy(1, jj, k).start()

            @pl.when(has_fed)
            def _(k=k):
                onward_copy(to_fed, jj, k).start()

        adjoint_mine(1, d_mate, jj)
        return carry

    with jax.named_scope("mate"):
        lax.fori_loop(0, half_slots, mate_step, 0)

    adjoint_theirs(1, d_mate)

    def far_step(jj, carry):
        for k in range(slots_uv):
            onward_copy(to_giving, jj, k).wait_recv()
            par_copy(0, jj, k).start()
        adjoint_mine(0, d_far, jj)
        return carry

    @pl.when(has_far)
    def _():
        with jax.named_scope("far"):
            lax.fori_loop(0, half_slots, far_step, 0)
        adjoint_theirs(0, d_far)

    @pl.when(has_beyond)
    def _():
        edge_send[...] = acc_outer[...].astype(BF16)
        last_edge().start()

    inner_send[...] = acc_inner[...].astype(BF16)
    last_inner().start()

    @pl.when(jnp.logical_not(has_beyond))
    def _():
        no_edge().start()

    sky_partner().wait_send()
    weight_copy().wait_send()

    @pl.when(has_beyond)
    def _():
        sky_beyond().wait_send()

    for side in range(2):

        @pl.when(has_row[side])
        def _(side=side):
            for copy in meta_send(side):
                copy.wait_send()

    for jj in range(half_slots):
        for g in (1, 2):
            part_copy(g, jj).wait_send()
            for k in range(slots_uv):
                par_copy(g, jj, k).wait_send()
        for k in range(slots_uv):
            sum_copy(jj, k).wait_send()
            scaled_copy(jj, k).wait_send()

            @pl.when(has_fed)
            def _(jj=jj, k=k):
                onward_copy(to_fed, jj, k).wait_send()

        @pl.when(has_far)
        def _(jj=jj):
            part_copy(0, jj).wait_send()
            for k in range(slots_uv):
                par_copy(0, jj, k).wait_send()
                raw_copy(to_giving, jj, k).wait_send()

    with jax.named_scope("last"):
        last_inner().wait()

        @pl.when(has_beyond)
        def _():
            last_edge().wait()

        @pl.when(jnp.logical_not(has_beyond))
        def _():
            no_edge().wait()


def add_kernel(inner_hbm, edge_hbm, out_hbm, inner_ref, edge_ref, out_ref, sems):
    band = out_ref.shape[0] // BANDS
    bands = [slice(i * band, (i + 1) * band) for i in range(BANDS)]
    moves = [
        [
            pltpu.make_async_copy(inner_hbm.at[rows], inner_ref.at[rows], sems.at[0, i]),
            pltpu.make_async_copy(edge_hbm.at[rows], edge_ref.at[rows], sems.at[1, i]),
            pltpu.make_async_copy(out_ref.at[rows], out_hbm.at[rows], sems.at[2, i]),
        ]
        for i, rows in enumerate(bands)
    ]
    for inner, edge, out in moves:
        inner.start()
        edge.start()
    for rows, (inner, edge, out) in zip(bands, moves):
        inner.wait()
        edge.wait()
        out_ref[rows, :] = inner_ref[rows, :].astype(F32) + edge_ref[rows, :].astype(F32)
        out.start()
    for inner, edge, out in moves:
        out.wait()


def shards(sky, point_count, point_offset, beam_width, uv_bins, uv_count, uv_weight):
    size = sky.shape[0]
    length = 2 * size
    slots, slots_uv, block = uv_weight.shape[2], uv_weight.shape[3], uv_weight.shape[4]
    half_slots = slots // 2
    depth = 2 * slots_uv * block
    seeds = seed_tables(length, FINE)
    count = point_count.reshape(1, 1)
    offset = jnp.transpose(point_offset, (0, 1, 3, 2)).reshape(2, slots)
    width = beam_width.reshape(1, slots)
    bins = jnp.transpose(uv_bins, (0, 1, 3, 4, 2)).reshape(slots_uv, 2, slots)
    used = uv_count.reshape(1, slots)
    weight = uv_weight.reshape(slots, slots_uv, block, block)

    dma = pltpu.SemaphoreType.DMA
    meta_shape = (slots + 1, FIELDS)
    tile = pltpu.VMEM((size, size), BF16)
    plane = pltpu.VMEM((size, size), F32)
    patch = (slots_uv, block, 2 * block)
    smem, anywhere = pl.BlockSpec(memory_space=pltpu.SMEM), pl.BlockSpec(memory_space=pl.ANY)
    inner, edge = pl.pallas_call(
        kernel,
        out_shape=(jax.ShapeDtypeStruct((size, size), BF16),) * 2,
        in_specs=[smem, smem, pl.BlockSpec(memory_space=pltpu.VMEM), smem, smem] + [anywhere] * 3,
        out_specs=(anywhere, anywhere),
        scratch_shapes=[
            pltpu.SMEM(meta_shape, I32),
            tuple([pltpu.SMEM(meta_shape, I32)] * 5),
            pltpu.SMEM((3, 2) + meta_shape, I32),
            tile,
            tile,
            tile,
            pltpu.VMEM(weight.shape, BF16),
            pltpu.VMEM(weight.shape, BF16),
            pltpu.VMEM(seeds.shape, F32),
            pltpu.VMEM((length // block, 2 * block, size), BF16),
            pltpu.VMEM((length // block, size, 2 * block), BF16),
            pltpu.VMEM((length // block, 2 * block, size), BF16),
            (tile, tile),
            (pltpu.VMEM((depth, size), BF16),) * 2,
            (pltpu.VMEM((depth, size), BF16),) * 2,
            pltpu.VMEM((3, slots, 2, 8, size), F32),
            pltpu.VMEM((3, slots, size, 128), F32),
            pltpu.VMEM((3, half_slots) + patch, BF16),
            pltpu.VMEM((3, half_slots) + patch, BF16),
            pltpu.VMEM((3, half_slots) + patch, F32),
            pltpu.VMEM((half_slots,) + patch, BF16),
            pltpu.VMEM((half_slots,) + patch, BF16),
            pltpu.VMEM((half_slots,) + patch, BF16),
            pltpu.VMEM((half_slots,) + patch, BF16),
            pltpu.VMEM((3, half_slots) + patch, BF16),
            pltpu.VMEM((3, half_slots) + patch, BF16),
            plane,
            plane,
            tile,
            tile,
            dma((4,)),
            dma((2, 5)),
            dma((2, 2)),
            dma((2, 1)),
            dma((2, 3, half_slots)),
            dma((2, half_slots, slots_uv)),
            dma((2, half_slots, slots_uv)),
            dma((2, half_slots, slots_uv)),
            dma((2, half_slots, slots_uv)),
            dma((2, 3, half_slots, slots_uv)),
            dma((2, 2)),
        ],
        compiler_params=pltpu.CompilerParams(
            vmem_limit_bytes=int(56 * 1024 * 1024), collective_id=0, has_side_effects=True
        ),
    )(count, offset, width, bins, used, seeds, sky, weight)
    return pl.pallas_call(
        add_kernel,
        out_shape=jax.ShapeDtypeStruct((size, size), F32),
        in_specs=[anywhere, anywhere],
        out_specs=anywhere,
        scratch_shapes=[tile, tile, plane, dma((3, BANDS))],
        compiler_params=pltpu.CompilerParams(vmem_limit_bytes=56 * 1024 * 1024),
        cost_estimate=pl.CostEstimate(flops=size * size, bytes_accessed=10 * size * size, transcendentals=0),
    )(inner, edge)


def solution(mesh):
    in_specs = (
        P("ty", "tx"),
        P("ty", "tx"),
        P("ty", "tx", None, None),
        P("ty", "tx", None),
        P("ty", "tx", None, None, None),
        P("ty", "tx", None),
        P("ty", "tx", None, None, None, None),
    )
    out_specs = P("ty", "tx")
    return jax.shard_map(shards, mesh=mesh, in_specs=in_specs, out_specs=out_specs, check_vma=False)
```

```python
import functools
import math

import jax
import jax.numpy as jnp
import numpy as np
from jax import lax
from jax.experimental import pallas as pl
from jax.experimental.pallas import tpu as pltpu
from jax.sharding import PartitionSpec as P

F32 = jnp.float32
BF16 = jnp.bfloat16
I32 = jnp.int32
FINE = 32
CHUNK = 256
BANDS = 4
FIELDS = 8
MESH = pl.DeviceIdType.MESH


def seed_tables(length, fine):
    pixels = np.arange(length, dtype=np.int64)
    rows = np.concatenate([np.arange(fine), fine * np.arange(length // fine)])
    angle = (rows[:, None] * pixels[None, :] % length) * (2.0 * math.pi / length)
    scale = np.where(np.arange(rows.shape[0]) < fine, 1.0 / math.sqrt(length), 1.0)[:, None]
    return np.stack([np.cos(angle) * scale, np.sin(angle) * scale]).astype(np.float32)


def wide(column, width):
    return jnp.concatenate([column] * (width // column.shape[1]), axis=1)


def kernel(
    count_in, offset_in, width_in, bins_in, used_in, seeds_in, sky_in, weight_in,
    inner_got, edge_got,
    meta_ref, meta_got, meta_all, sky_ref, outer_ref, inner_ref, weight_ref, weight_got,
    seeds_ref, row_tab, flip_tab, col_tab,
    beamed, first, spread, gx_ref, gy_ref,
    part_send, part_got, totals, raw_send, raw_got, sum_send, sum_got,
    scaled_own, scaled_par, acc_outer, acc_inner, edge_send, inner_send,
    local_sems, meta_sems, sky_sems, weight_sems, part_sems, raw_sems, sum_sems, scaled_sems,
    onward_sems, par_sems, last_sems,
):
    size = sky_ref.shape[0]
    length = 2 * size
    slots, slots_uv, block = weight_ref.shape[0], weight_ref.shape[1], weight_ref.shape[2]
    half_slots = slots // 2
    ty, tx = lax.axis_index("ty"), lax.axis_index("tx")
    ny, nx = lax.axis_size("ty"), lax.axis_size("tx")
    core = tx % 2
    partner = tx + 1 - 2 * core
    beyond = tx - 1 + 2 * core
    has_up, has_down = ty > 0, ty < ny - 1
    has_beyond = jnp.logical_and(beyond >= 0, beyond < nx)
    has_row = (has_up, has_down)
    row_half = pl.multiple_of((ty % 2) * size, size)
    col_half = pl.multiple_of((1 - core) * size, size)
    to_partner = {"tx": partner}
    to_beyond = {"tx": beyond}
    to_row = ({"ty": ty - 1}, {"ty": ty + 1})
    to_cross = ({"ty": ty - 1, "tx": partner}, {"ty": ty + 1, "tx": partner})
    odd_row = ty % 2
    d_far, d_mate = 2 * odd_row, 2 * (1 - odd_row)
    giving, fed = ty - 2 + 4 * odd_row, ty + 2 - 4 * odd_row
    has_far = jnp.logical_and(giving >= 0, giving < ny)
    has_fed = jnp.logical_and(fed >= 0, fed < ny)
    to_mate, to_giving, to_fed = {"ty": ty + 1 - 2 * odd_row}, {"ty": giving}, {"ty": fed}

    local = [
        pltpu.make_async_copy(source, target, local_sems.at[i])
        for i, (source, target) in enumerate(
            (
                (sky_in, sky_ref),
                (seeds_in, seeds_ref),
                (weight_in, weight_ref),
            )
        )
    ]

    def remote(src, dst, sems, at, target):
        return pltpu.make_async_remote_copy(
            src_ref=src,
            dst_ref=dst,
            send_sem=sems.at[(0,) + at],
            recv_sem=sems.at[(1,) + at],
            device_id=target,
            device_id_type=MESH,
        )

    def meta_copy(slot, target):
        return remote(meta_ref, meta_got[slot], meta_sems, (slot,), target)

    def meta_partner():
        return meta_copy(0, to_partner)

    def meta_send(side):
        return meta_copy(2 - side, to_row[side]), meta_copy(4 - side, to_cross[side])

    def meta_take(side):
        return meta_copy(1 + side, to_row[side]), meta_copy(3 + side, to_cross[side])

    def sky_partner():
        return remote(sky_ref, inner_ref, sky_sems, (0,), to_partner)

    def sky_beyond():
        return remote(sky_ref, outer_ref, sky_sems, (1,), to_beyond)

    def weight_copy():
        return remote(weight_ref, weight_got, weight_sems, (0,), to_partner)

    def part_copy(g, jj):
        return remote(part_send.at[g, jj], part_got.at[g, jj], part_sems, (g, jj), to_partner)

    def raw_copy(target, jj, k):
        return remote(raw_send.at[jj, k], raw_got.at[jj, k], raw_sems, (jj, k), target)

    def sum_copy(jj, k):
        return remote(sum_send.at[jj, k], sum_got.at[jj, k], sum_sems, (jj, k), to_mate)

    def scaled_copy(jj, k):
        return remote(
            scaled_own.at[2, jj, k], scaled_own.at[1, jj, k], scaled_sems, (jj, k), to_mate
        )

    def onward_copy(target, jj, k):
        return remote(
            scaled_own.at[1, jj, k], scaled_own.at[0, jj, k], onward_sems, (jj, k), target
        )

    def par_copy(g, jj, k):
        return remote(
            scaled_own.at[g, jj, k], scaled_par.at[g, jj, k], par_sems, (g, jj, k), to_partner
        )

    def last_edge():
        return remote(edge_send, edge_got, last_sems, (0,), to_beyond)

    def last_inner():
        return remote(inner_send, inner_got, last_sems, (1,), to_partner)

    def no_edge():
        return pltpu.make_async_copy(edge_send, edge_got, local_sems.at[len(local)])

    barrier = pltpu.get_barrier_semaphore()
    pl.semaphore_signal(barrier, inc=1, device_id=to_partner, device_id_type=MESH)

    @pl.when(has_beyond)
    def _():
        pl.semaphore_signal(barrier, inc=1, device_id=to_beyond, device_id_type=MESH)

    for side in range(2):

        @pl.when(has_row[side])
        def _(side=side):
            pl.semaphore_signal(barrier, inc=1, device_id=to_row[side], device_id_type=MESH)
            pl.semaphore_signal(barrier, inc=1, device_id=to_cross[side], device_id_type=MESH)

    for has, target in ((has_far, to_giving), (has_fed, to_fed)):

        @pl.when(has)
        def _(target=target):
            pl.semaphore_signal(barrier, inc=1, device_id=target, device_id_type=MESH)

    for copy in local:
        copy.start()

    lane = lax.broadcasted_iota(I32, (1, slots), 1)
    widths = width_in[...].astype(F32)
    meta_ref[slots, 0] = count_in[0, 0]
    for s in range(slots):
        meta_ref[s, 0] = offset_in[0, s]
        meta_ref[s, 1] = offset_in[1, s]
        meta_ref[s, 2] = jnp.sum(jnp.where(lane == s, widths, 0.0)).astype(I32)
        for k in range(slots_uv):
            for which in range(2):
                meta_ref[s, 3 + 2 * k + which] = bins_in[k, which, s]
        meta_ref[s, 3 + 2 * slots_uv] = used_in[0, s]

    @pl.when(jnp.logical_not(has_beyond))
    def _():
        outer_ref[...] = jnp.zeros_like(outer_ref)
        edge_send[...] = jnp.zeros_like(edge_send)

    with jax.named_scope("barrier"):
        local[0].wait()
        pl.semaphore_wait(
            barrier,
            1 + has_beyond.astype(I32) + 2 * has_up.astype(I32) + 2 * has_down.astype(I32)
            + has_far.astype(I32) + has_fed.astype(I32),
        )

    @pl.when(has_beyond)
    def _():
        sky_beyond().start()

    sky_partner().start()
    meta_partner().start()
    for side in range(2):

        @pl.when(has_row[side])
        def _(side=side):
            for copy in meta_send(side):
                copy.start()

    for copy in local[1:]:
        copy.wait()

    acc_outer[...] = jnp.zeros_like(acc_outer)
    acc_inner[...] = jnp.zeros_like(acc_inner)

    per_block = block // FINE

    def table(j, carry):
        blk, at = j // per_block, pl.ds(pl.multiple_of((j % per_block) * FINE, FINE), FINE)
        for tab, half in ((row_tab, row_half), (col_tab, col_half)):
            lanes = pl.ds(half, size)
            c, s = seeds_ref[0, pl.ds(FINE + j, 1), lanes], seeds_ref[1, pl.ds(FINE + j, 1), lanes]
            fc, fs = seeds_ref[0, :FINE, lanes], seeds_ref[1, :FINE, lanes]
            tab[blk, at, :] = (fc * c - fs * s).astype(BF16)
            tab[blk, pl.ds(pl.multiple_of(block + (j % per_block) * FINE, FINE), FINE), :] = (fs * c + fc * s).astype(BF16)
        return carry

    with jax.named_scope("tables"):
        lax.fori_loop(0, length // FINE, table, 0)

    def flipped(j, carry):
        row = (ty % 2) * (size // FINE) + j
        c, s = seeds_ref[0, pl.ds(FINE + row, 1), :], seeds_ref[1, pl.ds(FINE + row, 1), :]
        fc, fs = seeds_ref[0, :FINE, :], seeds_ref[1, :FINE, :]
        at = pl.ds(pl.multiple_of(j * FINE, FINE), FINE)
        cos, sin = (fc * c - fs * s).astype(BF16), (fs * c + fc * s).astype(BF16)
        for blk in range(length // block):
            flip_tab[blk, at, :block] = cos[:, blk * block : (blk + 1) * block]
            flip_tab[blk, at, block:] = sin[:, blk * block : (blk + 1) * block]
        return carry

    with jax.named_scope("flips"):
        lax.fori_loop(0, size // FINE, flipped, 0)

    with jax.named_scope("meta"):
        meta_partner().wait()
        for side in range(2):

            @pl.when(has_row[side])
            def _(side=side):
                for copy in meta_take(side):
                    copy.wait_recv()

            @pl.when(jnp.logical_not(has_row[side]))
            def _(side=side):
                for slot in (1 + side, 3 + side):
                    meta_got[slot][slots, 0] = 0
                    for s in range(slots):
                        for f in range(FIELDS):
                            meta_got[slot][s, f] = 0

    sources = ((meta_got[1], meta_got[3]), (meta_ref, meta_got[0]), (meta_got[2], meta_got[4]))
    even_here = core == 0

    def gather(s, f):
        for d, (same, other) in enumerate(sources):
            a, b = same[s, f], other[s, f]
            meta_all[d, 0, s, f] = jnp.where(even_here, a, b)
            meta_all[d, 1, s, f] = jnp.where(even_here, b, a)

    def gather_slot(s, carry):
        for f in range(FIELDS):
            gather(s, f)
        return carry

    lax.fori_loop(0, slots, gather_slot, 0)
    gather(slots, 0)

    def pointing(d, j):
        even, odd = meta_all[d, 0, slots, 0], meta_all[d, 1, slots, 0]
        from_odd = (j >= even).astype(I32)
        slot = jnp.clip(j - from_odd * even, 0, slots - 1)
        live = j < even + odd
        return from_odd, slot, live

    def bins(d, from_odd, slot, k, which):
        b = meta_all[d, from_odd, slot, 3 + 2 * k + which]
        return jnp.clip(b, 0, length // block - 1)

    def gaussian(shape, axis, shift, decay, live):
        away = lax.broadcasted_iota(I32, shape, axis) + shift
        inside = jnp.logical_and(away >= -size, away < size)
        inside = jnp.logical_and(inside, live)
        away = away.astype(F32)
        if axis == 0:
            fold = away.reshape(shape[0] // 8, 8, shape[1])
            value = jnp.exp(-(fold * fold) * decay[None]).reshape(shape)
        else:
            value = jnp.exp(-(away * away) * wide(decay, shape[1]))
        return jnp.where(inside, value, jnp.zeros(shape, F32))

    def beams(i, carry):
        d, j = i // slots, i % slots
        from_odd, slot, live = pointing(d, j)
        oy, ox = meta_all[d, from_odd, slot, 0], meta_all[d, from_odd, slot, 1]
        width = jnp.full((8, 128), meta_all[d, from_odd, slot, 2], I32).astype(F32)
        decay = 1.0 / (2.0 * width * width)
        gy_ref[d, j] = gaussian((size, 128), 0, (1 - d) * size - oy, decay, live)
        outer_at, inner_at = 3 * core - 1, 1 - core
        gx_ref[d, j, 0] = gaussian((8, size), 1, (outer_at - from_odd) * size - ox, decay, live)
        gx_ref[d, j, 1] = gaussian((8, size), 1, (inner_at - from_odd) * size - ox, decay, live)
        return carry

    with jax.named_scope("beams"):
        lax.fori_loop(0, 3 * slots, beams, 0)

    def column_table(d, from_odd, slot, k):
        return col_tab[bins(d, from_odd, slot, k, 1)]

    def prepare(d, j, beamed_ref):
        gy = wide(gy_ref[d, j], CHUNK)
        for at in range(0, size, CHUNK):
            cols = slice(at, at + CHUNK)
            value = gx_ref[d, j, 0, 0:1, cols] * outer_ref[:, cols].astype(F32)
            value = value + gx_ref[d, j, 1, 0:1, cols] * inner_ref[:, cols].astype(F32)
            beamed_ref[:, cols] = (gy * value).astype(BF16)

    def multiply(d, j, beamed_ref, first_ref, result_ref):
        from_odd, slot, live = pointing(d, j)
        rows = jnp.concatenate(
            [row_tab[bins(d, from_odd, slot, k, 0)] for k in range(slots_uv)], axis=0
        )
        for at in range(0, size, CHUNK):
            cols = slice(at, at + CHUNK)
            first_ref[:, cols] = jnp.dot(
                rows, beamed_ref[:, cols], preferred_element_type=F32
            ).astype(BF16)
        for k in range(slots_uv):
            both = lax.dot_general(
                first_ref[2 * k * block : (2 * k + 2) * block, :],
                col_tab[bins(d, from_odd, slot, k, 1)],
                (((1,), (1,)), ((), ())),
                preferred_element_type=F32,
            )
            real = both[:block, :block] - both[block:, block:]
            turned = both[:block, block:] + both[block:, :block]
            result_ref[k, :, :block] = real.astype(result_ref.dtype)
            result_ref[k, :, block:] = turned.astype(result_ref.dtype)

    def adjoint(d, j, scaled_ref, spread_ref):
        from_odd, slot, live = pointing(d, j)
        rows = jnp.concatenate(
            [flip_tab[bins(d, from_odd, slot, k, 0)] for k in range(slots_uv)], axis=1
        )
        gy = wide(gy_ref[d, j], CHUNK)
        for k in range(slots_uv):
            value = scaled_ref[k]
            real, turned = value[:, :block], value[:, block:]
            square = jnp.concatenate(
                [value, jnp.concatenate([turned, -real], axis=1)], axis=0
            )
            spread_ref[2 * k * block : (2 * k + 2) * block, :] = jnp.dot(
                square, column_table(d, from_odd, slot, k), preferred_element_type=F32
            ).astype(BF16)
        for at in range(0, size, CHUNK):
            cols = slice(at, at + CHUNK)
            back = gy * jnp.dot(rows, spread_ref[:, cols], preferred_element_type=F32)
            acc_outer[:, cols] += gx_ref[d, j, 0, 0:1, cols] * back
            acc_inner[:, cols] += gx_ref[d, j, 1, 0:1, cols] * back

    mine, theirs = half_slots * core, half_slots * (1 - core)

    with jax.named_scope("sky"):
        sky_partner().wait_recv()

        @pl.when(has_beyond)
        def _():
            sky_beyond().wait_recv()

    weight_copy().start()

    def pass_sum(jj, k, value):
        sum_send[jj, k] = value.astype(BF16)
        sum_copy(jj, k).start()

    def row_of(g):
        own = g // 2
        return 2 * (odd_row * (1 - g) + (1 - odd_row) * g) * (1 - own) + own

    def settle(g, jj):
        part_copy(g, jj).wait_recv()
        for k in range(slots_uv):
            totals[g, jj, k] = totals[g, jj, k] + part_got[g, jj, k].astype(F32)

        @pl.when(g == 0)
        def _():
            for k in range(slots_uv):
                raw_send[jj, k] = totals[0, jj, k].astype(BF16)
                raw_copy(to_giving, jj, k).start()

        @pl.when(jnp.logical_and(g == 1, jnp.logical_not(has_fed)))
        def _():
            for k in range(slots_uv):
                pass_sum(jj, k, totals[1, jj, k])

    far = has_far.astype(I32)

    def forward_units(s, carry):
        own = s // half_slots
        units = (
            (2 * own + (1 - own) * (1 - far), (1 - own) * far * s),
            (2 * own + (1 - own), own + (1 - own) * (far * s + 1 - far)),
        )
        for i, (g, jj) in enumerate(units):
            prepare(row_of(g), theirs + jj, beamed[i])
            multiply(row_of(g), theirs + jj, beamed[i], first[i], part_send.at[g, jj])
            part_copy(g, jj).start()
        for i, (g, jj) in enumerate(units):
            prepare(row_of(g), mine + jj, beamed[i])
            multiply(row_of(g), mine + jj, beamed[i], first[i], totals.at[g, jj])
            settle(g, jj)
        return carry

    with jax.named_scope("forward"):
        lax.fori_loop(1 - far, half_slots + 1, forward_units, 0)

    with jax.named_scope("pass_sums"):

        @pl.when(has_fed)
        def _():
            for jj in range(half_slots):
                for k in range(slots_uv):
                    raw_copy(to_fed, jj, k).wait_recv()
                    pass_sum(jj, k, totals[1, jj, k] + raw_got[jj, k].astype(F32))

    def adjoint_mine(g, d, jj):
        adjoint(d, mine + jj, scaled_own.at[g, jj], spread[0])

    def adjoint_theirs(g, d):
        with jax.named_scope(f"theirs{g}"):
            for jj in range(half_slots):
                for k in range(slots_uv):
                    par_copy(g, jj, k).wait_recv()
            for jj in range(half_slots):
                adjoint(d, theirs + jj, scaled_par.at[g, jj], spread[jj % 2])

    weight_copy().wait_recv()

    def scale_step(jj, carry):
        from_odd, slot, live = pointing(1, mine + jj)
        used = meta_all[1, from_odd, slot, 3 + 2 * slots_uv]
        here = from_odd == core
        for k in range(slots_uv):
            weight = jnp.where(here, weight_ref[slot, k], weight_got[slot, k]).astype(F32)
            weight = weight * jnp.where(k < used, 1.0, 0.0).astype(F32)
            sum_copy(jj, k).wait_recv()
            total = totals[2, jj, k] + sum_got[jj, k].astype(F32)
            scaled_own[2, jj, k] = (total * wide(weight, 2 * block)).astype(BF16)
            par_copy(2, jj, k).start()
            scaled_copy(jj, k).start()
        adjoint_mine(2, 1, jj)
        return carry

    with jax.named_scope("scale"):
        lax.fori_loop(0, half_slots, scale_step, 0)

    adjoint_theirs(2, 1)

    def mate_step(jj, carry):
        for k in range(slots_uv):
            scaled_copy(jj, k).wait_recv()
            par_copy(1, jj, k).start()

            @pl.when(has_fed)
            def _(k=k):
                onward_copy(to_fed, jj, k).start()

        adjoint_mine(1, d_mate, jj)
        return carry

    with jax.named_scope("mate"):
        lax.fori_loop(0, half_slots, mate_step, 0)

    adjoint_theirs(1, d_mate)

    def far_step(jj, carry):
        for k in range(slots_uv):
            onward_copy(to_giving, jj, k).wait_recv()
            par_copy(0, jj, k).start()
        adjoint_mine(0, d_far, jj)
        return carry

    @pl.when(has_far)
    def _():
        with jax.named_scope("far"):
            lax.fori_loop(0, half_slots, far_step, 0)
        adjoint_theirs(0, d_far)

    @pl.when(has_beyond)
    def _():
        edge_send[...] = acc_outer[...].astype(BF16)
        last_edge().start()

    inner_send[...] = acc_inner[...].astype(BF16)
    last_inner().start()

    @pl.when(jnp.logical_not(has_beyond))
    def _():
        no_edge().start()

    sky_partner().wait_send()
    weight_copy().wait_send()

    @pl.when(has_beyond)
    def _():
        sky_beyond().wait_send()

    for side in range(2):

        @pl.when(has_row[side])
        def _(side=side):
            for copy in meta_send(side):
                copy.wait_send()

    for jj in range(half_slots):
        for g in (1, 2):
            part_copy(g, jj).wait_send()
            for k in range(slots_uv):
                par_copy(g, jj, k).wait_send()
        for k in range(slots_uv):
            sum_copy(jj, k).wait_send()
            scaled_copy(jj, k).wait_send()

            @pl.when(has_fed)
            def _(jj=jj, k=k):
                onward_copy(to_fed, jj, k).wait_send()

        @pl.when(has_far)
        def _(jj=jj):
            part_copy(0, jj).wait_send()
            for k in range(slots_uv):
                par_copy(0, jj, k).wait_send()
                raw_copy(to_giving, jj, k).wait_send()

    with jax.named_scope("last"):
        last_inner().wait()

        @pl.when(has_beyond)
        def _():
            last_edge().wait()

        @pl.when(jnp.logical_not(has_beyond))
        def _():
            no_edge().wait()


def add_kernel(inner_hbm, edge_hbm, out_hbm, inner_ref, edge_ref, out_ref, sems):
    band = out_ref.shape[0] // BANDS
    bands = [slice(i * band, (i + 1) * band) for i in range(BANDS)]
    moves = [
        [
            pltpu.make_async_copy(inner_hbm.at[rows], inner_ref.at[rows], sems.at[0, i]),
            pltpu.make_async_copy(edge_hbm.at[rows], edge_ref.at[rows], sems.at[1, i]),
            pltpu.make_async_copy(out_ref.at[rows], out_hbm.at[rows], sems.at[2, i]),
        ]
        for i, rows in enumerate(bands)
    ]
    for inner, edge, out in moves:
        inner.start()
        edge.start()
    for rows, (inner, edge, out) in zip(bands, moves):
        inner.wait()
        edge.wait()
        out_ref[rows, :] = inner_ref[rows, :].astype(F32) + edge_ref[rows, :].astype(F32)
        out.start()
    for inner, edge, out in moves:
        out.wait()


def shards(sky, point_count, point_offset, beam_width, uv_bins, uv_count, uv_weight):
    size = sky.shape[0]
    length = 2 * size
    slots, slots_uv, block = uv_weight.shape[2], uv_weight.shape[3], uv_weight.shape[4]
    half_slots = slots // 2
    depth = 2 * slots_uv * block
    seeds = seed_tables(length, FINE)
    count = point_count.reshape(1, 1)
    offset = jnp.transpose(point_offset, (0, 1, 3, 2)).reshape(2, slots)
    width = beam_width.reshape(1, slots)
    bins = jnp.transpose(uv_bins, (0, 1, 3, 4, 2)).reshape(slots_uv, 2, slots)
    used = uv_count.reshape(1, slots)
    weight = uv_weight.reshape(slots, slots_uv, block, block)

    dma = pltpu.SemaphoreType.DMA
    meta_shape = (slots + 1, FIELDS)
    tile = pltpu.VMEM((size, size), BF16)
    plane = pltpu.VMEM((size, size), F32)
    patch = (slots_uv, block, 2 * block)
    smem, anywhere = pl.BlockSpec(memory_space=pltpu.SMEM), pl.BlockSpec(memory_space=pl.ANY)
    inner, edge = pl.pallas_call(
        kernel,
        out_shape=(jax.ShapeDtypeStruct((size, size), BF16),) * 2,
        in_specs=[smem, smem, pl.BlockSpec(memory_space=pltpu.VMEM), smem, smem] + [anywhere] * 3,
        out_specs=(anywhere, anywhere),
        scratch_shapes=[
            pltpu.SMEM(meta_shape, I32),
            tuple([pltpu.SMEM(meta_shape, I32)] * 5),
            pltpu.SMEM((3, 2) + meta_shape, I32),
            tile,
            tile,
            tile,
            pltpu.VMEM(weight.shape, BF16),
            pltpu.VMEM(weight.shape, BF16),
            pltpu.VMEM(seeds.shape, F32),
            pltpu.VMEM((length // block, 2 * block, size), BF16),
            pltpu.VMEM((length // block, size, 2 * block), BF16),
            pltpu.VMEM((length // block, 2 * block, size), BF16),
            (tile, tile),
            (pltpu.VMEM((depth, size), BF16),) * 2,
            (pltpu.VMEM((depth, size), BF16),) * 2,
            pltpu.VMEM((3, slots, 2, 8, size), F32),
            pltpu.VMEM((3, slots, size, 128), F32),
            pltpu.VMEM((3, half_slots) + patch, BF16),
            pltpu.VMEM((3, half_slots) + patch, BF16),
            pltpu.VMEM((3, half_slots) + patch, F32),
            pltpu.VMEM((half_slots,) + patch, BF16),
            pltpu.VMEM((half_slots,) + patch, BF16),
            pltpu.VMEM((half_slots,) + patch, BF16),
            pltpu.VMEM((half_slots,) + patch, BF16),
            pltpu.VMEM((3, half_slots) + patch, BF16),
            pltpu.VMEM((3, half_slots) + patch, BF16),
            plane,
            plane,
            tile,
            tile,
            dma((4,)),
            dma((2, 5)),
            dma((2, 2)),
            dma((2, 1)),
            dma((2, 3, half_slots)),
            dma((2, half_slots, slots_uv)),
            dma((2, half_slots, slots_uv)),
            dma((2, half_slots, slots_uv)),
            dma((2, half_slots, slots_uv)),
            dma((2, 3, half_slots, slots_uv)),
            dma((2, 2)),
        ],
        compiler_params=pltpu.CompilerParams(
            vmem_limit_bytes=int(56 * 1024 * 1024), collective_id=0, has_side_effects=True
        ),
    )(count, offset, width, bins, used, seeds, sky, weight)
    return pl.pallas_call(
        add_kernel,
        out_shape=jax.ShapeDtypeStruct((size, size), F32),
        in_specs=[anywhere, anywhere],
        out_specs=anywhere,
        scratch_shapes=[tile, tile, plane, dma((3, BANDS))],
        compiler_params=pltpu.CompilerParams(vmem_limit_bytes=56 * 1024 * 1024),
        cost_estimate=pl.CostEstimate(flops=size * size, bytes_accessed=10 * size * size, transcendentals=0),
    )(inner, edge)


def solution(mesh):
    in_specs = (
        P("ty", "tx"),
        P("ty", "tx"),
        P("ty", "tx", None, None),
        P("ty", "tx", None),
        P("ty", "tx", None, None, None),
        P("ty", "tx", None),
        P("ty", "tx", None, None, None, None),
    )
    out_specs = P("ty", "tx")
    return jax.shard_map(shards, mesh=mesh, in_specs=in_specs, out_specs=out_specs, check_vma=False)
```

```python
import functools
import math

import jax
import jax.numpy as jnp
import numpy as np
from jax import lax
from jax.experimental import pallas as pl
from jax.experimental.pallas import tpu as pltpu
from jax.sharding import PartitionSpec as P

F32 = jnp.float32
BF16 = jnp.bfloat16
I32 = jnp.int32
FINE = 32
CHUNK = 256
BANDS = 4
FIELDS = 8
MESH = pl.DeviceIdType.MESH


def seed_tables(length, fine):
    pixels = np.arange(length, dtype=np.int64)
    rows = np.concatenate([np.arange(fine), fine * np.arange(length // fine)])
    angle = (rows[:, None] * pixels[None, :] % length) * (2.0 * math.pi / length)
    scale = np.where(np.arange(rows.shape[0]) < fine, 1.0 / math.sqrt(length), 1.0)[:, None]
    return np.stack([np.cos(angle) * scale, np.sin(angle) * scale]).astype(np.float32)


def wide(column, width):
    return jnp.concatenate([column] * (width // column.shape[1]), axis=1)


def kernel(
    count_in, offset_in, width_in, bins_in, used_in, seeds_in, sky_in, weight_in,
    inner_got, edge_got,
    meta_ref, meta_got, meta_all, sky_ref, outer_ref, inner_ref, weight_ref, weight_got,
    seeds_ref, row_tab, flip_tab, col_tab,
    beamed, first, spread, gx_ref, gy_ref, gx_half, gy_half,
    part_send, part_got, totals, raw_send, raw_got, own_send, own_got,
    sum_send, sum_got, back_send, back_got, weights, scaled_own, scaled_par, acc_outer, acc_inner, edge_send, inner_send,
    local_sems, meta_sems, sky_sems, weight_sems, part_sems, raw_sems, own_sems, sum_sems,
    back_sems, par_sems, last_sems,
):
    size = sky_ref.shape[0]
    length = 2 * size
    slots, slots_uv, block = weight_ref.shape[0], weight_ref.shape[1], weight_ref.shape[2]
    half_slots = slots // 2
    ty, tx = lax.axis_index("ty"), lax.axis_index("tx")
    ny, nx = lax.axis_size("ty"), lax.axis_size("tx")
    core = tx % 2
    partner = tx + 1 - 2 * core
    beyond = tx - 1 + 2 * core
    has_up, has_down = ty > 0, ty < ny - 1
    has_beyond = jnp.logical_and(beyond >= 0, beyond < nx)
    has_row = (has_up, has_down)
    row_half = pl.multiple_of((ty % 2) * size, size)
    col_half = pl.multiple_of((1 - core) * size, size)
    to_partner = {"tx": partner}
    to_beyond = {"tx": beyond}
    to_row = ({"ty": ty - 1}, {"ty": ty + 1})
    to_cross = ({"ty": ty - 1, "tx": partner}, {"ty": ty + 1, "tx": partner})
    odd_row = ty % 2
    d_far, d_mate = 2 * odd_row, 2 * (1 - odd_row)
    giving, fed = ty - 2 + 4 * odd_row, ty + 2 - 4 * odd_row
    has_far = jnp.logical_and(giving >= 0, giving < ny)
    has_fed = jnp.logical_and(fed >= 0, fed < ny)
    to_mate, to_giving, to_fed = {"ty": ty + 1 - 2 * odd_row}, {"ty": giving}, {"ty": fed}
    to_far = {"ty": ty - 1 + 2 * odd_row}

    local = [
        pltpu.make_async_copy(source, target, local_sems.at[i])
        for i, (source, target) in enumerate(
            (
                (sky_in, sky_ref),
                (seeds_in, seeds_ref),
                (weight_in, weight_ref),
            )
        )
    ]

    def remote(src, dst, sems, at, target):
        return pltpu.make_async_remote_copy(
            src_ref=src,
            dst_ref=dst,
            send_sem=sems.at[(0,) + at],
            recv_sem=sems.at[(1,) + at],
            device_id=target,
            device_id_type=MESH,
        )

    def meta_copy(slot, target):
        return remote(meta_ref, meta_got[slot], meta_sems, (slot,), target)

    def meta_partner():
        return meta_copy(0, to_partner)

    def meta_send(side):
        return meta_copy(2 - side, to_row[side]), meta_copy(4 - side, to_cross[side])

    def meta_take(side):
        return meta_copy(1 + side, to_row[side]), meta_copy(3 + side, to_cross[side])

    def sky_partner():
        return remote(sky_ref, inner_ref, sky_sems, (0,), to_partner)

    def sky_beyond():
        return remote(sky_ref, outer_ref, sky_sems, (1,), to_beyond)

    def weight_copy():
        return remote(weight_ref, weight_got, weight_sems, (0,), to_partner)

    def part_copy(g, jj):
        return remote(part_send.at[g, jj], part_got.at[g, jj], part_sems, (g, jj), to_partner)

    def raw_copy(target, jj, k):
        return remote(raw_send.at[jj, k], raw_got.at[jj, k], raw_sems, (jj, k), target)

    def own_copy(jj, k):
        return remote(own_send.at[jj, k], own_got.at[jj, k], own_sems, (jj, k), to_mate)

    def sum_copy(jj, k):
        return remote(sum_send.at[jj, k], sum_got.at[jj, k], sum_sems, (jj, k), to_mate)

    def back_copy(target, jj, k):
        return remote(back_send.at[jj, k], back_got.at[jj, k], back_sems, (jj, k), target)

    def weights_mate():
        return remote(weights.at[2], weights.at[1], weight_sems, (1,), to_mate)

    def weights_far():
        return remote(weights.at[2], weights.at[0], weight_sems, (2,), to_far)

    def par_copy(g, jj, k):
        return remote(
            scaled_own.at[g, jj, k], scaled_par.at[g, jj, k], par_sems, (g, jj, k), to_partner
        )

    def last_edge():
        return remote(edge_send, edge_got, last_sems, (0,), to_beyond)

    def last_inner():
        return remote(inner_send, inner_got, last_sems, (1,), to_partner)

    def no_edge():
        return pltpu.make_async_copy(edge_send, edge_got, local_sems.at[len(local)])

    barrier = pltpu.get_barrier_semaphore()
    pl.semaphore_signal(barrier, inc=1, device_id=to_partner, device_id_type=MESH)

    @pl.when(has_beyond)
    def _():
        pl.semaphore_signal(barrier, inc=1, device_id=to_beyond, device_id_type=MESH)

    for side in range(2):

        @pl.when(has_row[side])
        def _(side=side):
            pl.semaphore_signal(barrier, inc=1, device_id=to_row[side], device_id_type=MESH)
            pl.semaphore_signal(barrier, inc=1, device_id=to_cross[side], device_id_type=MESH)

    for has, target in ((has_far, to_giving), (has_fed, to_fed)):

        @pl.when(has)
        def _(target=target):
            pl.semaphore_signal(barrier, inc=1, device_id=target, device_id_type=MESH)

    for copy in local:
        copy.start()

    lane = lax.broadcasted_iota(I32, (1, slots), 1)
    widths = width_in[...].astype(F32)
    meta_ref[slots, 0] = count_in[0, 0]
    for s in range(slots):
        meta_ref[s, 0] = offset_in[0, s]
        meta_ref[s, 1] = offset_in[1, s]
        meta_ref[s, 2] = jnp.sum(jnp.where(lane == s, widths, 0.0)).astype(I32)
        for k in range(slots_uv):
            for which in range(2):
                meta_ref[s, 3 + 2 * k + which] = bins_in[k, which, s]
        meta_ref[s, 3 + 2 * slots_uv] = used_in[0, s]

    @pl.when(jnp.logical_not(has_beyond))
    def _():
        outer_ref[...] = jnp.zeros_like(outer_ref)
        edge_send[...] = jnp.zeros_like(edge_send)

    with jax.named_scope("barrier"):
        local[0].wait()
        pl.semaphore_wait(
            barrier,
            1 + has_beyond.astype(I32) + 2 * has_up.astype(I32) + 2 * has_down.astype(I32)
            + has_far.astype(I32) + has_fed.astype(I32),
        )

    @pl.when(has_beyond)
    def _():
        sky_beyond().start()

    sky_partner().start()
    meta_partner().start()
    for side in range(2):

        @pl.when(has_row[side])
        def _(side=side):
            for copy in meta_send(side):
                copy.start()

    for copy in local[1:]:
        copy.wait()
    weight_copy().start()

    acc_outer[...] = jnp.zeros_like(acc_outer)
    acc_inner[...] = jnp.zeros_like(acc_inner)

    per_block = block // FINE

    def table(j, carry):
        blk, at = j // per_block, pl.ds(pl.multiple_of((j % per_block) * FINE, FINE), FINE)
        for tab, half in ((row_tab, row_half), (col_tab, col_half)):
            lanes = pl.ds(half, size)
            c, s = seeds_ref[0, pl.ds(FINE + j, 1), lanes], seeds_ref[1, pl.ds(FINE + j, 1), lanes]
            fc, fs = seeds_ref[0, :FINE, lanes], seeds_ref[1, :FINE, lanes]
            tab[blk, at, :] = (fc * c - fs * s).astype(BF16)
            tab[blk, pl.ds(pl.multiple_of(block + (j % per_block) * FINE, FINE), FINE), :] = (fs * c + fc * s).astype(BF16)
        return carry

    with jax.named_scope("tables"):
        lax.fori_loop(0, length // FINE, table, 0)

    def flipped(j, carry):
        row = (ty % 2) * (size // FINE) + j
        c, s = seeds_ref[0, pl.ds(FINE + row, 1), :], seeds_ref[1, pl.ds(FINE + row, 1), :]
        fc, fs = seeds_ref[0, :FINE, :], seeds_ref[1, :FINE, :]
        at = pl.ds(pl.multiple_of(j * FINE, FINE), FINE)
        cos, sin = (fc * c - fs * s).astype(BF16), (fs * c + fc * s).astype(BF16)
        for blk in range(length // block):
            flip_tab[blk, at, :block] = cos[:, blk * block : (blk + 1) * block]
            flip_tab[blk, at, block:] = sin[:, blk * block : (blk + 1) * block]
        return carry

    with jax.named_scope("flips"):
        lax.fori_loop(0, size // FINE, flipped, 0)

    with jax.named_scope("meta"):
        meta_partner().wait()
        for side in range(2):

            @pl.when(has_row[side])
            def _(side=side):
                for copy in meta_take(side):
                    copy.wait_recv()

            @pl.when(jnp.logical_not(has_row[side]))
            def _(side=side):
                for slot in (1 + side, 3 + side):
                    meta_got[slot][slots, 0] = 0
                    for s in range(slots):
                        for f in range(FIELDS):
                            meta_got[slot][s, f] = 0

    sources = ((meta_got[1], meta_got[3]), (meta_ref, meta_got[0]), (meta_got[2], meta_got[4]))
    even_here = core == 0

    def gather(s, f):
        for d, (same, other) in enumerate(sources):
            a, b = same[s, f], other[s, f]
            meta_all[d, 0, s, f] = jnp.where(even_here, a, b)
            meta_all[d, 1, s, f] = jnp.where(even_here, b, a)

    def gather_slot(s, carry):
        for f in range(FIELDS):
            gather(s, f)
        return carry

    lax.fori_loop(0, slots, gather_slot, 0)
    gather(slots, 0)

    def pointing(d, j):
        even, odd = meta_all[d, 0, slots, 0], meta_all[d, 1, slots, 0]
        from_odd = (j >= even).astype(I32)
        slot = jnp.clip(j - from_odd * even, 0, slots - 1)
        live = j < even + odd
        return from_odd, slot, live

    def bins(d, from_odd, slot, k, which):
        b = meta_all[d, from_odd, slot, 3 + 2 * k + which]
        return jnp.clip(b, 0, length // block - 1)

    def gaussian(shape, axis, shift, decay, live):
        away = lax.broadcasted_iota(I32, shape, axis) + shift
        inside = jnp.logical_and(away >= -size, away < size)
        inside = jnp.logical_and(inside, live)
        away = away.astype(F32)
        if axis == 0:
            fold = away.reshape(shape[0] // 8, 8, shape[1])
            value = jnp.exp(-(fold * fold) * decay[None]).reshape(shape)
        else:
            value = jnp.exp(-(away * away) * wide(decay, shape[1]))
        return jnp.where(inside, value, jnp.zeros(shape, F32))

    def beams(i, carry):
        d, j = i // slots, i % slots
        from_odd, slot, live = pointing(d, j)
        oy, ox = meta_all[d, from_odd, slot, 0], meta_all[d, from_odd, slot, 1]
        width = jnp.full((8, 128), meta_all[d, from_odd, slot, 2], I32).astype(F32)
        decay = 1.0 / (2.0 * width * width)
        gy = gaussian((size, 128), 0, (1 - d) * size - oy, decay, live)
        gy_ref[d, j] = gy
        gy_half[d, j] = gy.astype(BF16)
        outer_at, inner_at = 3 * core - 1, 1 - core
        for i, tile_at in enumerate((outer_at, inner_at)):
            gx = gaussian((8, size), 1, (tile_at - from_odd) * size - ox, decay, live)
            gx_ref[d, j, i] = gx
            gx_half[d, j, i] = jnp.concatenate([gx, gx], axis=0).astype(BF16)
        return carry

    with jax.named_scope("weights"):
        weight_copy().wait_recv()
        for jj in range(half_slots):
            from_odd, slot, live = pointing(1, half_slots * core + jj)
            used = meta_all[1, from_odd, slot, 3 + 2 * slots_uv]
            for k in range(slots_uv):
                weight = jnp.where(from_odd == core, weight_ref[slot, k], weight_got[slot, k])
                weight = weight.astype(F32) * jnp.where(k < used, 1.0, 0.0).astype(F32)
                weights[2, jj, k] = weight.astype(BF16)

        weights_mate().start()

        @pl.when(has_far)
        def _():
            weights_far().start()

    with jax.named_scope("beams"):
        lax.fori_loop(0, 3 * slots, beams, 0)

    def column_table(d, from_odd, slot, k):
        return col_tab[bins(d, from_odd, slot, k, 1)]

    def prepare(d, j, beamed_ref):
        gy = wide(gy_half[d, j], CHUNK)
        for at in range(0, size, CHUNK):
            cols = slice(at, at + CHUNK)
            gx = [jnp.concatenate([gx_half[d, j, i, :, cols]] * (size // 16), axis=0) for i in range(2)]
            value = gx[0] * outer_ref[:, cols] + gx[1] * inner_ref[:, cols]
            beamed_ref[:, cols] = gy * value

    def multiply(d, j, beamed_ref, first_ref, result_ref):
        from_odd, slot, live = pointing(d, j)
        rows = jnp.concatenate(
            [row_tab[bins(d, from_odd, slot, k, 0)] for k in range(slots_uv)], axis=0
        )
        for at in range(0, size, CHUNK):
            cols = slice(at, at + CHUNK)
            first_ref[:, cols] = jnp.dot(
                rows, beamed_ref[:, cols], preferred_element_type=F32
            ).astype(BF16)
        for k in range(slots_uv):
            both = lax.dot_general(
                first_ref[2 * k * block : (2 * k + 2) * block, :],
                col_tab[bins(d, from_odd, slot, k, 1)],
                (((1,), (1,)), ((), ())),
                preferred_element_type=F32,
            )
            real = both[:block, :block] - both[block:, block:]
            turned = both[:block, block:] + both[block:, :block]
            result_ref[k, :, :block] = real.astype(result_ref.dtype)
            result_ref[k, :, block:] = turned.astype(result_ref.dtype)

    def adjoint(d, j, scaled_ref, spread_ref):
        from_odd, slot, live = pointing(d, j)
        rows = jnp.concatenate(
            [flip_tab[bins(d, from_odd, slot, k, 0)] for k in range(slots_uv)], axis=1
        )
        gy = wide(gy_ref[d, j], CHUNK)
        for k in range(slots_uv):
            value = scaled_ref[k]
            real, turned = value[:, :block], value[:, block:]
            square = jnp.concatenate(
                [value, jnp.concatenate([turned, -real], axis=1)], axis=0
            )
            spread_ref[2 * k * block : (2 * k + 2) * block, :] = jnp.dot(
                square, column_table(d, from_odd, slot, k), preferred_element_type=F32
            ).astype(BF16)
        for at in range(0, size, CHUNK):
            cols = slice(at, at + CHUNK)
            back = gy * jnp.dot(rows, spread_ref[:, cols], preferred_element_type=F32)
            acc_outer[:, cols] += gx_ref[d, j, 0, 0:1, cols] * back
            acc_inner[:, cols] += gx_ref[d, j, 1, 0:1, cols] * back

    mine, theirs = half_slots * core, half_slots * (1 - core)

    with jax.named_scope("sky"):
        sky_partner().wait_recv()

        @pl.when(has_beyond)
        def _():
            sky_beyond().wait_recv()

    def pass_sum(jj, k, value):
        sum_send[jj, k] = value.astype(BF16)
        sum_copy(jj, k).start()

    def row_of(g):
        own = g // 2
        return 2 * (odd_row * (1 - g) + (1 - odd_row) * g) * (1 - own) + own

    def settle(g, jj):
        part_copy(g, jj).wait_recv()
        for k in range(slots_uv):
            totals[g, jj, k] = totals[g, jj, k] + part_got[g, jj, k].astype(F32)

        @pl.when(g == 0)
        def _():
            for k in range(slots_uv):
                raw_send[jj, k] = totals[0, jj, k].astype(BF16)
                raw_copy(to_giving, jj, k).start()

        @pl.when(g == 2)
        def _():
            for k in range(slots_uv):
                own_send[jj, k] = totals[2, jj, k].astype(BF16)
                own_copy(jj, k).start()

        @pl.when(jnp.logical_and(g == 1, jnp.logical_not(has_fed)))
        def _():
            for k in range(slots_uv):
                pass_sum(jj, k, totals[1, jj, k])

    far = has_far.astype(I32)

    def forward_units(s, carry):
        end = s // half_slots
        slot = s * (1 - end)
        units = (
            (2 * (1 - end) * (1 - far) + end, slot),
            ((1 - end) * (1 + far) + end, slot + end),
        )
        for i, (g, jj) in enumerate(units):
            prepare(row_of(g), theirs + jj, beamed[i])
            multiply(row_of(g), theirs + jj, beamed[i], first[i], part_send.at[g, jj])
            part_copy(g, jj).start()
        for i, (g, jj) in enumerate(units):
            prepare(row_of(g), mine + jj, beamed[i])
            multiply(row_of(g), mine + jj, beamed[i], first[i], totals.at[g, jj])
            settle(g, jj)
        return carry

    with jax.named_scope("forward"):
        lax.fori_loop(0, half_slots + far, forward_units, 0)

    def scale(g, jj, k, total):
        weight = weights[g, jj, k].astype(F32)
        scaled_own[g, jj, k] = (total * wide(weight, 2 * block)).astype(BF16)
        par_copy(g, jj, k).start()

    def adjoint_mine(g, jj):
        adjoint(row_of(g), mine + jj, scaled_own.at[g, jj], spread[0])

    def adjoint_theirs(g):
        with jax.named_scope(f"theirs{g}"):
            for jj in range(half_slots):
                for k in range(slots_uv):
                    par_copy(g, jj, k).wait_recv()
            for jj in range(half_slots):
                adjoint(row_of(g), theirs + jj, scaled_par.at[g, jj], spread[jj % 2])

    with jax.named_scope("mate"):
        weights_mate().wait_recv()
        for jj in range(half_slots):
            for k in range(slots_uv):
                own_copy(jj, k).wait_recv()
                both = totals[1, jj, k] + own_got[jj, k].astype(F32)

                @pl.when(has_fed)
                def _(jj=jj, k=k, both=both):
                    back_send[jj, k] = both.astype(BF16)
                    back_copy(to_fed, jj, k).start()
                    raw_copy(to_fed, jj, k).wait_recv()
                    far_part = raw_got[jj, k].astype(F32)
                    pass_sum(jj, k, totals[1, jj, k] + far_part)
                    totals[1, jj, k] = totals[1, jj, k] + far_part

                scale(1, jj, k, totals[1, jj, k] + own_got[jj, k].astype(F32))

        for jj in range(half_slots):
            adjoint_mine(1, jj)

    adjoint_theirs(1)

    def far_step(jj, carry):
        for k in range(slots_uv):
            back_copy(to_giving, jj, k).wait_recv()
            scale(0, jj, k, totals[0, jj, k] + back_got[jj, k].astype(F32))
        adjoint_mine(0, jj)
        return carry

    @pl.when(has_far)
    def _():
        weights_far().wait_recv()
        with jax.named_scope("far"):
            lax.fori_loop(0, half_slots, far_step, 0)
        adjoint_theirs(0)

    def own_step(jj, carry):
        for k in range(slots_uv):
            sum_copy(jj, k).wait_recv()
            scale(2, jj, k, totals[2, jj, k] + sum_got[jj, k].astype(F32))
        adjoint_mine(2, jj)
        return carry

    with jax.named_scope("own"):
        lax.fori_loop(0, half_slots, own_step, 0)

    adjoint_theirs(2)

    @pl.when(has_beyond)
    def _():
        edge_send[...] = acc_outer[...].astype(BF16)
        last_edge().start()

    inner_send[...] = acc_inner[...].astype(BF16)
    last_inner().start()

    @pl.when(jnp.logical_not(has_beyond))
    def _():
        no_edge().start()

    sky_partner().wait_send()
    weight_copy().wait_send()

    @pl.when(has_beyond)
    def _():
        sky_beyond().wait_send()

    for side in range(2):

        @pl.when(has_row[side])
        def _(side=side):
            for copy in meta_send(side):
                copy.wait_send()

    for jj in range(half_slots):
        for g in (1, 2):
            part_copy(g, jj).wait_send()
            for k in range(slots_uv):
                par_copy(g, jj, k).wait_send()
        for k in range(slots_uv):
            own_copy(jj, k).wait_send()
            sum_copy(jj, k).wait_send()

            @pl.when(has_fed)
            def _(jj=jj, k=k):
                back_copy(to_fed, jj, k).wait_send()

        @pl.when(has_far)
        def _(jj=jj):
            part_copy(0, jj).wait_send()
            for k in range(slots_uv):
                par_copy(0, jj, k).wait_send()
                raw_copy(to_giving, jj, k).wait_send()

    weights_mate().wait_send()

    @pl.when(has_far)
    def _():
        weights_far().wait_send()

    with jax.named_scope("last"):
        last_inner().wait()

        @pl.when(has_beyond)
        def _():
            last_edge().wait()

        @pl.when(jnp.logical_not(has_beyond))
        def _():
            no_edge().wait()


def add_kernel(inner_hbm, edge_hbm, out_hbm, inner_ref, edge_ref, out_ref, sems):
    band = out_ref.shape[0] // BANDS
    bands = [slice(i * band, (i + 1) * band) for i in range(BANDS)]
    moves = [
        [
            pltpu.make_async_copy(inner_hbm.at[rows], inner_ref.at[rows], sems.at[0, i]),
            pltpu.make_async_copy(edge_hbm.at[rows], edge_ref.at[rows], sems.at[1, i]),
            pltpu.make_async_copy(out_ref.at[rows], out_hbm.at[rows], sems.at[2, i]),
        ]
        for i, rows in enumerate(bands)
    ]
    for inner, edge, out in moves:
        inner.start()
        edge.start()
    for rows, (inner, edge, out) in zip(bands, moves):
        inner.wait()
        edge.wait()
        out_ref[rows, :] = inner_ref[rows, :].astype(F32) + edge_ref[rows, :].astype(F32)
        out.start()
    for inner, edge, out in moves:
        out.wait()


def shards(sky, point_count, point_offset, beam_width, uv_bins, uv_count, uv_weight):
    size = sky.shape[0]
    length = 2 * size
    slots, slots_uv, block = uv_weight.shape[2], uv_weight.shape[3], uv_weight.shape[4]
    half_slots = slots // 2
    depth = 2 * slots_uv * block
    seeds = seed_tables(length, FINE)
    count = point_count.reshape(1, 1)
    offset = jnp.transpose(point_offset, (0, 1, 3, 2)).reshape(2, slots)
    width = beam_width.reshape(1, slots)
    bins = jnp.transpose(uv_bins, (0, 1, 3, 4, 2)).reshape(slots_uv, 2, slots)
    used = uv_count.reshape(1, slots)
    weight = uv_weight.reshape(slots, slots_uv, block, block)

    dma = pltpu.SemaphoreType.DMA
    meta_shape = (slots + 1, FIELDS)
    tile = pltpu.VMEM((size, size), BF16)
    plane = pltpu.VMEM((size, size), F32)
    patch = (slots_uv, block, 2 * block)
    smem, anywhere = pl.BlockSpec(memory_space=pltpu.SMEM), pl.BlockSpec(memory_space=pl.ANY)
    inner, edge = pl.pallas_call(
        kernel,
        out_shape=(jax.ShapeDtypeStruct((size, size), BF16),) * 2,
        in_specs=[smem, smem, pl.BlockSpec(memory_space=pltpu.VMEM), smem, smem] + [anywhere] * 3,
        out_specs=(anywhere, anywhere),
        scratch_shapes=[
            pltpu.SMEM(meta_shape, I32),
            tuple([pltpu.SMEM(meta_shape, I32)] * 5),
            pltpu.SMEM((3, 2) + meta_shape, I32),
            tile,
            tile,
            tile,
            pltpu.VMEM(weight.shape, BF16),
            pltpu.VMEM(weight.shape, BF16),
            pltpu.VMEM(seeds.shape, F32),
            pltpu.VMEM((length // block, 2 * block, size), BF16),
            pltpu.VMEM((length // block, size, 2 * block), BF16),
            pltpu.VMEM((length // block, 2 * block, size), BF16),
            (tile, tile),
            (pltpu.VMEM((depth, size), BF16),) * 2,
            (pltpu.VMEM((depth, size), BF16),) * 2,
            pltpu.VMEM((3, slots, 2, 8, size), F32),
            pltpu.VMEM((3, slots, size, 128), F32),
            pltpu.VMEM((3, slots, 2, 16, size), BF16),
            pltpu.VMEM((3, slots, size, 128), BF16),
            pltpu.VMEM((3, half_slots) + patch, BF16),
            pltpu.VMEM((3, half_slots) + patch, BF16),
            pltpu.VMEM((3, half_slots) + patch, F32),
            *[pltpu.VMEM((half_slots,) + patch, BF16)] * 8,
            pltpu.VMEM((3, half_slots, slots_uv, block, block), BF16),
            pltpu.VMEM((3, half_slots) + patch, BF16),
            pltpu.VMEM((3, half_slots) + patch, BF16),
            plane,
            plane,
            tile,
            tile,
            dma((4,)),
            dma((2, 5)),
            dma((2, 2)),
            dma((2, 3)),
            dma((2, 3, half_slots)),
            dma((2, half_slots, slots_uv)),
            dma((2, half_slots, slots_uv)),
            dma((2, half_slots, slots_uv)),
            dma((2, half_slots, slots_uv)),
            dma((2, 3, half_slots, slots_uv)),
            dma((2, 2)),
        ],
        compiler_params=pltpu.CompilerParams(
            vmem_limit_bytes=int(56 * 1024 * 1024), collective_id=0, has_side_effects=True
        ),
    )(count, offset, width, bins, used, seeds, sky, weight)
    return pl.pallas_call(
        add_kernel,
        out_shape=jax.ShapeDtypeStruct((size, size), F32),
        in_specs=[anywhere, anywhere],
        out_specs=anywhere,
        scratch_shapes=[tile, tile, plane, dma((3, BANDS))],
        compiler_params=pltpu.CompilerParams(vmem_limit_bytes=56 * 1024 * 1024),
        cost_estimate=pl.CostEstimate(flops=size * size, bytes_accessed=10 * size * size, transcendentals=0),
    )(inner, edge)


def solution(mesh):
    in_specs = (
        P("ty", "tx"),
        P("ty", "tx"),
        P("ty", "tx", None, None),
        P("ty", "tx", None),
        P("ty", "tx", None, None, None),
        P("ty", "tx", None),
        P("ty", "tx", None, None, None, None),
    )
    out_specs = P("ty", "tx")
    return jax.shard_map(shards, mesh=mesh, in_specs=in_specs, out_specs=out_specs, check_vma=False)
```

```python
import functools
import math

import jax
import jax.numpy as jnp
import numpy as np
from jax import lax
from jax.experimental import pallas as pl
from jax.experimental.pallas import tpu as pltpu
from jax.sharding import PartitionSpec as P

F32 = jnp.float32
BF16 = jnp.bfloat16
I32 = jnp.int32
FINE = 32
CHUNK = 256
BANDS = 4
EDGES = 2
FIELDS = 8
MESH = pl.DeviceIdType.MESH


def seed_tables(length, fine):
    pixels = np.arange(length, dtype=np.int64)
    rows = np.concatenate([np.arange(fine), fine * np.arange(length // fine)])
    angle = (rows[:, None] * pixels[None, :] % length) * (2.0 * math.pi / length)
    scale = np.where(np.arange(rows.shape[0]) < fine, 1.0 / math.sqrt(length), 1.0)[:, None]
    return np.stack([np.cos(angle) * scale, np.sin(angle) * scale]).astype(np.float32)


def wide(column, width):
    return jnp.concatenate([column] * (width // column.shape[1]), axis=1)


def kernel(
    count_in, offset_in, width_in, bins_in, used_in, seeds_in, sky_in, weight_in,
    inner_got, edge_got,
    meta_ref, meta_got, meta_all, sky_ref, outer_ref, inner_ref, weight_ref, weight_got,
    seeds_ref, row_tab, flip_tab, col_tab,
    beamed, first, spread, gx_ref, gy_ref, gx_half, gy_half,
    part_send, part_got, totals, raw_send, raw_got, own_send, own_got,
    sum_send, sum_got, back_send, back_got, weights, scaled_own, scaled_par, acc_outer, acc_inner, edge_send, inner_send,
    local_sems, meta_sems, sky_sems, weight_sems, part_sems, raw_sems, own_sems, sum_sems,
    back_sems, par_sems, last_sems,
):
    size = sky_ref.shape[0]
    length = 2 * size
    slots, slots_uv, block = weight_ref.shape[0], weight_ref.shape[1], weight_ref.shape[2]
    half_slots = slots // 2
    ty, tx = lax.axis_index("ty"), lax.axis_index("tx")
    ny, nx = lax.axis_size("ty"), lax.axis_size("tx")
    core = tx % 2
    partner = tx + 1 - 2 * core
    beyond = tx - 1 + 2 * core
    has_up, has_down = ty > 0, ty < ny - 1
    has_beyond = jnp.logical_and(beyond >= 0, beyond < nx)
    has_row = (has_up, has_down)
    row_half = pl.multiple_of((ty % 2) * size, size)
    col_half = pl.multiple_of((1 - core) * size, size)
    to_partner = {"tx": partner}
    to_beyond = {"tx": beyond}
    to_row = ({"ty": ty - 1}, {"ty": ty + 1})
    to_cross = ({"ty": ty - 1, "tx": partner}, {"ty": ty + 1, "tx": partner})
    odd_row = ty % 2
    d_far, d_mate = 2 * odd_row, 2 * (1 - odd_row)
    giving, fed = ty - 2 + 4 * odd_row, ty + 2 - 4 * odd_row
    has_far = jnp.logical_and(giving >= 0, giving < ny)
    has_fed = jnp.logical_and(fed >= 0, fed < ny)
    to_mate, to_giving, to_fed = {"ty": ty + 1 - 2 * odd_row}, {"ty": giving}, {"ty": fed}
    to_far = {"ty": ty - 1 + 2 * odd_row}

    local = [
        pltpu.make_async_copy(source, target, local_sems.at[i])
        for i, (source, target) in enumerate(
            (
                (sky_in, sky_ref),
                (seeds_in, seeds_ref),
                (weight_in, weight_ref),
            )
        )
    ]

    def remote(src, dst, sems, at, target):
        return pltpu.make_async_remote_copy(
            src_ref=src,
            dst_ref=dst,
            send_sem=sems.at[(0,) + at],
            recv_sem=sems.at[(1,) + at],
            device_id=target,
            device_id_type=MESH,
        )

    def meta_copy(slot, target):
        return remote(meta_ref, meta_got[slot], meta_sems, (slot,), target)

    def meta_partner():
        return meta_copy(0, to_partner)

    def meta_send(side):
        return meta_copy(2 - side, to_row[side]), meta_copy(4 - side, to_cross[side])

    def meta_take(side):
        return meta_copy(1 + side, to_row[side]), meta_copy(3 + side, to_cross[side])

    def sky_partner():
        return remote(sky_ref, inner_ref, sky_sems, (0,), to_partner)

    def sky_beyond():
        return remote(sky_ref, outer_ref, sky_sems, (1,), to_beyond)

    def weight_copy():
        return remote(weight_ref, weight_got, weight_sems, (0,), to_partner)

    def part_copy(g, jj):
        return remote(part_send.at[g, jj], part_got.at[g, jj], part_sems, (g, jj), to_partner)

    def raw_copy(target, jj, k):
        return remote(raw_send.at[jj, k], raw_got.at[jj, k], raw_sems, (jj, k), target)

    def own_copy(jj, k):
        return remote(own_send.at[jj, k], own_got.at[jj, k], own_sems, (jj, k), to_mate)

    def sum_copy(jj, k):
        return remote(sum_send.at[jj, k], sum_got.at[jj, k], sum_sems, (jj, k), to_mate)

    def back_copy(target, jj, k):
        return remote(back_send.at[jj, k], back_got.at[jj, k], back_sems, (jj, k), target)

    def weights_mate():
        return remote(weights.at[2], weights.at[1], weight_sems, (1,), to_mate)

    def weights_far():
        return remote(weights.at[2], weights.at[0], weight_sems, (2,), to_far)

    def par_copy(g, jj, k):
        return remote(
            scaled_own.at[g, jj, k], scaled_par.at[g, jj, k], par_sems, (g, jj, k), to_partner
        )

    def last_edge(band):
        rows = slice(band * size // EDGES, (band + 1) * size // EDGES)
        return remote(edge_send.at[rows], edge_got.at[rows], last_sems, (1 + band,), to_beyond)

    def last_inner():
        return remote(inner_send, inner_got, last_sems, (0,), to_partner)

    def no_edge():
        return pltpu.make_async_copy(edge_send, edge_got, local_sems.at[len(local)])

    barrier = pltpu.get_barrier_semaphore()
    pl.semaphore_signal(barrier, inc=1, device_id=to_partner, device_id_type=MESH)

    @pl.when(has_beyond)
    def _():
        pl.semaphore_signal(barrier, inc=1, device_id=to_beyond, device_id_type=MESH)

    for side in range(2):

        @pl.when(has_row[side])
        def _(side=side):
            pl.semaphore_signal(barrier, inc=1, device_id=to_row[side], device_id_type=MESH)
            pl.semaphore_signal(barrier, inc=1, device_id=to_cross[side], device_id_type=MESH)

    for has, target in ((has_far, to_giving), (has_fed, to_fed)):

        @pl.when(has)
        def _(target=target):
            pl.semaphore_signal(barrier, inc=1, device_id=target, device_id_type=MESH)

    for copy in local:
        copy.start()

    lane = lax.broadcasted_iota(I32, (1, slots), 1)
    widths = width_in[...].astype(F32)
    meta_ref[slots, 0] = count_in[0, 0]
    for s in range(slots):
        meta_ref[s, 0] = offset_in[0, s]
        meta_ref[s, 1] = offset_in[1, s]
        meta_ref[s, 2] = jnp.sum(jnp.where(lane == s, widths, 0.0)).astype(I32)
        for k in range(slots_uv):
            for which in range(2):
                meta_ref[s, 3 + 2 * k + which] = bins_in[k, which, s]
        meta_ref[s, 3 + 2 * slots_uv] = used_in[0, s]

    @pl.when(jnp.logical_not(has_beyond))
    def _():
        outer_ref[...] = jnp.zeros_like(outer_ref)
        edge_send[...] = jnp.zeros_like(edge_send)

    with jax.named_scope("barrier"):
        local[0].wait()
        pl.semaphore_wait(
            barrier,
            1 + has_beyond.astype(I32) + 2 * has_up.astype(I32) + 2 * has_down.astype(I32)
            + has_far.astype(I32) + has_fed.astype(I32),
        )

    @pl.when(has_beyond)
    def _():
        sky_beyond().start()

    sky_partner().start()
    meta_partner().start()
    for side in range(2):

        @pl.when(has_row[side])
        def _(side=side):
            for copy in meta_send(side):
                copy.start()

    for copy in local[1:]:
        copy.wait()
    weight_copy().start()

    acc_outer[...] = jnp.zeros_like(acc_outer)
    acc_inner[...] = jnp.zeros_like(acc_inner)

    per_block = block // FINE

    def table(j, carry):
        blk, at = j // per_block, pl.ds(pl.multiple_of((j % per_block) * FINE, FINE), FINE)
        for tab, half in ((row_tab, row_half), (col_tab, col_half)):
            lanes = pl.ds(half, size)
            c, s = seeds_ref[0, pl.ds(FINE + j, 1), lanes], seeds_ref[1, pl.ds(FINE + j, 1), lanes]
            fc, fs = seeds_ref[0, :FINE, lanes], seeds_ref[1, :FINE, lanes]
            tab[blk, at, :] = (fc * c - fs * s).astype(BF16)
            tab[blk, pl.ds(pl.multiple_of(block + (j % per_block) * FINE, FINE), FINE), :] = (fs * c + fc * s).astype(BF16)
        return carry

    with jax.named_scope("tables"):
        lax.fori_loop(0, length // FINE, table, 0)

    def flipped(j, carry):
        row = (ty % 2) * (size // FINE) + j
        c, s = seeds_ref[0, pl.ds(FINE + row, 1), :], seeds_ref[1, pl.ds(FINE + row, 1), :]
        fc, fs = seeds_ref[0, :FINE, :], seeds_ref[1, :FINE, :]
        at = pl.ds(pl.multiple_of(j * FINE, FINE), FINE)
        cos, sin = (fc * c - fs * s).astype(BF16), (fs * c + fc * s).astype(BF16)
        for blk in range(length // block):
            flip_tab[blk, at, :block] = cos[:, blk * block : (blk + 1) * block]
            flip_tab[blk, at, block:] = sin[:, blk * block : (blk + 1) * block]
        return carry

    with jax.named_scope("flips"):
        lax.fori_loop(0, size // FINE, flipped, 0)

    with jax.named_scope("meta"):
        meta_partner().wait()
        for side in range(2):

            @pl.when(has_row[side])
            def _(side=side):
                for copy in meta_take(side):
                    copy.wait_recv()

            @pl.when(jnp.logical_not(has_row[side]))
            def _(side=side):
                for slot in (1 + side, 3 + side):
                    meta_got[slot][slots, 0] = 0
                    for s in range(slots):
                        for f in range(FIELDS):
                            meta_got[slot][s, f] = 0

    sources = ((meta_got[1], meta_got[3]), (meta_ref, meta_got[0]), (meta_got[2], meta_got[4]))
    even_here = core == 0

    def gather(s, f):
        for d, (same, other) in enumerate(sources):
            a, b = same[s, f], other[s, f]
            meta_all[d, 0, s, f] = jnp.where(even_here, a, b)
            meta_all[d, 1, s, f] = jnp.where(even_here, b, a)

    def gather_slot(s, carry):
        for f in range(FIELDS):
            gather(s, f)
        return carry

    lax.fori_loop(0, slots, gather_slot, 0)
    gather(slots, 0)

    def pointing(d, j):
        even, odd = meta_all[d, 0, slots, 0], meta_all[d, 1, slots, 0]
        from_odd = (j >= even).astype(I32)
        slot = jnp.clip(j - from_odd * even, 0, slots - 1)
        live = j < even + odd
        return from_odd, slot, live

    def bins(d, from_odd, slot, k, which):
        b = meta_all[d, from_odd, slot, 3 + 2 * k + which]
        return jnp.clip(b, 0, length // block - 1)

    def gaussian(shape, axis, shift, decay, live):
        away = lax.broadcasted_iota(I32, shape, axis) + shift
        inside = jnp.logical_and(away >= -size, away < size)
        inside = jnp.logical_and(inside, live)
        away = away.astype(F32)
        if axis == 0:
            fold = away.reshape(shape[0] // 8, 8, shape[1])
            value = jnp.exp(-(fold * fold) * decay[None]).reshape(shape)
        else:
            value = jnp.exp(-(away * away) * wide(decay, shape[1]))
        return jnp.where(inside, value, jnp.zeros(shape, F32))

    def beams(i, carry):
        d, j = i // slots, i % slots
        from_odd, slot, live = pointing(d, j)
        oy, ox = meta_all[d, from_odd, slot, 0], meta_all[d, from_odd, slot, 1]
        width = jnp.full((8, 128), meta_all[d, from_odd, slot, 2], I32).astype(F32)
        decay = 1.0 / (2.0 * width * width)
        gy = gaussian((size, 128), 0, (1 - d) * size - oy, decay, live)
        gy_ref[d, j] = gy
        gy_half[d, j] = gy.astype(BF16)
        outer_at, inner_at = 3 * core - 1, 1 - core
        for i, tile_at in enumerate((outer_at, inner_at)):
            gx = gaussian((8, size), 1, (tile_at - from_odd) * size - ox, decay, live)
            gx_ref[d, j, i] = gx
            gx_half[d, j, i] = jnp.concatenate([gx, gx], axis=0).astype(BF16)
        return carry

    with jax.named_scope("weights"):
        weight_copy().wait_recv()
        for jj in range(half_slots):
            from_odd, slot, live = pointing(1, half_slots * core + jj)
            used = meta_all[1, from_odd, slot, 3 + 2 * slots_uv]
            for k in range(slots_uv):
                weight = jnp.where(from_odd == core, weight_ref[slot, k], weight_got[slot, k])
                weight = weight.astype(F32) * jnp.where(k < used, 1.0, 0.0).astype(F32)
                weights[2, jj, k] = weight.astype(BF16)

        weights_mate().start()

        @pl.when(has_far)
        def _():
            weights_far().start()

    with jax.named_scope("beams"):
        lax.fori_loop(0, 3 * slots, beams, 0)

    def column_table(d, from_odd, slot, k):
        return col_tab[bins(d, from_odd, slot, k, 1)]

    def prepare(d, j, beamed_ref):
        gy = wide(gy_half[d, j], CHUNK)
        for at in range(0, size, CHUNK):
            cols = slice(at, at + CHUNK)
            gx = [jnp.concatenate([gx_half[d, j, i, :, cols]] * (size // 16), axis=0) for i in range(2)]
            value = gx[0] * outer_ref[:, cols] + gx[1] * inner_ref[:, cols]
            beamed_ref[:, cols] = gy * value

    def multiply(d, j, beamed_ref, first_ref, result_ref):
        from_odd, slot, live = pointing(d, j)
        rows = jnp.concatenate(
            [row_tab[bins(d, from_odd, slot, k, 0)] for k in range(slots_uv)], axis=0
        )
        for at in range(0, size, CHUNK):
            cols = slice(at, at + CHUNK)
            first_ref[:, cols] = jnp.dot(
                rows, beamed_ref[:, cols], preferred_element_type=F32
            ).astype(BF16)
        for k in range(slots_uv):
            both = lax.dot_general(
                first_ref[2 * k * block : (2 * k + 2) * block, :],
                col_tab[bins(d, from_odd, slot, k, 1)],
                (((1,), (1,)), ((), ())),
                preferred_element_type=F32,
            )
            real = both[:block, :block] - both[block:, block:]
            turned = both[:block, block:] + both[block:, :block]
            result_ref[k, :, :block] = real.astype(result_ref.dtype)
            result_ref[k, :, block:] = turned.astype(result_ref.dtype)

    def spread_out(d, j, scaled_ref, spread_ref):
        from_odd, slot, live = pointing(d, j)
        for k in range(slots_uv):
            value = scaled_ref[k]
            real, turned = value[:, :block], value[:, block:]
            square = jnp.concatenate(
                [value, jnp.concatenate([turned, -real], axis=1)], axis=0
            )
            spread_ref[2 * k * block : (2 * k + 2) * block, :] = jnp.dot(
                square, col_tab[bins(d, from_odd, slot, k, 1)], preferred_element_type=F32
            ).astype(BF16)

    def bring_back(d, j, spread_ref, start, stop):
        from_odd, slot, live = pointing(d, j)
        rows = jnp.concatenate(
            [flip_tab[bins(d, from_odd, slot, k, 0), start:stop] for k in range(slots_uv)], axis=1
        )
        gy = wide(gy_ref[d, j, start:stop], CHUNK)
        for at in range(0, size, CHUNK):
            cols = slice(at, at + CHUNK)
            back = gy * jnp.dot(rows, spread_ref[:, cols], preferred_element_type=F32)
            acc_outer[start:stop, cols] += gx_ref[d, j, 0, 0:1, cols] * back
            acc_inner[start:stop, cols] += gx_ref[d, j, 1, 0:1, cols] * back

    def adjoint(d, j, scaled_ref, spread_ref):
        spread_out(d, j, scaled_ref, spread_ref)
        bring_back(d, j, spread_ref, 0, size)

    mine, theirs = half_slots * core, half_slots * (1 - core)

    with jax.named_scope("sky"):
        sky_partner().wait_recv()

        @pl.when(has_beyond)
        def _():
            sky_beyond().wait_recv()

    def pass_sum(jj, k, value):
        sum_send[jj, k] = value.astype(BF16)
        sum_copy(jj, k).start()

    def row_of(g):
        own = g // 2
        return 2 * (odd_row * (1 - g) + (1 - odd_row) * g) * (1 - own) + own

    def settle(g, jj):
        part_copy(g, jj).wait_recv()
        for k in range(slots_uv):
            totals[g, jj, k] = totals[g, jj, k] + part_got[g, jj, k].astype(F32)

        @pl.when(g == 0)
        def _():
            for k in range(slots_uv):
                raw_send[jj, k] = totals[0, jj, k].astype(BF16)
                raw_copy(to_giving, jj, k).start()

        @pl.when(g == 2)
        def _():
            for k in range(slots_uv):
                own_send[jj, k] = totals[2, jj, k].astype(BF16)
                own_copy(jj, k).start()

        @pl.when(jnp.logical_and(g == 1, jnp.logical_not(has_fed)))
        def _():
            for k in range(slots_uv):
                pass_sum(jj, k, totals[1, jj, k])

    far = has_far.astype(I32)

    def forward_units(s, carry):
        end = s // half_slots
        slot = s * (1 - end)
        units = (
            (2 * (1 - end) * (1 - far) + end, slot),
            ((1 - end) * (1 + far) + end, slot + end),
        )
        for i, (g, jj) in enumerate(units):
            prepare(row_of(g), theirs + jj, beamed[i])
            multiply(row_of(g), theirs + jj, beamed[i], first[i], part_send.at[g, jj])
            part_copy(g, jj).start()
        for i, (g, jj) in enumerate(units):
            prepare(row_of(g), mine + jj, beamed[i])
            multiply(row_of(g), mine + jj, beamed[i], first[i], totals.at[g, jj])
            settle(g, jj)
        return carry

    with jax.named_scope("forward"):
        lax.fori_loop(0, half_slots + far, forward_units, 0)

    def scale(g, jj, k, total):
        weight = weights[g, jj, k].astype(F32)
        scaled_own[g, jj, k] = (total * wide(weight, 2 * block)).astype(BF16)
        par_copy(g, jj, k).start()

    def adjoint_mine(g, jj):
        adjoint(row_of(g), mine + jj, scaled_own.at[g, jj], spread[0])

    def adjoint_theirs(g):
        with jax.named_scope(f"theirs{g}"):
            for jj in range(half_slots):
                for k in range(slots_uv):
                    par_copy(g, jj, k).wait_recv()
            for jj in range(half_slots):
                adjoint(row_of(g), theirs + jj, scaled_par.at[g, jj], spread[jj % 2])

    with jax.named_scope("mate"):
        weights_mate().wait_recv()
        for jj in range(half_slots):
            for k in range(slots_uv):
                own_copy(jj, k).wait_recv()
                both = totals[1, jj, k] + own_got[jj, k].astype(F32)

                @pl.when(has_fed)
                def _(jj=jj, k=k, both=both):
                    back_send[jj, k] = both.astype(BF16)
                    back_copy(to_fed, jj, k).start()
                    raw_copy(to_fed, jj, k).wait_recv()
                    far_part = raw_got[jj, k].astype(F32)
                    pass_sum(jj, k, totals[1, jj, k] + far_part)
                    totals[1, jj, k] = totals[1, jj, k] + far_part

                scale(1, jj, k, totals[1, jj, k] + own_got[jj, k].astype(F32))

        for jj in range(half_slots):
            adjoint_mine(1, jj)

    adjoint_theirs(1)

    def far_step(jj, carry):
        for k in range(slots_uv):
            back_copy(to_giving, jj, k).wait_recv()
            scale(0, jj, k, totals[0, jj, k] + back_got[jj, k].astype(F32))
        adjoint_mine(0, jj)
        return carry

    @pl.when(has_far)
    def _():
        weights_far().wait_recv()
        with jax.named_scope("far"):
            lax.fori_loop(0, half_slots, far_step, 0)

    def own_step(jj, carry):
        for k in range(slots_uv):
            sum_copy(jj, k).wait_recv()
            scale(2, jj, k, totals[2, jj, k] + sum_got[jj, k].astype(F32))
        adjoint_mine(2, jj)
        return carry

    with jax.named_scope("own"):
        lax.fori_loop(0, half_slots, own_step, 0)

    @pl.when(has_far)
    def _():
        adjoint_theirs(0)

    with jax.named_scope("theirs2"):
        for jj in range(half_slots):
            for k in range(slots_uv):
                par_copy(2, jj, k).wait_recv()
            spread_out(1, theirs + jj, scaled_par.at[2, jj], spread[jj % 2])
        for band in range(EDGES):
            start, stop = band * size // EDGES, (band + 1) * size // EDGES
            for jj in range(half_slots):
                bring_back(1, theirs + jj, spread[jj % 2], start, stop)

            @pl.when(has_beyond)
            def _(band=band, start=start, stop=stop):
                edge_send[start:stop] = acc_outer[start:stop].astype(BF16)
                last_edge(band).start()

    inner_send[...] = acc_inner[...].astype(BF16)
    last_inner().start()

    @pl.when(jnp.logical_not(has_beyond))
    def _():
        no_edge().start()

    sky_partner().wait_send()
    weight_copy().wait_send()

    @pl.when(has_beyond)
    def _():
        sky_beyond().wait_send()

    for side in range(2):

        @pl.when(has_row[side])
        def _(side=side):
            for copy in meta_send(side):
                copy.wait_send()

    for jj in range(half_slots):
        for g in (1, 2):
            part_copy(g, jj).wait_send()
            for k in range(slots_uv):
                par_copy(g, jj, k).wait_send()
        for k in range(slots_uv):
            own_copy(jj, k).wait_send()
            sum_copy(jj, k).wait_send()

            @pl.when(has_fed)
            def _(jj=jj, k=k):
                back_copy(to_fed, jj, k).wait_send()

        @pl.when(has_far)
        def _(jj=jj):
            part_copy(0, jj).wait_send()
            for k in range(slots_uv):
                par_copy(0, jj, k).wait_send()
                raw_copy(to_giving, jj, k).wait_send()

    weights_mate().wait_send()

    @pl.when(has_far)
    def _():
        weights_far().wait_send()

    with jax.named_scope("last"):
        last_inner().wait()

        @pl.when(has_beyond)
        def _():
            for band in range(EDGES):
                last_edge(band).wait()

        @pl.when(jnp.logical_not(has_beyond))
        def _():
            no_edge().wait()


def add_kernel(inner_hbm, edge_hbm, out_hbm, inner_ref, edge_ref, out_ref, sems):
    band = out_ref.shape[0] // BANDS
    bands = [slice(i * band, (i + 1) * band) for i in range(BANDS)]
    moves = [
        [
            pltpu.make_async_copy(inner_hbm.at[rows], inner_ref.at[rows], sems.at[0, i]),
            pltpu.make_async_copy(edge_hbm.at[rows], edge_ref.at[rows], sems.at[1, i]),
            pltpu.make_async_copy(out_ref.at[rows], out_hbm.at[rows], sems.at[2, i]),
        ]
        for i, rows in enumerate(bands)
    ]
    for inner, edge, out in moves:
        inner.start()
        edge.start()
    for rows, (inner, edge, out) in zip(bands, moves):
        inner.wait()
        edge.wait()
        out_ref[rows, :] = inner_ref[rows, :].astype(F32) + edge_ref[rows, :].astype(F32)
        out.start()
    for inner, edge, out in moves:
        out.wait()


def shards(sky, point_count, point_offset, beam_width, uv_bins, uv_count, uv_weight):
    size = sky.shape[0]
    length = 2 * size
    slots, slots_uv, block = uv_weight.shape[2], uv_weight.shape[3], uv_weight.shape[4]
    half_slots = slots // 2
    depth = 2 * slots_uv * block
    seeds = seed_tables(length, FINE)
    count = point_count.reshape(1, 1)
    offset = jnp.transpose(point_offset, (0, 1, 3, 2)).reshape(2, slots)
    width = beam_width.reshape(1, slots)
    bins = jnp.transpose(uv_bins, (0, 1, 3, 4, 2)).reshape(slots_uv, 2, slots)
    used = uv_count.reshape(1, slots)
    weight = uv_weight.reshape(slots, slots_uv, block, block)

    dma = pltpu.SemaphoreType.DMA
    meta_shape = (slots + 1, FIELDS)
    tile = pltpu.VMEM((size, size), BF16)
    plane = pltpu.VMEM((size, size), F32)
    patch = (slots_uv, block, 2 * block)
    smem, anywhere = pl.BlockSpec(memory_space=pltpu.SMEM), pl.BlockSpec(memory_space=pl.ANY)
    inner, edge = pl.pallas_call(
        kernel,
        out_shape=(jax.ShapeDtypeStruct((size, size), BF16),) * 2,
        in_specs=[smem, smem, pl.BlockSpec(memory_space=pltpu.VMEM), smem, smem] + [anywhere] * 3,
        out_specs=(anywhere, anywhere),
        scratch_shapes=[
            pltpu.SMEM(meta_shape, I32),
            tuple([pltpu.SMEM(meta_shape, I32)] * 5),
            pltpu.SMEM((3, 2) + meta_shape, I32),
            tile,
            tile,
            tile,
            pltpu.VMEM(weight.shape, BF16),
            pltpu.VMEM(weight.shape, BF16),
            pltpu.VMEM(seeds.shape, F32),
            pltpu.VMEM((length // block, 2 * block, size), BF16),
            pltpu.VMEM((length // block, size, 2 * block), BF16),
            pltpu.VMEM((length // block, 2 * block, size), BF16),
            (tile, tile),
            (pltpu.VMEM((depth, size), BF16),) * 2,
            (pltpu.VMEM((depth, size), BF16),) * 2,
            pltpu.VMEM((3, slots, 2, 8, size), F32),
            pltpu.VMEM((3, slots, size, 128), F32),
            pltpu.VMEM((3, slots, 2, 16, size), BF16),
            pltpu.VMEM((3, slots, size, 128), BF16),
            pltpu.VMEM((3, half_slots) + patch, BF16),
            pltpu.VMEM((3, half_slots) + patch, BF16),
            pltpu.VMEM((3, half_slots) + patch, F32),
            *[pltpu.VMEM((half_slots,) + patch, BF16)] * 8,
            pltpu.VMEM((3, half_slots, slots_uv, block, block), BF16),
            pltpu.VMEM((3, half_slots) + patch, BF16),
            pltpu.VMEM((3, half_slots) + patch, BF16),
            plane,
            plane,
            tile,
            tile,
            dma((4,)),
            dma((2, 5)),
            dma((2, 2)),
            dma((2, 3)),
            dma((2, 3, half_slots)),
            dma((2, half_slots, slots_uv)),
            dma((2, half_slots, slots_uv)),
            dma((2, half_slots, slots_uv)),
            dma((2, half_slots, slots_uv)),
            dma((2, 3, half_slots, slots_uv)),
            dma((2, 1 + EDGES)),
        ],
        compiler_params=pltpu.CompilerParams(
            vmem_limit_bytes=int(56 * 1024 * 1024), collective_id=0, has_side_effects=True
        ),
    )(count, offset, width, bins, used, seeds, sky, weight)
    return pl.pallas_call(
        add_kernel,
        out_shape=jax.ShapeDtypeStruct((size, size), F32),
        in_specs=[anywhere, anywhere],
        out_specs=anywhere,
        scratch_shapes=[tile, tile, plane, dma((3, BANDS))],
        compiler_params=pltpu.CompilerParams(vmem_limit_bytes=56 * 1024 * 1024),
        cost_estimate=pl.CostEstimate(flops=size * size, bytes_accessed=10 * size * size, transcendentals=0),
    )(inner, edge)


def solution(mesh):
    in_specs = (
        P("ty", "tx"),
        P("ty", "tx"),
        P("ty", "tx", None, None),
        P("ty", "tx", None),
        P("ty", "tx", None, None, None),
        P("ty", "tx", None),
        P("ty", "tx", None, None, None, None),
    )
    out_specs = P("ty", "tx")
    return jax.shard_map(shards, mesh=mesh, in_specs=in_specs, out_specs=out_specs, check_vma=False)
```

```python
import functools
import math

import jax
import jax.numpy as jnp
import numpy as np
from jax import lax
from jax.experimental import pallas as pl
from jax.experimental.pallas import tpu as pltpu
from jax.sharding import PartitionSpec as P

F32 = jnp.float32
BF16 = jnp.bfloat16
I32 = jnp.int32
FINE = 32
CHUNK = 256
BANDS = 4
EDGES = 2
FIELDS = 8
MESH = pl.DeviceIdType.MESH


def seed_tables(length, fine):
    pixels = np.arange(length, dtype=np.int64)
    rows = np.concatenate([np.arange(fine), fine * np.arange(length // fine)])
    angle = (rows[:, None] * pixels[None, :] % length) * (2.0 * math.pi / length)
    scale = np.where(np.arange(rows.shape[0]) < fine, 1.0 / math.sqrt(length), 1.0)[:, None]
    return np.stack([np.cos(angle) * scale, np.sin(angle) * scale]).astype(np.float32)


def wide(column, width):
    return jnp.concatenate([column] * (width // column.shape[1]), axis=1)


def kernel(
    count_in, offset_in, width_in, bins_in, used_in, seeds_in, sky_in, weight_in,
    inner_got, edge_got,
    meta_ref, meta_got, meta_all, sky_ref, outer_ref, inner_ref, weight_ref, weight_got,
    seeds_ref, row_tab, flip_tab, col_tab, turn_tab,
    beamed, first, spread, gx_ref, gy_ref, gx_half, gy_half,
    part_send, part_got, totals, raw_send, raw_got, own_send, own_got,
    sum_send, sum_got, back_send, back_got, weights, scaled_own, scaled_par, acc_outer, acc_inner, edge_send, inner_send,
    local_sems, meta_sems, sky_sems, weight_sems, part_sems, raw_sems, own_sems, sum_sems,
    back_sems, par_sems, last_sems,
):
    size = sky_ref.shape[0]
    length = 2 * size
    slots, slots_uv, block = weight_ref.shape[0], weight_ref.shape[1], weight_ref.shape[2]
    half_slots = slots // 2
    ty, tx = lax.axis_index("ty"), lax.axis_index("tx")
    ny, nx = lax.axis_size("ty"), lax.axis_size("tx")
    core = tx % 2
    partner = tx + 1 - 2 * core
    beyond = tx - 1 + 2 * core
    has_up, has_down = ty > 0, ty < ny - 1
    has_beyond = jnp.logical_and(beyond >= 0, beyond < nx)
    has_row = (has_up, has_down)
    row_half = pl.multiple_of((ty % 2) * size, size)
    col_half = pl.multiple_of((1 - core) * size, size)
    to_partner = {"tx": partner}
    to_beyond = {"tx": beyond}
    to_row = ({"ty": ty - 1}, {"ty": ty + 1})
    to_cross = ({"ty": ty - 1, "tx": partner}, {"ty": ty + 1, "tx": partner})
    odd_row = ty % 2
    d_far, d_mate = 2 * odd_row, 2 * (1 - odd_row)
    giving, fed = ty - 2 + 4 * odd_row, ty + 2 - 4 * odd_row
    has_far = jnp.logical_and(giving >= 0, giving < ny)
    has_fed = jnp.logical_and(fed >= 0, fed < ny)
    to_mate, to_giving, to_fed = {"ty": ty + 1 - 2 * odd_row}, {"ty": giving}, {"ty": fed}
    to_far = {"ty": ty - 1 + 2 * odd_row}

    local = [
        pltpu.make_async_copy(source, target, local_sems.at[i])
        for i, (source, target) in enumerate(
            (
                (sky_in, sky_ref),
                (seeds_in, seeds_ref),
                (weight_in, weight_ref),
            )
        )
    ]

    def remote(src, dst, sems, at, target):
        return pltpu.make_async_remote_copy(
            src_ref=src,
            dst_ref=dst,
            send_sem=sems.at[(0,) + at],
            recv_sem=sems.at[(1,) + at],
            device_id=target,
            device_id_type=MESH,
        )

    def meta_copy(slot, target):
        return remote(meta_ref, meta_got[slot], meta_sems, (slot,), target)

    def meta_partner():
        return meta_copy(0, to_partner)

    def meta_send(side):
        return meta_copy(2 - side, to_row[side]), meta_copy(4 - side, to_cross[side])

    def meta_take(side):
        return meta_copy(1 + side, to_row[side]), meta_copy(3 + side, to_cross[side])

    def sky_partner():
        return remote(sky_ref, inner_ref, sky_sems, (0,), to_partner)

    def sky_beyond():
        return remote(sky_ref, outer_ref, sky_sems, (1,), to_beyond)

    def weight_copy():
        return remote(weight_ref, weight_got, weight_sems, (0,), to_partner)

    def part_copy(g, jj):
        return remote(part_send.at[g, jj], part_got.at[g, jj], part_sems, (g, jj), to_partner)

    def raw_copy(target, jj, k):
        return remote(raw_send.at[jj, k], raw_got.at[jj, k], raw_sems, (jj, k), target)

    def own_copy(jj, k):
        return remote(own_send.at[jj, k], own_got.at[jj, k], own_sems, (jj, k), to_mate)

    def sum_copy(jj, k):
        return remote(sum_send.at[jj, k], sum_got.at[jj, k], sum_sems, (jj, k), to_mate)

    def back_copy(target, jj, k):
        return remote(back_send.at[jj, k], back_got.at[jj, k], back_sems, (jj, k), target)

    def weights_mate():
        return remote(weights.at[2], weights.at[1], weight_sems, (1,), to_mate)

    def weights_far():
        return remote(weights.at[2], weights.at[0], weight_sems, (2,), to_far)

    def par_copy(g, jj, k):
        return remote(
            scaled_own.at[g, jj, k], scaled_par.at[g, jj, k], par_sems, (g, jj, k), to_partner
        )

    def last_edge(band):
        rows = slice(band * size // EDGES, (band + 1) * size // EDGES)
        return remote(edge_send.at[rows], edge_got.at[rows], last_sems, (1 + band,), to_beyond)

    def last_inner():
        return remote(inner_send, inner_got, last_sems, (0,), to_partner)

    def no_edge():
        return pltpu.make_async_copy(edge_send, edge_got, local_sems.at[len(local)])

    barrier = pltpu.get_barrier_semaphore()
    pl.semaphore_signal(barrier, inc=1, device_id=to_partner, device_id_type=MESH)

    @pl.when(has_beyond)
    def _():
        pl.semaphore_signal(barrier, inc=1, device_id=to_beyond, device_id_type=MESH)

    for side in range(2):

        @pl.when(has_row[side])
        def _(side=side):
            pl.semaphore_signal(barrier, inc=1, device_id=to_row[side], device_id_type=MESH)
            pl.semaphore_signal(barrier, inc=1, device_id=to_cross[side], device_id_type=MESH)

    for has, target in ((has_far, to_giving), (has_fed, to_fed)):

        @pl.when(has)
        def _(target=target):
            pl.semaphore_signal(barrier, inc=1, device_id=target, device_id_type=MESH)

    for copy in local:
        copy.start()

    lane = lax.broadcasted_iota(I32, (1, slots), 1)
    widths = width_in[...].astype(F32)
    meta_ref[slots, 0] = count_in[0, 0]
    for s in range(slots):
        meta_ref[s, 0] = offset_in[0, s]
        meta_ref[s, 1] = offset_in[1, s]
        meta_ref[s, 2] = jnp.sum(jnp.where(lane == s, widths, 0.0)).astype(I32)
        for k in range(slots_uv):
            for which in range(2):
                meta_ref[s, 3 + 2 * k + which] = bins_in[k, which, s]
        meta_ref[s, 3 + 2 * slots_uv] = used_in[0, s]

    @pl.when(jnp.logical_not(has_beyond))
    def _():
        outer_ref[...] = jnp.zeros_like(outer_ref)
        edge_send[...] = jnp.zeros_like(edge_send)

    with jax.named_scope("barrier"):
        local[0].wait()
        pl.semaphore_wait(
            barrier,
            1 + has_beyond.astype(I32) + 2 * has_up.astype(I32) + 2 * has_down.astype(I32)
            + has_far.astype(I32) + has_fed.astype(I32),
        )

    @pl.when(has_beyond)
    def _():
        sky_beyond().start()

    sky_partner().start()
    meta_partner().start()
    for side in range(2):

        @pl.when(has_row[side])
        def _(side=side):
            for copy in meta_send(side):
                copy.start()

    for copy in local[1:]:
        copy.wait()
    weight_copy().start()

    acc_outer[...] = jnp.zeros_like(acc_outer)
    acc_inner[...] = jnp.zeros_like(acc_inner)

    per_block = block // FINE

    def table(j, carry):
        blk, at = j // per_block, pl.ds(pl.multiple_of((j % per_block) * FINE, FINE), FINE)
        for tab, half in ((row_tab, row_half), (col_tab, col_half)):
            lanes = pl.ds(half, size)
            c, s = seeds_ref[0, pl.ds(FINE + j, 1), lanes], seeds_ref[1, pl.ds(FINE + j, 1), lanes]
            fc, fs = seeds_ref[0, :FINE, lanes], seeds_ref[1, :FINE, lanes]
            tab[blk, at, :] = (fc * c - fs * s).astype(BF16)
            tab[blk, pl.ds(pl.multiple_of(block + (j % per_block) * FINE, FINE), FINE), :] = (fs * c + fc * s).astype(BF16)
        return carry

    with jax.named_scope("tables"):
        lax.fori_loop(0, length // FINE, table, 0)

    def flipped(j, carry):
        at = pl.ds(pl.multiple_of(j * FINE, FINE), FINE)
        for tab, parity in ((flip_tab, odd_row), (turn_tab, 1 - core)):
            row = parity * (size // FINE) + j
            c, s = seeds_ref[0, pl.ds(FINE + row, 1), :], seeds_ref[1, pl.ds(FINE + row, 1), :]
            fc, fs = seeds_ref[0, :FINE, :], seeds_ref[1, :FINE, :]
            cos, sin = (fc * c - fs * s).astype(BF16), (fs * c + fc * s).astype(BF16)
            for blk in range(length // block):
                tab[blk, at, :block] = cos[:, blk * block : (blk + 1) * block]
                tab[blk, at, block:] = sin[:, blk * block : (blk + 1) * block]
        return carry

    with jax.named_scope("flips"):
        lax.fori_loop(0, size // FINE, flipped, 0)

    with jax.named_scope("meta"):
        meta_partner().wait()
        for side in range(2):

            @pl.when(has_row[side])
            def _(side=side):
                for copy in meta_take(side):
                    copy.wait_recv()

            @pl.when(jnp.logical_not(has_row[side]))
            def _(side=side):
                for slot in (1 + side, 3 + side):
                    meta_got[slot][slots, 0] = 0
                    for s in range(slots):
                        for f in range(FIELDS):
                            meta_got[slot][s, f] = 0

    sources = ((meta_got[1], meta_got[3]), (meta_ref, meta_got[0]), (meta_got[2], meta_got[4]))
    even_here = core == 0

    def gather(s, f):
        for d, (same, other) in enumerate(sources):
            a, b = same[s, f], other[s, f]
            meta_all[d, 0, s, f] = jnp.where(even_here, a, b)
            meta_all[d, 1, s, f] = jnp.where(even_here, b, a)

    def gather_slot(s, carry):
        for f in range(FIELDS):
            gather(s, f)
        return carry

    lax.fori_loop(0, slots, gather_slot, 0)
    gather(slots, 0)

    def pointing(d, j):
        even, odd = meta_all[d, 0, slots, 0], meta_all[d, 1, slots, 0]
        from_odd = (j >= even).astype(I32)
        slot = jnp.clip(j - from_odd * even, 0, slots - 1)
        live = j < even + odd
        return from_odd, slot, live

    def bins(d, from_odd, slot, k, which):
        b = meta_all[d, from_odd, slot, 3 + 2 * k + which]
        return jnp.clip(b, 0, length // block - 1)

    def gaussian(shape, axis, shift, decay, live):
        away = lax.broadcasted_iota(I32, shape, axis) + shift
        inside = jnp.logical_and(away >= -size, away < size)
        inside = jnp.logical_and(inside, live)
        away = away.astype(F32)
        if axis == 0:
            fold = away.reshape(shape[0] // 8, 8, shape[1])
            value = jnp.exp(-(fold * fold) * decay[None]).reshape(shape)
        else:
            value = jnp.exp(-(away * away) * wide(decay, shape[1]))
        return jnp.where(inside, value, jnp.zeros(shape, F32))

    def beams(i, carry):
        d, j = i // slots, i % slots
        from_odd, slot, live = pointing(d, j)
        oy, ox = meta_all[d, from_odd, slot, 0], meta_all[d, from_odd, slot, 1]
        width = jnp.full((8, 128), meta_all[d, from_odd, slot, 2], I32).astype(F32)
        decay = 1.0 / (2.0 * width * width)
        gy = gaussian((size, 128), 0, (1 - d) * size - oy, decay, live)
        gy_ref[d, j] = gy
        gy_half[d, j] = gy.astype(BF16)
        outer_at, inner_at = 3 * core - 1, 1 - core
        for i, tile_at in enumerate((outer_at, inner_at)):
            gx = gaussian((8, size), 1, (tile_at - from_odd) * size - ox, decay, live)
            gx_ref[d, j, i] = gx
            gx_half[d, j, i] = jnp.concatenate([gx, gx], axis=0).astype(BF16)
        return carry

    with jax.named_scope("weights"):
        weight_copy().wait_recv()
        for jj in range(half_slots):
            from_odd, slot, live = pointing(1, half_slots * core + jj)
            used = meta_all[1, from_odd, slot, 3 + 2 * slots_uv]
            for k in range(slots_uv):
                weight = jnp.where(from_odd == core, weight_ref[slot, k], weight_got[slot, k])
                weight = weight.astype(F32) * jnp.where(k < used, 1.0, 0.0).astype(F32)
                weights[2, jj, k] = weight.astype(BF16)

        weights_mate().start()

        @pl.when(has_far)
        def _():
            weights_far().start()

    with jax.named_scope("beams"):
        lax.fori_loop(0, 3 * slots, beams, 0)

    def column_table(d, from_odd, slot, k):
        return col_tab[bins(d, from_odd, slot, k, 1)]

    def prepare(d, j, beamed_ref):
        gy = wide(gy_half[d, j], CHUNK)
        for at in range(0, size, CHUNK):
            cols = slice(at, at + CHUNK)
            gx = [jnp.concatenate([gx_half[d, j, i, :, cols]] * (size // 16), axis=0) for i in range(2)]
            value = gx[0] * outer_ref[:, cols] + gx[1] * inner_ref[:, cols]
            beamed_ref[:, cols] = gy * value

    def transform_rows(d, j, beamed_ref, first_ref):
        from_odd, slot, live = pointing(d, j)
        rows = jnp.concatenate(
            [row_tab[bins(d, from_odd, slot, k, 0)] for k in range(slots_uv)], axis=0
        )
        for at in range(0, size, CHUNK):
            cols = slice(at, at + CHUNK)
            first_ref[:, cols] = jnp.dot(
                rows, beamed_ref[:, cols], preferred_element_type=F32
            ).astype(BF16)

    def transform_columns(d, j, first_ref, result_ref):
        from_odd, slot, live = pointing(d, j)
        for k in range(slots_uv):
            both = jnp.dot(
                first_ref[2 * k * block : (2 * k + 2) * block, :],
                turn_tab[bins(d, from_odd, slot, k, 1)],
                preferred_element_type=F32,
            )
            real = both[:block, :block] - both[block:, block:]
            turned = both[:block, block:] + both[block:, :block]
            result_ref[k, :, :block] = real.astype(result_ref.dtype)
            result_ref[k, :, block:] = turned.astype(result_ref.dtype)

    def spread_out(d, j, scaled_ref, spread_ref):
        from_odd, slot, live = pointing(d, j)
        for k in range(slots_uv):
            value = scaled_ref[k]
            real, turned = value[:, :block], value[:, block:]
            square = jnp.concatenate(
                [value, jnp.concatenate([turned, -real], axis=1)], axis=0
            )
            spread_ref[2 * k * block : (2 * k + 2) * block, :] = jnp.dot(
                square, col_tab[bins(d, from_odd, slot, k, 1)], preferred_element_type=F32
            ).astype(BF16)

    def bring_back(d, j, spread_ref, start, stop):
        from_odd, slot, live = pointing(d, j)
        rows = jnp.concatenate(
            [flip_tab[bins(d, from_odd, slot, k, 0), start:stop] for k in range(slots_uv)], axis=1
        )
        gy = wide(gy_ref[d, j, start:stop], CHUNK)
        for at in range(0, size, CHUNK):
            cols = slice(at, at + CHUNK)
            back = gy * jnp.dot(rows, spread_ref[:, cols], preferred_element_type=F32)
            acc_outer[start:stop, cols] += gx_ref[d, j, 0, 0:1, cols] * back
            acc_inner[start:stop, cols] += gx_ref[d, j, 1, 0:1, cols] * back

    mine, theirs = half_slots * core, half_slots * (1 - core)

    with jax.named_scope("sky"):
        sky_partner().wait_recv()

        @pl.when(has_beyond)
        def _():
            sky_beyond().wait_recv()

    def pass_sum(jj, k, value):
        sum_send[jj, k] = value.astype(BF16)
        sum_copy(jj, k).start()

    def row_of(g):
        own = g // 2
        return 2 * (odd_row * (1 - g) + (1 - odd_row) * g) * (1 - own) + own

    def settle(g, jj):
        part_copy(g, jj).wait_recv()
        for k in range(slots_uv):
            totals[g, jj, k] = totals[g, jj, k] + part_got[g, jj, k].astype(F32)

        @pl.when(g == 0)
        def _():
            for k in range(slots_uv):
                raw_send[jj, k] = totals[0, jj, k].astype(BF16)
                raw_copy(to_giving, jj, k).start()

        @pl.when(g == 2)
        def _():
            for k in range(slots_uv):
                own_send[jj, k] = totals[2, jj, k].astype(BF16)
                own_copy(jj, k).start()

        @pl.when(jnp.logical_and(g == 1, jnp.logical_not(has_fed)))
        def _():
            for k in range(slots_uv):
                pass_sum(jj, k, totals[1, jj, k])

    far = has_far.astype(I32)

    def forward_units(s, carry):
        end = s // half_slots
        slot = s * (1 - end)
        units = (
            (2 * (1 - end) * (1 - far) + end, slot),
            ((1 - end) * (1 + far) + end, slot + end),
        )
        for base in (theirs, mine):
            for i, (g, jj) in enumerate(units):
                prepare(row_of(g), base + jj, beamed[i])
            for i, (g, jj) in enumerate(units):
                transform_rows(row_of(g), base + jj, beamed[i], first[i])
            for i, (g, jj) in enumerate(units):
                result = part_send.at[g, jj] if base is theirs else totals.at[g, jj]
                transform_columns(row_of(g), base + jj, first[i], result)
            for g, jj in units:
                if base is theirs:
                    part_copy(g, jj).start()
                else:
                    settle(g, jj)
        return carry

    with jax.named_scope("forward"):
        lax.fori_loop(0, half_slots + far, forward_units, 0)

    def scale(g, jj, k, total):
        weight = weights[g, jj, k].astype(F32)
        scaled_own[g, jj, k] = (total * wide(weight, 2 * block)).astype(BF16)
        par_copy(g, jj, k).start()

    def adjoint_all(g, base, scaled_ref):
        for jj in range(half_slots):
            spread_out(row_of(g), base + jj, scaled_ref.at[g, jj], spread[jj])
        for jj in range(half_slots):
            bring_back(row_of(g), base + jj, spread[jj], 0, size)

    def adjoint_one(g, base, jj, scaled_ref):
        spread_out(row_of(g), base + jj, scaled_ref.at[g, jj], spread[0])
        bring_back(row_of(g), base + jj, spread[0], 0, size)

    def adjoint_theirs(g):
        with jax.named_scope(f"theirs{g}"):
            for jj in range(half_slots):
                for k in range(slots_uv):
                    par_copy(g, jj, k).wait_recv()
            adjoint_all(g, theirs, scaled_par)

    def mate_slot(jj, carry):
        for k in range(slots_uv):
            own_copy(jj, k).wait_recv()
            own_part = own_got[jj, k].astype(F32)

            @pl.when(has_fed)
            def _(k=k):
                back_send[jj, k] = (totals[1, jj, k] + own_got[jj, k].astype(F32)).astype(BF16)
                back_copy(to_fed, jj, k).start()
                raw_copy(to_fed, jj, k).wait_recv()
                both = totals[1, jj, k] + raw_got[jj, k].astype(F32)
                pass_sum(jj, k, both)
                totals[1, jj, k] = both

            scale(1, jj, k, totals[1, jj, k] + own_part)
        adjoint_one(1, mine, jj, scaled_own)
        return carry

    with jax.named_scope("mate"):
        weights_mate().wait_recv()
        lax.fori_loop(0, half_slots, mate_slot, 0)

    adjoint_theirs(1)

    def far_slot(jj, carry):
        for k in range(slots_uv):
            back_copy(to_giving, jj, k).wait_recv()
            scale(0, jj, k, totals[0, jj, k] + back_got[jj, k].astype(F32))
        adjoint_one(0, mine, jj, scaled_own)
        return carry

    @pl.when(has_far)
    def _():
        with jax.named_scope("far"):
            weights_far().wait_recv()
            lax.fori_loop(0, half_slots, far_slot, 0)

    def own_slot(jj):
        with jax.named_scope(f"own{jj}"):
            for k in range(slots_uv):
                sum_copy(jj, k).wait_recv()
                scale(2, jj, k, totals[2, jj, k] + sum_got[jj, k].astype(F32))
            adjoint_one(2, mine, jj, scaled_own)

    own_slot(0)

    @pl.when(has_far)
    def _():
        adjoint_theirs(0)

    for jj in range(half_slots - 1):
        for k in range(slots_uv):
            par_copy(2, jj, k).wait_recv()
        adjoint_one(2, theirs, jj, scaled_par)
        own_slot(jj + 1)

    with jax.named_scope("final"):
        jj = half_slots - 1
        for k in range(slots_uv):
            par_copy(2, jj, k).wait_recv()
        spread_out(1, theirs + jj, scaled_par.at[2, jj], spread[0])
        for band in range(EDGES):
            start, stop = band * size // EDGES, (band + 1) * size // EDGES
            bring_back(1, theirs + jj, spread[0], start, stop)

            @pl.when(has_beyond)
            def _(band=band, start=start, stop=stop):
                edge_send[start:stop] = acc_outer[start:stop].astype(BF16)
                last_edge(band).start()

    inner_send[...] = acc_inner[...].astype(BF16)
    last_inner().start()

    @pl.when(jnp.logical_not(has_beyond))
    def _():
        no_edge().start()

    sky_partner().wait_send()
    weight_copy().wait_send()

    @pl.when(has_beyond)
    def _():
        sky_beyond().wait_send()

    for side in range(2):

        @pl.when(has_row[side])
        def _(side=side):
            for copy in meta_send(side):
                copy.wait_send()

    for jj in range(half_slots):
        for g in (1, 2):
            part_copy(g, jj).wait_send()
            for k in range(slots_uv):
                par_copy(g, jj, k).wait_send()
        for k in range(slots_uv):
            own_copy(jj, k).wait_send()
            sum_copy(jj, k).wait_send()

            @pl.when(has_fed)
            def _(jj=jj, k=k):
                back_copy(to_fed, jj, k).wait_send()

        @pl.when(has_far)
        def _(jj=jj):
            part_copy(0, jj).wait_send()
            for k in range(slots_uv):
                par_copy(0, jj, k).wait_send()
                raw_copy(to_giving, jj, k).wait_send()

    weights_mate().wait_send()

    @pl.when(has_far)
    def _():
        weights_far().wait_send()

    with jax.named_scope("last"):
        last_inner().wait()

        @pl.when(has_beyond)
        def _():
            for band in range(EDGES):
                last_edge(band).wait()

        @pl.when(jnp.logical_not(has_beyond))
        def _():
            no_edge().wait()


def add_kernel(inner_hbm, edge_hbm, out_hbm, inner_ref, edge_ref, out_ref, sems):
    band = out_ref.shape[0] // BANDS
    bands = [slice(i * band, (i + 1) * band) for i in range(BANDS)]
    moves = [
        [
            pltpu.make_async_copy(inner_hbm.at[rows], inner_ref.at[rows], sems.at[0, i]),
            pltpu.make_async_copy(edge_hbm.at[rows], edge_ref.at[rows], sems.at[1, i]),
            pltpu.make_async_copy(out_ref.at[rows], out_hbm.at[rows], sems.at[2, i]),
        ]
        for i, rows in enumerate(bands)
    ]
    for inner, edge, out in moves:
        inner.start()
        edge.start()
    for rows, (inner, edge, out) in zip(bands, moves):
        inner.wait()
        edge.wait()
        out_ref[rows, :] = inner_ref[rows, :].astype(F32) + edge_ref[rows, :].astype(F32)
        out.start()
    for inner, edge, out in moves:
        out.wait()


def shards(sky, point_count, point_offset, beam_width, uv_bins, uv_count, uv_weight):
    size = sky.shape[0]
    length = 2 * size
    slots, slots_uv, block = uv_weight.shape[2], uv_weight.shape[3], uv_weight.shape[4]
    half_slots = slots // 2
    depth = 2 * slots_uv * block
    seeds = seed_tables(length, FINE)
    count = point_count.reshape(1, 1)
    offset = jnp.transpose(point_offset, (0, 1, 3, 2)).reshape(2, slots)
    width = beam_width.reshape(1, slots)
    bins = jnp.transpose(uv_bins, (0, 1, 3, 4, 2)).reshape(slots_uv, 2, slots)
    used = uv_count.reshape(1, slots)
    weight = uv_weight.reshape(slots, slots_uv, block, block)

    dma = pltpu.SemaphoreType.DMA
    meta_shape = (slots + 1, FIELDS)
    tile = pltpu.VMEM((size, size), BF16)
    plane = pltpu.VMEM((size, size), F32)
    patch = (slots_uv, block, 2 * block)
    smem, anywhere = pl.BlockSpec(memory_space=pltpu.SMEM), pl.BlockSpec(memory_space=pl.ANY)
    inner, edge = pl.pallas_call(
        kernel,
        out_shape=(jax.ShapeDtypeStruct((size, size), BF16),) * 2,
        in_specs=[smem, smem, pl.BlockSpec(memory_space=pltpu.VMEM), smem, smem] + [anywhere] * 3,
        out_specs=(anywhere, anywhere),
        scratch_shapes=[
            pltpu.SMEM(meta_shape, I32),
            tuple([pltpu.SMEM(meta_shape, I32)] * 5),
            pltpu.SMEM((3, 2) + meta_shape, I32),
            tile,
            tile,
            tile,
            pltpu.VMEM(weight.shape, BF16),
            pltpu.VMEM(weight.shape, BF16),
            pltpu.VMEM(seeds.shape, F32),
            pltpu.VMEM((length // block, 2 * block, size), BF16),
            pltpu.VMEM((length // block, size, 2 * block), BF16),
            pltpu.VMEM((length // block, 2 * block, size), BF16),
            pltpu.VMEM((length // block, size, 2 * block), BF16),
            (tile, tile),
            (pltpu.VMEM((depth, size), BF16),) * 2,
            (pltpu.VMEM((depth, size), BF16),) * half_slots,
            pltpu.VMEM((3, slots, 2, 8, size), F32),
            pltpu.VMEM((3, slots, size, 128), F32),
            pltpu.VMEM((3, slots, 2, 16, size), BF16),
            pltpu.VMEM((3, slots, size, 128), BF16),
            pltpu.VMEM((3, half_slots) + patch, BF16),
            pltpu.VMEM((3, half_slots) + patch, BF16),
            pltpu.VMEM((3, half_slots) + patch, F32),
            *[pltpu.VMEM((half_slots,) + patch, BF16)] * 8,
            pltpu.VMEM((3, half_slots, slots_uv, block, block), BF16),
            pltpu.VMEM((3, half_slots) + patch, BF16),
            pltpu.VMEM((3, half_slots) + patch, BF16),
            plane,
            plane,
            tile,
            tile,
            dma((4,)),
            dma((2, 5)),
            dma((2, 2)),
            dma((2, 3)),
            dma((2, 3, half_slots)),
            dma((2, half_slots, slots_uv)),
            dma((2, half_slots, slots_uv)),
            dma((2, half_slots, slots_uv)),
            dma((2, half_slots, slots_uv)),
            dma((2, 3, half_slots, slots_uv)),
            dma((2, 1 + EDGES)),
        ],
        compiler_params=pltpu.CompilerParams(
            vmem_limit_bytes=int(56 * 1024 * 1024), collective_id=0, has_side_effects=True
        ),
    )(count, offset, width, bins, used, seeds, sky, weight)
    return pl.pallas_call(
        add_kernel,
        out_shape=jax.ShapeDtypeStruct((size, size), F32),
        in_specs=[anywhere, anywhere],
        out_specs=anywhere,
        scratch_shapes=[tile, tile, plane, dma((3, BANDS))],
        compiler_params=pltpu.CompilerParams(vmem_limit_bytes=56 * 1024 * 1024),
        cost_estimate=pl.CostEstimate(flops=size * size, bytes_accessed=10 * size * size, transcendentals=0),
    )(inner, edge)


def solution(mesh):
    in_specs = (
        P("ty", "tx"),
        P("ty", "tx"),
        P("ty", "tx", None, None),
        P("ty", "tx", None),
        P("ty", "tx", None, None, None),
        P("ty", "tx", None),
        P("ty", "tx", None, None, None, None),
    )
    out_specs = P("ty", "tx")
    return jax.shard_map(shards, mesh=mesh, in_specs=in_specs, out_specs=out_specs, check_vma=False)
```

```python
import functools
import math

import jax
import jax.numpy as jnp
import numpy as np
from jax import lax
from jax.experimental import pallas as pl
from jax.experimental.pallas import tpu as pltpu
from jax.sharding import PartitionSpec as P

F32 = jnp.float32
BF16 = jnp.bfloat16
I32 = jnp.int32
FINE = 32
CHUNK = 256
BANDS = 4
EDGES = 2
FIELDS = 8
MESH = pl.DeviceIdType.MESH


def seed_tables(length, fine):
    pixels = np.arange(length, dtype=np.int64)
    rows = np.concatenate([np.arange(fine), fine * np.arange(length // fine)])
    angle = (rows[:, None] * pixels[None, :] % length) * (2.0 * math.pi / length)
    scale = np.where(np.arange(rows.shape[0]) < fine, 1.0 / math.sqrt(length), 1.0)[:, None]
    return np.stack([np.cos(angle) * scale, np.sin(angle) * scale]).astype(np.float32)


def wide(column, width):
    return jnp.concatenate([column] * (width // column.shape[1]), axis=1)


def kernel(
    count_hbm, offset_hbm, width_hbm, bins_hbm, used_hbm, seeds_in, sky_in, weight_in,
    inner_got, edge_got,
    count_in, offset_in, width_in, bins_in, used_in,
    meta_ref, meta_got, meta_all, sky_ref, outer_ref, inner_ref, weight_ref, weight_got,
    seeds_ref, row_tab, flip_tab, col_tab, turn_tab,
    beamed, first, spread, gx_ref, gy_ref, gx_half, gy_half,
    part_send, part_got, totals, raw_send, raw_got, own_send, own_got,
    sum_send, sum_got, back_send, back_got, weights, scaled_own, scaled_par, acc_outer, acc_inner, edge_send, inner_send,
    local_sems, meta_sems, sky_sems, weight_sems, part_sems, raw_sems, own_sems, sum_sems,
    back_sems, par_sems, last_sems,
):
    size = sky_ref.shape[0]
    length = 2 * size
    slots, slots_uv, block = weight_ref.shape[0], weight_ref.shape[1], weight_ref.shape[2]
    half_slots = slots // 2
    ty, tx = lax.axis_index("ty"), lax.axis_index("tx")
    ny, nx = lax.axis_size("ty"), lax.axis_size("tx")
    core = tx % 2
    partner = tx + 1 - 2 * core
    beyond = tx - 1 + 2 * core
    has_up, has_down = ty > 0, ty < ny - 1
    has_beyond = jnp.logical_and(beyond >= 0, beyond < nx)
    has_row = (has_up, has_down)
    row_half = pl.multiple_of((ty % 2) * size, size)
    col_half = pl.multiple_of((1 - core) * size, size)
    to_partner = {"tx": partner}
    to_beyond = {"tx": beyond}
    to_row = ({"ty": ty - 1}, {"ty": ty + 1})
    to_cross = ({"ty": ty - 1, "tx": partner}, {"ty": ty + 1, "tx": partner})
    odd_row = ty % 2
    d_far, d_mate = 2 * odd_row, 2 * (1 - odd_row)
    giving, fed = ty - 2 + 4 * odd_row, ty + 2 - 4 * odd_row
    has_far = jnp.logical_and(giving >= 0, giving < ny)
    has_fed = jnp.logical_and(fed >= 0, fed < ny)
    to_mate, to_giving, to_fed = {"ty": ty + 1 - 2 * odd_row}, {"ty": giving}, {"ty": fed}
    to_far = {"ty": ty - 1 + 2 * odd_row}

    local = [
        pltpu.make_async_copy(source, target, local_sems.at[i])
        for i, (source, target) in enumerate(
            (
                (sky_in, sky_ref),
                (count_hbm, count_in),
                (offset_hbm, offset_in),
                (width_hbm, width_in),
                (bins_hbm, bins_in),
                (used_hbm, used_in),
                (seeds_in, seeds_ref),
                (weight_in, weight_ref),
            )
        )
    ]

    def remote(src, dst, sems, at, target):
        return pltpu.make_async_remote_copy(
            src_ref=src,
            dst_ref=dst,
            send_sem=sems.at[(0,) + at],
            recv_sem=sems.at[(1,) + at],
            device_id=target,
            device_id_type=MESH,
        )

    def meta_copy(slot, target):
        return remote(meta_ref, meta_got[slot], meta_sems, (slot,), target)

    def meta_partner():
        return meta_copy(0, to_partner)

    def meta_send(side):
        return meta_copy(2 - side, to_row[side]), meta_copy(4 - side, to_cross[side])

    def meta_take(side):
        return meta_copy(1 + side, to_row[side]), meta_copy(3 + side, to_cross[side])

    def sky_partner():
        return remote(sky_ref, inner_ref, sky_sems, (0,), to_partner)

    def sky_beyond():
        return remote(sky_ref, outer_ref, sky_sems, (1,), to_beyond)

    def weight_copy():
        return remote(weight_ref, weight_got, weight_sems, (0,), to_partner)

    def part_copy(g, jj):
        return remote(part_send.at[g, jj], part_got.at[g, jj], part_sems, (g, jj), to_partner)

    def raw_copy(target, jj, k):
        return remote(raw_send.at[jj, k], raw_got.at[jj, k], raw_sems, (jj, k), target)

    def own_copy(jj, k):
        return remote(own_send.at[jj, k], own_got.at[jj, k], own_sems, (jj, k), to_mate)

    def sum_copy(jj, k):
        return remote(sum_send.at[jj, k], sum_got.at[jj, k], sum_sems, (jj, k), to_mate)

    def back_copy(target, jj, k):
        return remote(back_send.at[jj, k], back_got.at[jj, k], back_sems, (jj, k), target)

    def weights_mate():
        return remote(weights.at[2], weights.at[1], weight_sems, (1,), to_mate)

    def weights_far():
        return remote(weights.at[2], weights.at[0], weight_sems, (2,), to_far)

    def par_copy(g, jj, k):
        return remote(
            scaled_own.at[g, jj, k], scaled_par.at[g, jj, k], par_sems, (g, jj, k), to_partner
        )

    def last_edge(band):
        rows = slice(band * size // EDGES, (band + 1) * size // EDGES)
        return remote(edge_send.at[rows], edge_got.at[rows], last_sems, (1 + band,), to_beyond)

    def last_inner():
        return remote(inner_send, inner_got, last_sems, (0,), to_partner)

    def no_edge():
        return pltpu.make_async_copy(edge_send, edge_got, local_sems.at[len(local)])

    barrier = pltpu.get_barrier_semaphore()
    pl.semaphore_signal(barrier, inc=1, device_id=to_partner, device_id_type=MESH)

    @pl.when(has_beyond)
    def _():
        pl.semaphore_signal(barrier, inc=1, device_id=to_beyond, device_id_type=MESH)

    for side in range(2):

        @pl.when(has_row[side])
        def _(side=side):
            pl.semaphore_signal(barrier, inc=1, device_id=to_row[side], device_id_type=MESH)
            pl.semaphore_signal(barrier, inc=1, device_id=to_cross[side], device_id_type=MESH)

    for has, target in ((has_far, to_giving), (has_fed, to_fed)):

        @pl.when(has)
        def _(target=target):
            pl.semaphore_signal(barrier, inc=1, device_id=target, device_id_type=MESH)

    for copy in local:
        copy.start()

    for copy in local[1:6]:
        copy.wait()

    lane = lax.broadcasted_iota(I32, (1, slots), 1)
    widths = width_in[...].astype(F32)
    meta_ref[slots, 0] = count_in[0, 0]
    for s in range(slots):
        meta_ref[s, 0] = offset_in[0, s]
        meta_ref[s, 1] = offset_in[1, s]
        meta_ref[s, 2] = jnp.sum(jnp.where(lane == s, widths, 0.0)).astype(I32)
        for k in range(slots_uv):
            for which in range(2):
                meta_ref[s, 3 + 2 * k + which] = bins_in[k, which, s]
        meta_ref[s, 3 + 2 * slots_uv] = used_in[0, s]

    @pl.when(jnp.logical_not(has_beyond))
    def _():
        outer_ref[...] = jnp.zeros_like(outer_ref)
        edge_send[...] = jnp.zeros_like(edge_send)

    with jax.named_scope("barrier"):
        local[0].wait()
        pl.semaphore_wait(
            barrier,
            1 + has_beyond.astype(I32) + 2 * has_up.astype(I32) + 2 * has_down.astype(I32)
            + has_far.astype(I32) + has_fed.astype(I32),
        )

    @pl.when(has_beyond)
    def _():
        sky_beyond().start()

    sky_partner().start()
    meta_partner().start()
    for side in range(2):

        @pl.when(has_row[side])
        def _(side=side):
            for copy in meta_send(side):
                copy.start()

    for copy in local[6:]:
        copy.wait()
    weight_copy().start()

    acc_outer[...] = jnp.zeros_like(acc_outer)
    acc_inner[...] = jnp.zeros_like(acc_inner)

    per_block = block // FINE

    def table(j, carry):
        blk, at = j // per_block, pl.ds(pl.multiple_of((j % per_block) * FINE, FINE), FINE)
        for tab, half in ((row_tab, row_half), (col_tab, col_half)):
            lanes = pl.ds(half, size)
            c, s = seeds_ref[0, pl.ds(FINE + j, 1), lanes], seeds_ref[1, pl.ds(FINE + j, 1), lanes]
            fc, fs = seeds_ref[0, :FINE, lanes], seeds_ref[1, :FINE, lanes]
            tab[blk, at, :] = (fc * c - fs * s).astype(BF16)
            tab[blk, pl.ds(pl.multiple_of(block + (j % per_block) * FINE, FINE), FINE), :] = (fs * c + fc * s).astype(BF16)
        return carry

    with jax.named_scope("tables"):
        lax.fori_loop(0, length // FINE, table, 0)

    def flipped(j, carry):
        at = pl.ds(pl.multiple_of(j * FINE, FINE), FINE)
        for tab, parity in ((flip_tab, odd_row), (turn_tab, 1 - core)):
            row = parity * (size // FINE) + j
            c, s = seeds_ref[0, pl.ds(FINE + row, 1), :], seeds_ref[1, pl.ds(FINE + row, 1), :]
            fc, fs = seeds_ref[0, :FINE, :], seeds_ref[1, :FINE, :]
            cos, sin = (fc * c - fs * s).astype(BF16), (fs * c + fc * s).astype(BF16)
            for blk in range(length // block):
                tab[blk, at, :block] = cos[:, blk * block : (blk + 1) * block]
                tab[blk, at, block:] = sin[:, blk * block : (blk + 1) * block]
        return carry

    with jax.named_scope("flips"):
        lax.fori_loop(0, size // FINE, flipped, 0)

    with jax.named_scope("meta"):
        meta_partner().wait()
        for side in range(2):

            @pl.when(has_row[side])
            def _(side=side):
                for copy in meta_take(side):
                    copy.wait_recv()

            @pl.when(jnp.logical_not(has_row[side]))
            def _(side=side):
                for slot in (1 + side, 3 + side):
                    meta_got[slot][slots, 0] = 0
                    for s in range(slots):
                        for f in range(FIELDS):
                            meta_got[slot][s, f] = 0

    sources = ((meta_got[1], meta_got[3]), (meta_ref, meta_got[0]), (meta_got[2], meta_got[4]))
    even_here = core == 0

    def gather(s, f):
        for d, (same, other) in enumerate(sources):
            a, b = same[s, f], other[s, f]
            meta_all[d, 0, s, f] = jnp.where(even_here, a, b)
            meta_all[d, 1, s, f] = jnp.where(even_here, b, a)

    def gather_slot(s, carry):
        for f in range(FIELDS):
            gather(s, f)
        return carry

    lax.fori_loop(0, slots, gather_slot, 0)
    gather(slots, 0)

    def pointing(d, j):
        even, odd = meta_all[d, 0, slots, 0], meta_all[d, 1, slots, 0]
        from_odd = (j >= even).astype(I32)
        slot = jnp.clip(j - from_odd * even, 0, slots - 1)
        live = j < even + odd
        return from_odd, slot, live

    def bins(d, from_odd, slot, k, which):
        b = meta_all[d, from_odd, slot, 3 + 2 * k + which]
        return jnp.clip(b, 0, length // block - 1)

    def gaussian(shape, axis, shift, decay, live):
        away = lax.broadcasted_iota(I32, shape, axis) + shift
        inside = jnp.logical_and(away >= -size, away < size)
        inside = jnp.logical_and(inside, live)
        away = away.astype(F32)
        if axis == 0:
            fold = away.reshape(shape[0] // 8, 8, shape[1])
            value = jnp.exp(-(fold * fold) * decay[None]).reshape(shape)
        else:
            value = jnp.exp(-(away * away) * wide(decay, shape[1]))
        return jnp.where(inside, value, jnp.zeros(shape, F32))

    def beams(i, carry):
        d, j = i // slots, i % slots
        from_odd, slot, live = pointing(d, j)
        oy, ox = meta_all[d, from_odd, slot, 0], meta_all[d, from_odd, slot, 1]
        width = jnp.full((8, 128), meta_all[d, from_odd, slot, 2], I32).astype(F32)
        decay = 1.0 / (2.0 * width * width)
        gy = gaussian((size, 128), 0, (1 - d) * size - oy, decay, live)
        gy_ref[d, j] = gy
        gy_half[d, j] = gy.astype(BF16)
        outer_at, inner_at = 3 * core - 1, 1 - core
        for i, tile_at in enumerate((outer_at, inner_at)):
            gx = gaussian((8, size), 1, (tile_at - from_odd) * size - ox, decay, live)
            gx_ref[d, j, i] = gx
            gx_half[d, j, i] = jnp.concatenate([gx, gx], axis=0).astype(BF16)
        return carry

    with jax.named_scope("weights"):
        weight_copy().wait_recv()
        for jj in range(half_slots):
            from_odd, slot, live = pointing(1, half_slots * core + jj)
            used = meta_all[1, from_odd, slot, 3 + 2 * slots_uv]
            for k in range(slots_uv):
                weight = jnp.where(from_odd == core, weight_ref[slot, k], weight_got[slot, k])
                weight = weight.astype(F32) * jnp.where(k < used, 1.0, 0.0).astype(F32)
                weights[2, jj, k] = weight.astype(BF16)

        weights_mate().start()

        @pl.when(has_far)
        def _():
            weights_far().start()

    with jax.named_scope("beams"):
        lax.fori_loop(0, 3 * slots, beams, 0)

    def column_table(d, from_odd, slot, k):
        return col_tab[bins(d, from_odd, slot, k, 1)]

    def prepare(d, j, beamed_ref):
        gy = wide(gy_half[d, j], CHUNK)
        for at in range(0, size, CHUNK):
            cols = slice(at, at + CHUNK)
            gx = [jnp.concatenate([gx_half[d, j, i, :, cols]] * (size // 16), axis=0) for i in range(2)]
            value = gx[0] * outer_ref[:, cols] + gx[1] * inner_ref[:, cols]
            beamed_ref[:, cols] = gy * value

    def transform_rows(d, j, beamed_ref, first_ref):
        from_odd, slot, live = pointing(d, j)
        rows = jnp.concatenate(
            [row_tab[bins(d, from_odd, slot, k, 0)] for k in range(slots_uv)], axis=0
        )
        for at in range(0, size, CHUNK):
            cols = slice(at, at + CHUNK)
            first_ref[:, cols] = jnp.dot(
                rows, beamed_ref[:, cols], preferred_element_type=F32
            ).astype(BF16)

    def transform_columns(d, j, first_ref, result_ref):
        from_odd, slot, live = pointing(d, j)
        for k in range(slots_uv):
            both = jnp.dot(
                first_ref[2 * k * block : (2 * k + 2) * block, :],
                turn_tab[bins(d, from_odd, slot, k, 1)],
                preferred_element_type=F32,
            )
            real = both[:block, :block] - both[block:, block:]
            turned = both[:block, block:] + both[block:, :block]
            result_ref[k, :, :block] = real.astype(result_ref.dtype)
            result_ref[k, :, block:] = turned.astype(result_ref.dtype)

    def spread_out(d, j, scaled_ref, spread_ref):
        from_odd, slot, live = pointing(d, j)
        for k in range(slots_uv):
            value = scaled_ref[k]
            real, turned = value[:, :block], value[:, block:]
            square = jnp.concatenate(
                [value, jnp.concatenate([turned, -real], axis=1)], axis=0
            )
            spread_ref[2 * k * block : (2 * k + 2) * block, :] = jnp.dot(
                square, col_tab[bins(d, from_odd, slot, k, 1)], preferred_element_type=F32
            ).astype(BF16)

    def bring_back(d, j, spread_ref, start, stop):
        from_odd, slot, live = pointing(d, j)
        rows = jnp.concatenate(
            [flip_tab[bins(d, from_odd, slot, k, 0), start:stop] for k in range(slots_uv)], axis=1
        )
        gy = wide(gy_ref[d, j, start:stop], CHUNK)
        for at in range(0, size, CHUNK):
            cols = slice(at, at + CHUNK)
            back = gy * jnp.dot(rows, spread_ref[:, cols], preferred_element_type=F32)
            acc_outer[start:stop, cols] += gx_ref[d, j, 0, 0:1, cols] * back
            acc_inner[start:stop, cols] += gx_ref[d, j, 1, 0:1, cols] * back

    mine, theirs = half_slots * core, half_slots * (1 - core)

    with jax.named_scope("sky"):
        sky_partner().wait_recv()

        @pl.when(has_beyond)
        def _():
            sky_beyond().wait_recv()

    def pass_sum(jj, k, value):
        sum_send[jj, k] = value.astype(BF16)
        sum_copy(jj, k).start()

    def row_of(g):
        own = g // 2
        return 2 * (odd_row * (1 - g) + (1 - odd_row) * g) * (1 - own) + own

    def settle(g, jj):
        part_copy(g, jj).wait_recv()
        for k in range(slots_uv):
            totals[g, jj, k] = totals[g, jj, k] + part_got[g, jj, k].astype(F32)

        @pl.when(g == 0)
        def _():
            for k in range(slots_uv):
                raw_send[jj, k] = totals[0, jj, k].astype(BF16)
                raw_copy(to_giving, jj, k).start()

        @pl.when(g == 2)
        def _():
            for k in range(slots_uv):
                own_send[jj, k] = totals[2, jj, k].astype(BF16)
                own_copy(jj, k).start()

        @pl.when(jnp.logical_and(g == 1, jnp.logical_not(has_fed)))
        def _():
            for k in range(slots_uv):
                pass_sum(jj, k, totals[1, jj, k])

    far = has_far.astype(I32)

    def forward_units(s, carry):
        end = s // half_slots
        slot = s * (1 - end)
        units = (
            (2 * (1 - end) * (1 - far) + end, slot),
            ((1 - end) * (1 + far) + end, slot + end),
        )
        for base in (theirs, mine):
            for i, (g, jj) in enumerate(units):
                prepare(row_of(g), base + jj, beamed[i])
            for i, (g, jj) in enumerate(units):
                transform_rows(row_of(g), base + jj, beamed[i], first[i])
            for i, (g, jj) in enumerate(units):
                result = part_send.at[g, jj] if base is theirs else totals.at[g, jj]
                transform_columns(row_of(g), base + jj, first[i], result)
            for g, jj in units:
                if base is theirs:
                    part_copy(g, jj).start()
                else:
                    settle(g, jj)
        return carry

    with jax.named_scope("forward"):
        lax.fori_loop(0, half_slots + far, forward_units, 0)

    def scale(g, jj, k, total):
        weight = weights[g, jj, k].astype(F32)
        scaled_own[g, jj, k] = (total * wide(weight, 2 * block)).astype(BF16)
        par_copy(g, jj, k).start()

    def adjoint_all(g, base, scaled_ref):
        for jj in range(half_slots):
            spread_out(row_of(g), base + jj, scaled_ref.at[g, jj], spread[jj])
        for jj in range(half_slots):
            bring_back(row_of(g), base + jj, spread[jj], 0, size)

    def adjoint_one(g, base, jj, scaled_ref):
        spread_out(row_of(g), base + jj, scaled_ref.at[g, jj], spread[0])
        bring_back(row_of(g), base + jj, spread[0], 0, size)

    def adjoint_theirs(g):
        with jax.named_scope(f"theirs{g}"):
            for jj in range(half_slots):
                for k in range(slots_uv):
                    par_copy(g, jj, k).wait_recv()
            adjoint_all(g, theirs, scaled_par)

    def mate_slot(jj, carry):
        for k in range(slots_uv):
            own_copy(jj, k).wait_recv()
            own_part = own_got[jj, k].astype(F32)

            @pl.when(has_fed)
            def _(k=k):
                back_send[jj, k] = (totals[1, jj, k] + own_got[jj, k].astype(F32)).astype(BF16)
                back_copy(to_fed, jj, k).start()
                raw_copy(to_fed, jj, k).wait_recv()
                both = totals[1, jj, k] + raw_got[jj, k].astype(F32)
                pass_sum(jj, k, both)
                totals[1, jj, k] = both

            scale(1, jj, k, totals[1, jj, k] + own_part)
        adjoint_one(1, mine, jj, scaled_own)
        return carry

    with jax.named_scope("mate"):
        weights_mate().wait_recv()
        lax.fori_loop(0, half_slots, mate_slot, 0)

    adjoint_theirs(1)

    def far_slot(jj, carry):
        for k in range(slots_uv):
            back_copy(to_giving, jj, k).wait_recv()
            scale(0, jj, k, totals[0, jj, k] + back_got[jj, k].astype(F32))
        adjoint_one(0, mine, jj, scaled_own)
        return carry

    @pl.when(has_far)
    def _():
        with jax.named_scope("far"):
            weights_far().wait_recv()
            lax.fori_loop(0, half_slots, far_slot, 0)

    def own_slot(jj):
        with jax.named_scope(f"own{jj}"):
            for k in range(slots_uv):
                sum_copy(jj, k).wait_recv()
                scale(2, jj, k, totals[2, jj, k] + sum_got[jj, k].astype(F32))
            adjoint_one(2, mine, jj, scaled_own)

    own_slot(0)

    @pl.when(has_far)
    def _():
        adjoint_theirs(0)

    for jj in range(half_slots - 1):
        for k in range(slots_uv):
            par_copy(2, jj, k).wait_recv()
        adjoint_one(2, theirs, jj, scaled_par)
        own_slot(jj + 1)

    with jax.named_scope("final"):
        jj = half_slots - 1
        for k in range(slots_uv):
            par_copy(2, jj, k).wait_recv()
        spread_out(1, theirs + jj, scaled_par.at[2, jj], spread[0])
        for band in range(EDGES):
            start, stop = band * size // EDGES, (band + 1) * size // EDGES
            bring_back(1, theirs + jj, spread[0], start, stop)

            @pl.when(has_beyond)
            def _(band=band, start=start, stop=stop):
                edge_send[start:stop] = acc_outer[start:stop].astype(BF16)
                last_edge(band).start()

    inner_send[...] = acc_inner[...].astype(BF16)
    last_inner().start()

    @pl.when(jnp.logical_not(has_beyond))
    def _():
        no_edge().start()

    sky_partner().wait_send()
    weight_copy().wait_send()

    @pl.when(has_beyond)
    def _():
        sky_beyond().wait_send()

    for side in range(2):

        @pl.when(has_row[side])
        def _(side=side):
            for copy in meta_send(side):
                copy.wait_send()

    for jj in range(half_slots):
        for g in (1, 2):
            part_copy(g, jj).wait_send()
            for k in range(slots_uv):
                par_copy(g, jj, k).wait_send()
        for k in range(slots_uv):
            own_copy(jj, k).wait_send()
            sum_copy(jj, k).wait_send()

            @pl.when(has_fed)
            def _(jj=jj, k=k):
                back_copy(to_fed, jj, k).wait_send()

        @pl.when(has_far)
        def _(jj=jj):
            part_copy(0, jj).wait_send()
            for k in range(slots_uv):
                par_copy(0, jj, k).wait_send()
                raw_copy(to_giving, jj, k).wait_send()

    weights_mate().wait_send()

    @pl.when(has_far)
    def _():
        weights_far().wait_send()

    with jax.named_scope("last"):
        last_inner().wait()

        @pl.when(has_beyond)
        def _():
            for band in range(EDGES):
                last_edge(band).wait()

        @pl.when(jnp.logical_not(has_beyond))
        def _():
            no_edge().wait()


def add_kernel(inner_hbm, edge_hbm, out_hbm, inner_ref, edge_ref, out_ref, sems):
    band = out_ref.shape[0] // BANDS
    bands = [slice(i * band, (i + 1) * band) for i in range(BANDS)]
    moves = [
        [
            pltpu.make_async_copy(inner_hbm.at[rows], inner_ref.at[rows], sems.at[0, i]),
            pltpu.make_async_copy(edge_hbm.at[rows], edge_ref.at[rows], sems.at[1, i]),
            pltpu.make_async_copy(out_ref.at[rows], out_hbm.at[rows], sems.at[2, i]),
        ]
        for i, rows in enumerate(bands)
    ]
    for inner, edge, out in moves:
        inner.start()
        edge.start()
    for rows, (inner, edge, out) in zip(bands, moves):
        inner.wait()
        edge.wait()
        out_ref[rows, :] = inner_ref[rows, :].astype(F32) + edge_ref[rows, :].astype(F32)
        out.start()
    for inner, edge, out in moves:
        out.wait()


def shards(sky, point_count, point_offset, beam_width, uv_bins, uv_count, uv_weight):
    size = sky.shape[0]
    length = 2 * size
    slots, slots_uv, block = uv_weight.shape[2], uv_weight.shape[3], uv_weight.shape[4]
    half_slots = slots // 2
    depth = 2 * slots_uv * block
    seeds = seed_tables(length, FINE)
    count = point_count.reshape(1, 1)
    offset = jnp.transpose(point_offset, (0, 1, 3, 2)).reshape(2, slots)
    width = beam_width.reshape(1, slots)
    bins = jnp.transpose(uv_bins, (0, 1, 3, 4, 2)).reshape(slots_uv, 2, slots)
    used = uv_count.reshape(1, slots)
    weight = uv_weight.reshape(slots, slots_uv, block, block)

    dma = pltpu.SemaphoreType.DMA
    meta_shape = (slots + 1, FIELDS)
    tile = pltpu.VMEM((size, size), BF16)
    plane = pltpu.VMEM((size, size), F32)
    patch = (slots_uv, block, 2 * block)
    anywhere = pl.BlockSpec(memory_space=pl.ANY)
    inner, edge = pl.pallas_call(
        kernel,
        out_shape=(jax.ShapeDtypeStruct((size, size), BF16),) * 2,
        in_specs=[anywhere] * 8,
        out_specs=(anywhere, anywhere),
        scratch_shapes=[
            pltpu.SMEM(count.shape, I32),
            pltpu.SMEM(offset.shape, I32),
            pltpu.VMEM(width.shape, BF16),
            pltpu.SMEM(bins.shape, I32),
            pltpu.SMEM(used.shape, I32),
            pltpu.SMEM(meta_shape, I32),
            tuple([pltpu.SMEM(meta_shape, I32)] * 5),
            pltpu.SMEM((3, 2) + meta_shape, I32),
            tile,
            tile,
            tile,
            pltpu.VMEM(weight.shape, BF16),
            pltpu.VMEM(weight.shape, BF16),
            pltpu.VMEM(seeds.shape, F32),
            pltpu.VMEM((length // block, 2 * block, size), BF16),
            pltpu.VMEM((length // block, size, 2 * block), BF16),
            pltpu.VMEM((length // block, 2 * block, size), BF16),
            pltpu.VMEM((length // block, size, 2 * block), BF16),
            (tile, tile),
            (pltpu.VMEM((depth, size), BF16),) * 2,
            (pltpu.VMEM((depth, size), BF16),) * half_slots,
            pltpu.VMEM((3, slots, 2, 8, size), F32),
            pltpu.VMEM((3, slots, size, 128), F32),
            pltpu.VMEM((3, slots, 2, 16, size), BF16),
            pltpu.VMEM((3, slots, size, 128), BF16),
            pltpu.VMEM((3, half_slots) + patch, BF16),
            pltpu.VMEM((3, half_slots) + patch, BF16),
            pltpu.VMEM((3, half_slots) + patch, F32),
            *[pltpu.VMEM((half_slots,) + patch, BF16)] * 8,
            pltpu.VMEM((3, half_slots, slots_uv, block, block), BF16),
            pltpu.VMEM((3, half_slots) + patch, BF16),
            pltpu.VMEM((3, half_slots) + patch, BF16),
            plane,
            plane,
            tile,
            tile,
            dma((9,)),
            dma((2, 5)),
            dma((2, 2)),
            dma((2, 3)),
            dma((2, 3, half_slots)),
            dma((2, half_slots, slots_uv)),
            dma((2, half_slots, slots_uv)),
            dma((2, half_slots, slots_uv)),
            dma((2, half_slots, slots_uv)),
            dma((2, 3, half_slots, slots_uv)),
            dma((2, 1 + EDGES)),
        ],
        compiler_params=pltpu.CompilerParams(
            vmem_limit_bytes=int(56 * 1024 * 1024), collective_id=0, has_side_effects=True
        ),
    )(count, offset, width, bins, used, seeds, sky, weight)
    return pl.pallas_call(
        add_kernel,
        out_shape=jax.ShapeDtypeStruct((size, size), F32),
        in_specs=[anywhere, anywhere],
        out_specs=anywhere,
        scratch_shapes=[tile, tile, plane, dma((3, BANDS))],
        compiler_params=pltpu.CompilerParams(vmem_limit_bytes=56 * 1024 * 1024),
        cost_estimate=pl.CostEstimate(flops=size * size, bytes_accessed=10 * size * size, transcendentals=0),
    )(inner, edge)


def solution(mesh):
    in_specs = (
        P("ty", "tx"),
        P("ty", "tx"),
        P("ty", "tx", None, None),
        P("ty", "tx", None),
        P("ty", "tx", None, None, None),
        P("ty", "tx", None),
        P("ty", "tx", None, None, None, None),
    )
    out_specs = P("ty", "tx")
    return jax.shard_map(shards, mesh=mesh, in_specs=in_specs, out_specs=out_specs, check_vma=False)
```

```python
import functools
import math

import jax
import jax.numpy as jnp
import numpy as np
from jax import lax
from jax.experimental import pallas as pl
from jax.experimental.pallas import tpu as pltpu
from jax.sharding import PartitionSpec as P

F32 = jnp.float32
BF16 = jnp.bfloat16
I32 = jnp.int32
FINE = 32
CHUNK = 512
BANDS = 4
EDGES = 2
FIELDS = 8
MESH = pl.DeviceIdType.MESH


def seed_tables(length, fine):
    pixels = np.arange(length, dtype=np.int64)
    rows = np.concatenate([np.arange(fine), fine * np.arange(length // fine)])
    angle = (rows[:, None] * pixels[None, :] % length) * (2.0 * math.pi / length)
    scale = np.where(np.arange(rows.shape[0]) < fine, 1.0 / math.sqrt(length), 1.0)[:, None]
    return np.stack([np.cos(angle) * scale, np.sin(angle) * scale]).astype(np.float32)


def wide(column, width):
    return jnp.concatenate([column] * (width // column.shape[1]), axis=1)


def kernel(
    count_hbm, offset_hbm, width_hbm, bins_hbm, used_hbm, seeds_in, sky_in, weight_in,
    inner_got, edge_got,
    count_in, offset_in, width_in, bins_in, used_in,
    meta_ref, meta_got, meta_all, sky_ref, outer_ref, inner_ref, weight_ref, weight_got,
    seeds_ref, row_tab, flip_tab, col_tab, turn_tab,
    beamed, first, spread, gx_ref, gy_ref, gx_half, gy_half,
    part_send, part_got, totals, raw_send, raw_got, own_send, own_got,
    sum_send, sum_got, back_send, back_got, weights, scaled_own, scaled_par, acc_outer, acc_inner, edge_send, inner_send,
    local_sems, meta_sems, sky_sems, weight_sems, part_sems, raw_sems, own_sems, sum_sems,
    back_sems, par_sems, last_sems,
):
    size = sky_ref.shape[0]
    length = 2 * size
    slots, slots_uv, block = weight_ref.shape[0], weight_ref.shape[1], weight_ref.shape[2]
    half_slots = slots // 2
    ty, tx = lax.axis_index("ty"), lax.axis_index("tx")
    ny, nx = lax.axis_size("ty"), lax.axis_size("tx")
    core = tx % 2
    partner = tx + 1 - 2 * core
    beyond = tx - 1 + 2 * core
    has_up, has_down = ty > 0, ty < ny - 1
    has_beyond = jnp.logical_and(beyond >= 0, beyond < nx)
    has_row = (has_up, has_down)
    row_half = pl.multiple_of((ty % 2) * size, size)
    col_half = pl.multiple_of((1 - core) * size, size)
    to_partner = {"tx": partner}
    to_beyond = {"tx": beyond}
    to_row = ({"ty": ty - 1}, {"ty": ty + 1})
    to_cross = ({"ty": ty - 1, "tx": partner}, {"ty": ty + 1, "tx": partner})
    odd_row = ty % 2
    d_far, d_mate = 2 * odd_row, 2 * (1 - odd_row)
    giving, fed = ty - 2 + 4 * odd_row, ty + 2 - 4 * odd_row
    has_far = jnp.logical_and(giving >= 0, giving < ny)
    has_fed = jnp.logical_and(fed >= 0, fed < ny)
    to_mate, to_giving, to_fed = {"ty": ty + 1 - 2 * odd_row}, {"ty": giving}, {"ty": fed}
    to_far = {"ty": ty - 1 + 2 * odd_row}

    local = [
        pltpu.make_async_copy(source, target, local_sems.at[i])
        for i, (source, target) in enumerate(
            (
                (sky_in, sky_ref),
                (count_hbm, count_in),
                (offset_hbm, offset_in),
                (width_hbm, width_in),
                (bins_hbm, bins_in),
                (used_hbm, used_in),
                (seeds_in, seeds_ref),
                (weight_in, weight_ref),
            )
        )
    ]

    def remote(src, dst, sems, at, target):
        return pltpu.make_async_remote_copy(
            src_ref=src,
            dst_ref=dst,
            send_sem=sems.at[(0,) + at],
            recv_sem=sems.at[(1,) + at],
            device_id=target,
            device_id_type=MESH,
        )

    def meta_copy(slot, target):
        return remote(meta_ref, meta_got[slot], meta_sems, (slot,), target)

    def meta_partner():
        return meta_copy(0, to_partner)

    def meta_send(side):
        return meta_copy(2 - side, to_row[side]), meta_copy(4 - side, to_cross[side])

    def meta_take(side):
        return meta_copy(1 + side, to_row[side]), meta_copy(3 + side, to_cross[side])

    def sky_partner():
        return remote(sky_ref, inner_ref, sky_sems, (0,), to_partner)

    def sky_beyond():
        return remote(sky_ref, outer_ref, sky_sems, (1,), to_beyond)

    def weight_copy():
        return remote(weight_ref, weight_got, weight_sems, (0,), to_partner)

    def part_copy(g, jj):
        return remote(part_send.at[g, jj], part_got.at[g, jj], part_sems, (g, jj), to_partner)

    def raw_copy(target, jj, k):
        return remote(raw_send.at[jj, k], raw_got.at[jj, k], raw_sems, (jj, k), target)

    def own_copy(jj, k):
        return remote(own_send.at[jj, k], own_got.at[jj, k], own_sems, (jj, k), to_mate)

    def sum_copy(jj, k):
        return remote(sum_send.at[jj, k], sum_got.at[jj, k], sum_sems, (jj, k), to_mate)

    def back_copy(target, jj, k):
        return remote(back_send.at[jj, k], back_got.at[jj, k], back_sems, (jj, k), target)

    def weights_mate():
        return remote(weights.at[2], weights.at[1], weight_sems, (1,), to_mate)

    def weights_far():
        return remote(weights.at[2], weights.at[0], weight_sems, (2,), to_far)

    def par_copy(g, jj, k):
        return remote(
            scaled_own.at[g, jj, k], scaled_par.at[g, jj, k], par_sems, (g, jj, k), to_partner
        )

    def last_edge(band):
        rows = slice(band * size // EDGES, (band + 1) * size // EDGES)
        return remote(edge_send.at[rows], edge_got.at[rows], last_sems, (1 + band,), to_beyond)

    def last_inner():
        return remote(inner_send, inner_got, last_sems, (0,), to_partner)

    def no_edge():
        return pltpu.make_async_copy(edge_send, edge_got, local_sems.at[len(local)])

    barrier = pltpu.get_barrier_semaphore()
    pl.semaphore_signal(barrier, inc=1, device_id=to_partner, device_id_type=MESH)

    @pl.when(has_beyond)
    def _():
        pl.semaphore_signal(barrier, inc=1, device_id=to_beyond, device_id_type=MESH)

    for side in range(2):

        @pl.when(has_row[side])
        def _(side=side):
            pl.semaphore_signal(barrier, inc=1, device_id=to_row[side], device_id_type=MESH)
            pl.semaphore_signal(barrier, inc=1, device_id=to_cross[side], device_id_type=MESH)

    for has, target in ((has_far, to_giving), (has_fed, to_fed)):

        @pl.when(has)
        def _(target=target):
            pl.semaphore_signal(barrier, inc=1, device_id=target, device_id_type=MESH)

    for copy in local:
        copy.start()

    for copy in local[1:6]:
        copy.wait()

    lane = lax.broadcasted_iota(I32, (1, slots), 1)
    widths = width_in[...].astype(F32)
    meta_ref[slots, 0] = count_in[0, 0]
    for s in range(slots):
        meta_ref[s, 0] = offset_in[0, s]
        meta_ref[s, 1] = offset_in[1, s]
        meta_ref[s, 2] = jnp.sum(jnp.where(lane == s, widths, 0.0)).astype(I32)
        for k in range(slots_uv):
            for which in range(2):
                meta_ref[s, 3 + 2 * k + which] = bins_in[k, which, s]
        meta_ref[s, 3 + 2 * slots_uv] = used_in[0, s]

    @pl.when(jnp.logical_not(has_beyond))
    def _():
        outer_ref[...] = jnp.zeros_like(outer_ref)
        edge_send[...] = jnp.zeros_like(edge_send)

    with jax.named_scope("barrier"):
        local[0].wait()
        pl.semaphore_wait(
            barrier,
            1 + has_beyond.astype(I32) + 2 * has_up.astype(I32) + 2 * has_down.astype(I32)
            + has_far.astype(I32) + has_fed.astype(I32),
        )

    @pl.when(has_beyond)
    def _():
        sky_beyond().start()

    sky_partner().start()
    meta_partner().start()
    for side in range(2):

        @pl.when(has_row[side])
        def _(side=side):
            for copy in meta_send(side):
                copy.start()

    for copy in local[6:]:
        copy.wait()
    weight_copy().start()

    acc_outer[...] = jnp.zeros_like(acc_outer)
    acc_inner[...] = jnp.zeros_like(acc_inner)

    per_block = block // FINE

    def table(j, carry):
        blk, at = j // per_block, pl.ds(pl.multiple_of((j % per_block) * FINE, FINE), FINE)
        for tab, half in ((row_tab, row_half), (col_tab, col_half)):
            lanes = pl.ds(half, size)
            c, s = seeds_ref[0, pl.ds(FINE + j, 1), lanes], seeds_ref[1, pl.ds(FINE + j, 1), lanes]
            fc, fs = seeds_ref[0, :FINE, lanes], seeds_ref[1, :FINE, lanes]
            tab[blk, at, :] = (fc * c - fs * s).astype(BF16)
            tab[blk, pl.ds(pl.multiple_of(block + (j % per_block) * FINE, FINE), FINE), :] = (fs * c + fc * s).astype(BF16)
        return carry

    with jax.named_scope("tables"):
        lax.fori_loop(0, length // FINE, table, 0)

    def flipped(j, carry):
        at = pl.ds(pl.multiple_of(j * FINE, FINE), FINE)
        for tab, parity in ((flip_tab, odd_row), (turn_tab, 1 - core)):
            row = parity * (size // FINE) + j
            c, s = seeds_ref[0, pl.ds(FINE + row, 1), :], seeds_ref[1, pl.ds(FINE + row, 1), :]
            fc, fs = seeds_ref[0, :FINE, :], seeds_ref[1, :FINE, :]
            cos, sin = (fc * c - fs * s).astype(BF16), (fs * c + fc * s).astype(BF16)
            for blk in range(length // block):
                tab[blk, at, :block] = cos[:, blk * block : (blk + 1) * block]
                tab[blk, at, block:] = sin[:, blk * block : (blk + 1) * block]
        return carry

    with jax.named_scope("flips"):
        lax.fori_loop(0, size // FINE, flipped, 0)

    with jax.named_scope("meta"):
        meta_partner().wait()
        for side in range(2):

            @pl.when(has_row[side])
            def _(side=side):
                for copy in meta_take(side):
                    copy.wait_recv()

            @pl.when(jnp.logical_not(has_row[side]))
            def _(side=side):
                for slot in (1 + side, 3 + side):
                    meta_got[slot][slots, 0] = 0
                    for s in range(slots):
                        for f in range(FIELDS):
                            meta_got[slot][s, f] = 0

    sources = ((meta_got[1], meta_got[3]), (meta_ref, meta_got[0]), (meta_got[2], meta_got[4]))
    even_here = core == 0

    def gather(s, f):
        for d, (same, other) in enumerate(sources):
            a, b = same[s, f], other[s, f]
            meta_all[d, 0, s, f] = jnp.where(even_here, a, b)
            meta_all[d, 1, s, f] = jnp.where(even_here, b, a)

    def gather_slot(s, carry):
        for f in range(FIELDS):
            gather(s, f)
        return carry

    lax.fori_loop(0, slots, gather_slot, 0)
    gather(slots, 0)

    def pointing(d, j):
        even, odd = meta_all[d, 0, slots, 0], meta_all[d, 1, slots, 0]
        from_odd = (j >= even).astype(I32)
        slot = jnp.clip(j - from_odd * even, 0, slots - 1)
        live = j < even + odd
        return from_odd, slot, live

    def bins(d, from_odd, slot, k, which):
        b = meta_all[d, from_odd, slot, 3 + 2 * k + which]
        return jnp.clip(b, 0, length // block - 1)

    def gaussian(shape, axis, shift, decay, live):
        away = lax.broadcasted_iota(I32, shape, axis) + shift
        inside = jnp.logical_and(away >= -size, away < size)
        inside = jnp.logical_and(inside, live)
        away = away.astype(F32)
        if axis == 0:
            fold = away.reshape(shape[0] // 8, 8, shape[1])
            value = jnp.exp(-(fold * fold) * decay[None]).reshape(shape)
        else:
            value = jnp.exp(-(away * away) * wide(decay, shape[1]))
        return jnp.where(inside, value, jnp.zeros(shape, F32))

    def beams(i, carry):
        d, j = i // slots, i % slots
        from_odd, slot, live = pointing(d, j)
        oy, ox = meta_all[d, from_odd, slot, 0], meta_all[d, from_odd, slot, 1]
        width = jnp.full((8, 128), meta_all[d, from_odd, slot, 2], I32).astype(F32)
        decay = 1.0 / (2.0 * width * width)
        gy = gaussian((size, 128), 0, (1 - d) * size - oy, decay, live)
        gy_ref[d, j] = gy
        gy_half[d, j] = gy.astype(BF16)
        outer_at, inner_at = 3 * core - 1, 1 - core
        for i, tile_at in enumerate((outer_at, inner_at)):
            gx = gaussian((8, size), 1, (tile_at - from_odd) * size - ox, decay, live)
            gx_ref[d, j, i] = gx
            gx_half[d, j, i] = jnp.concatenate([gx, gx], axis=0).astype(BF16)
        return carry

    with jax.named_scope("weights"):
        weight_copy().wait_recv()
        for jj in range(half_slots):
            from_odd, slot, live = pointing(1, half_slots * core + jj)
            used = meta_all[1, from_odd, slot, 3 + 2 * slots_uv]
            for k in range(slots_uv):
                weight = jnp.where(from_odd == core, weight_ref[slot, k], weight_got[slot, k])
                weight = weight.astype(F32) * jnp.where(k < used, 1.0, 0.0).astype(F32)
                weights[2, jj, k] = weight.astype(BF16)

        weights_mate().start()

        @pl.when(has_far)
        def _():
            weights_far().start()

    with jax.named_scope("beams"):
        lax.fori_loop(0, 3 * slots, beams, 0)

    def column_table(d, from_odd, slot, k):
        return col_tab[bins(d, from_odd, slot, k, 1)]

    def prepare(d, j, beamed_ref):
        gy = wide(gy_half[d, j], CHUNK)
        for at in range(0, size, CHUNK):
            cols = slice(at, at + CHUNK)
            gx = [jnp.concatenate([gx_half[d, j, i, :, cols]] * (size // 16), axis=0) for i in range(2)]
            value = gx[0] * outer_ref[:, cols] + gx[1] * inner_ref[:, cols]
            beamed_ref[:, cols] = gy * value

    def transform_rows(d, j, beamed_ref, first_ref):
        from_odd, slot, live = pointing(d, j)
        rows = jnp.concatenate(
            [row_tab[bins(d, from_odd, slot, k, 0)] for k in range(slots_uv)], axis=0
        )
        for at in range(0, size, CHUNK):
            cols = slice(at, at + CHUNK)
            first_ref[:, cols] = jnp.dot(
                rows, beamed_ref[:, cols], preferred_element_type=F32
            ).astype(BF16)

    def transform_columns(d, j, first_ref, result_ref):
        from_odd, slot, live = pointing(d, j)
        for k in range(slots_uv):
            both = jnp.dot(
                first_ref[2 * k * block : (2 * k + 2) * block, :],
                turn_tab[bins(d, from_odd, slot, k, 1)],
                preferred_element_type=F32,
            )
            real = both[:block, :block] - both[block:, block:]
            turned = both[:block, block:] + both[block:, :block]
            result_ref[k, :, :block] = real.astype(result_ref.dtype)
            result_ref[k, :, block:] = turned.astype(result_ref.dtype)

    def spread_out(d, j, scaled_ref, spread_ref):
        from_odd, slot, live = pointing(d, j)
        for k in range(slots_uv):
            value = scaled_ref[k]
            real, turned = value[:, :block], value[:, block:]
            square = jnp.concatenate(
                [value, jnp.concatenate([turned, -real], axis=1)], axis=0
            )
            spread_ref[2 * k * block : (2 * k + 2) * block, :] = jnp.dot(
                square, col_tab[bins(d, from_odd, slot, k, 1)], preferred_element_type=F32
            ).astype(BF16)

    def bring_back(d, j, spread_ref, start, stop):
        from_odd, slot, live = pointing(d, j)
        rows = jnp.concatenate(
            [flip_tab[bins(d, from_odd, slot, k, 0), start:stop] for k in range(slots_uv)], axis=1
        )
        gy = wide(gy_ref[d, j, start:stop], CHUNK)
        for at in range(0, size, CHUNK):
            cols = slice(at, at + CHUNK)
            back = gy * jnp.dot(rows, spread_ref[:, cols], preferred_element_type=F32)
            acc_outer[start:stop, cols] += gx_ref[d, j, 0, 0:1, cols] * back
            acc_inner[start:stop, cols] += gx_ref[d, j, 1, 0:1, cols] * back

    mine, theirs = half_slots * core, half_slots * (1 - core)

    with jax.named_scope("sky"):
        sky_partner().wait_recv()

        @pl.when(has_beyond)
        def _():
            sky_beyond().wait_recv()

    def pass_sum(jj, k, value):
        sum_send[jj, k] = value.astype(BF16)
        sum_copy(jj, k).start()

    def row_of(g):
        own = g // 2
        return 2 * (odd_row * (1 - g) + (1 - odd_row) * g) * (1 - own) + own

    def settle(g, jj):
        part_copy(g, jj).wait_recv()
        for k in range(slots_uv):
            totals[g, jj, k] = totals[g, jj, k] + part_got[g, jj, k].astype(F32)

        @pl.when(g == 0)
        def _():
            for k in range(slots_uv):
                raw_send[jj, k] = totals[0, jj, k].astype(BF16)
                raw_copy(to_giving, jj, k).start()

        @pl.when(g == 2)
        def _():
            for k in range(slots_uv):
                own_send[jj, k] = totals[2, jj, k].astype(BF16)
                own_copy(jj, k).start()

        @pl.when(jnp.logical_and(g == 1, jnp.logical_not(has_fed)))
        def _():
            for k in range(slots_uv):
                pass_sum(jj, k, totals[1, jj, k])

    far = has_far.astype(I32)

    def forward_units(s, carry):
        end = s // half_slots
        slot = s * (1 - end)
        units = (
            (2 * (1 - end) * (1 - far) + end, slot),
            ((1 - end) * (1 + far) + end, slot + end),
        )
        for base in (theirs, mine):
            for i, (g, jj) in enumerate(units):
                prepare(row_of(g), base + jj, beamed[i])
            for i, (g, jj) in enumerate(units):
                transform_rows(row_of(g), base + jj, beamed[i], first[i])
            for i, (g, jj) in enumerate(units):
                result = part_send.at[g, jj] if base is theirs else totals.at[g, jj]
                transform_columns(row_of(g), base + jj, first[i], result)
            for g, jj in units:
                if base is theirs:
                    part_copy(g, jj).start()
                else:
                    settle(g, jj)
        return carry

    with jax.named_scope("forward"):
        lax.fori_loop(0, half_slots + far, forward_units, 0)

    def scale(g, jj, k, total):
        weight = weights[g, jj, k].astype(F32)
        scaled_own[g, jj, k] = (total * wide(weight, 2 * block)).astype(BF16)
        par_copy(g, jj, k).start()

    def adjoint_all(g, base, scaled_ref):
        for jj in range(half_slots):
            spread_out(row_of(g), base + jj, scaled_ref.at[g, jj], spread[jj])
        for jj in range(half_slots):
            bring_back(row_of(g), base + jj, spread[jj], 0, size)

    def adjoint_one(g, base, jj, scaled_ref):
        spread_out(row_of(g), base + jj, scaled_ref.at[g, jj], spread[0])
        bring_back(row_of(g), base + jj, spread[0], 0, size)

    def adjoint_theirs(g):
        with jax.named_scope(f"theirs{g}"):
            for jj in range(half_slots):
                for k in range(slots_uv):
                    par_copy(g, jj, k).wait_recv()
            adjoint_all(g, theirs, scaled_par)

    def mate_slot(jj, carry):
        for k in range(slots_uv):
            own_copy(jj, k).wait_recv()
            own_part = own_got[jj, k].astype(F32)

            @pl.when(has_fed)
            def _(k=k):
                back_send[jj, k] = (totals[1, jj, k] + own_got[jj, k].astype(F32)).astype(BF16)
                back_copy(to_fed, jj, k).start()
                raw_copy(to_fed, jj, k).wait_recv()
                both = totals[1, jj, k] + raw_got[jj, k].astype(F32)
                pass_sum(jj, k, both)
                totals[1, jj, k] = both

            scale(1, jj, k, totals[1, jj, k] + own_part)
        adjoint_one(1, mine, jj, scaled_own)
        return carry

    with jax.named_scope("mate"):
        weights_mate().wait_recv()
        lax.fori_loop(0, half_slots, mate_slot, 0)

    adjoint_theirs(1)

    def far_slot(jj, carry):
        for k in range(slots_uv):
            back_copy(to_giving, jj, k).wait_recv()
            scale(0, jj, k, totals[0, jj, k] + back_got[jj, k].astype(F32))
        adjoint_one(0, mine, jj, scaled_own)
        return carry

    @pl.when(has_far)
    def _():
        with jax.named_scope("far"):
            weights_far().wait_recv()
            lax.fori_loop(0, half_slots, far_slot, 0)

    def own_slot(jj):
        with jax.named_scope(f"own{jj}"):
            for k in range(slots_uv):
                sum_copy(jj, k).wait_recv()
                scale(2, jj, k, totals[2, jj, k] + sum_got[jj, k].astype(F32))
            adjoint_one(2, mine, jj, scaled_own)

    own_slot(0)

    @pl.when(has_far)
    def _():
        adjoint_theirs(0)

    def own_theirs(jj):
        for k in range(slots_uv):
            par_copy(2, jj, k).wait_recv()
        adjoint_one(2, theirs, jj, scaled_par)

    for jj in range(half_slots - 1):

        @pl.when(jnp.logical_not(has_far))
        def _(jj=jj):
            own_theirs(jj)

        own_slot(jj + 1)

        @pl.when(has_far)
        def _(jj=jj):
            own_theirs(jj)

    with jax.named_scope("final"):
        jj = half_slots - 1
        for k in range(slots_uv):
            par_copy(2, jj, k).wait_recv()
        spread_out(1, theirs + jj, scaled_par.at[2, jj], spread[0])
        for band in range(EDGES):
            start, stop = band * size // EDGES, (band + 1) * size // EDGES
            bring_back(1, theirs + jj, spread[0], start, stop)

            @pl.when(has_beyond)
            def _(band=band, start=start, stop=stop):
                edge_send[start:stop] = acc_outer[start:stop].astype(BF16)
                last_edge(band).start()

    inner_send[...] = acc_inner[...].astype(BF16)
    last_inner().start()

    @pl.when(jnp.logical_not(has_beyond))
    def _():
        no_edge().start()

    sky_partner().wait_send()
    weight_copy().wait_send()

    @pl.when(has_beyond)
    def _():
        sky_beyond().wait_send()

    for side in range(2):

        @pl.when(has_row[side])
        def _(side=side):
            for copy in meta_send(side):
                copy.wait_send()

    for jj in range(half_slots):
        for g in (1, 2):
            part_copy(g, jj).wait_send()
            for k in range(slots_uv):
                par_copy(g, jj, k).wait_send()
        for k in range(slots_uv):
            own_copy(jj, k).wait_send()
            sum_copy(jj, k).wait_send()

            @pl.when(has_fed)
            def _(jj=jj, k=k):
                back_copy(to_fed, jj, k).wait_send()

        @pl.when(has_far)
        def _(jj=jj):
            part_copy(0, jj).wait_send()
            for k in range(slots_uv):
                par_copy(0, jj, k).wait_send()
                raw_copy(to_giving, jj, k).wait_send()

    weights_mate().wait_send()

    @pl.when(has_far)
    def _():
        weights_far().wait_send()

    with jax.named_scope("last"):
        last_inner().wait()

        @pl.when(has_beyond)
        def _():
            for band in range(EDGES):
                last_edge(band).wait()

        @pl.when(jnp.logical_not(has_beyond))
        def _():
            no_edge().wait()


def add_kernel(inner_hbm, edge_hbm, out_hbm, inner_ref, edge_ref, out_ref, sems):
    band = out_ref.shape[0] // BANDS
    bands = [slice(i * band, (i + 1) * band) for i in range(BANDS)]
    moves = [
        [
            pltpu.make_async_copy(inner_hbm.at[rows], inner_ref.at[rows], sems.at[0, i]),
            pltpu.make_async_copy(edge_hbm.at[rows], edge_ref.at[rows], sems.at[1, i]),
            pltpu.make_async_copy(out_ref.at[rows], out_hbm.at[rows], sems.at[2, i]),
        ]
        for i, rows in enumerate(bands)
    ]
    for inner, edge, out in moves:
        inner.start()
        edge.start()
    for rows, (inner, edge, out) in zip(bands, moves):
        inner.wait()
        edge.wait()
        out_ref[rows, :] = inner_ref[rows, :].astype(F32) + edge_ref[rows, :].astype(F32)
        out.start()
    for inner, edge, out in moves:
        out.wait()


def shards(sky, point_count, point_offset, beam_width, uv_bins, uv_count, uv_weight):
    size = sky.shape[0]
    length = 2 * size
    slots, slots_uv, block = uv_weight.shape[2], uv_weight.shape[3], uv_weight.shape[4]
    half_slots = slots // 2
    depth = 2 * slots_uv * block
    seeds = seed_tables(length, FINE)
    count = point_count.reshape(1, 1)
    offset = jnp.transpose(point_offset, (0, 1, 3, 2)).reshape(2, slots)
    width = beam_width.reshape(1, slots)
    bins = jnp.transpose(uv_bins, (0, 1, 3, 4, 2)).reshape(slots_uv, 2, slots)
    used = uv_count.reshape(1, slots)
    weight = uv_weight.reshape(slots, slots_uv, block, block)

    dma = pltpu.SemaphoreType.DMA
    meta_shape = (slots + 1, FIELDS)
    tile = pltpu.VMEM((size, size), BF16)
    plane = pltpu.VMEM((size, size), F32)
    patch = (slots_uv, block, 2 * block)
    anywhere = pl.BlockSpec(memory_space=pl.ANY)
    inner, edge = pl.pallas_call(
        kernel,
        out_shape=(jax.ShapeDtypeStruct((size, size), BF16),) * 2,
        in_specs=[anywhere] * 8,
        out_specs=(anywhere, anywhere),
        scratch_shapes=[
            pltpu.SMEM(count.shape, I32),
            pltpu.SMEM(offset.shape, I32),
            pltpu.VMEM(width.shape, BF16),
            pltpu.SMEM(bins.shape, I32),
            pltpu.SMEM(used.shape, I32),
            pltpu.SMEM(meta_shape, I32),
            tuple([pltpu.SMEM(meta_shape, I32)] * 5),
            pltpu.SMEM((3, 2) + meta_shape, I32),
            tile,
            tile,
            tile,
            pltpu.VMEM(weight.shape, BF16),
            pltpu.VMEM(weight.shape, BF16),
            pltpu.VMEM(seeds.shape, F32),
            pltpu.VMEM((length // block, 2 * block, size), BF16),
            pltpu.VMEM((length // block, size, 2 * block), BF16),
            pltpu.VMEM((length // block, 2 * block, size), BF16),
            pltpu.VMEM((length // block, size, 2 * block), BF16),
            (tile, tile),
            (pltpu.VMEM((depth, size), BF16),) * 2,
            (pltpu.VMEM((depth, size), BF16),) * half_slots,
            pltpu.VMEM((3, slots, 2, 8, size), F32),
            pltpu.VMEM((3, slots, size, 128), F32),
            pltpu.VMEM((3, slots, 2, 16, size), BF16),
            pltpu.VMEM((3, slots, size, 128), BF16),
            pltpu.VMEM((3, half_slots) + patch, BF16),
            pltpu.VMEM((3, half_slots) + patch, BF16),
            pltpu.VMEM((3, half_slots) + patch, F32),
            *[pltpu.VMEM((half_slots,) + patch, BF16)] * 8,
            pltpu.VMEM((3, half_slots, slots_uv, block, block), BF16),
            pltpu.VMEM((3, half_slots) + patch, BF16),
            pltpu.VMEM((3, half_slots) + patch, BF16),
            plane,
            plane,
            tile,
            tile,
            dma((9,)),
            dma((2, 5)),
            dma((2, 2)),
            dma((2, 3)),
            dma((2, 3, half_slots)),
            dma((2, half_slots, slots_uv)),
            dma((2, half_slots, slots_uv)),
            dma((2, half_slots, slots_uv)),
            dma((2, half_slots, slots_uv)),
            dma((2, 3, half_slots, slots_uv)),
            dma((2, 1 + EDGES)),
        ],
        compiler_params=pltpu.CompilerParams(
            vmem_limit_bytes=int(56 * 1024 * 1024), collective_id=0, has_side_effects=True
        ),
    )(count, offset, width, bins, used, seeds, sky, weight)
    return pl.pallas_call(
        add_kernel,
        out_shape=jax.ShapeDtypeStruct((size, size), F32),
        in_specs=[anywhere, anywhere],
        out_specs=anywhere,
        scratch_shapes=[tile, tile, plane, dma((3, BANDS))],
        compiler_params=pltpu.CompilerParams(vmem_limit_bytes=56 * 1024 * 1024),
        cost_estimate=pl.CostEstimate(flops=size * size, bytes_accessed=10 * size * size, transcendentals=0),
    )(inner, edge)


def solution(mesh):
    in_specs = (
        P("ty", "tx"),
        P("ty", "tx"),
        P("ty", "tx", None, None),
        P("ty", "tx", None),
        P("ty", "tx", None, None, None),
        P("ty", "tx", None),
        P("ty", "tx", None, None, None, None),
    )
    out_specs = P("ty", "tx")
    return jax.shard_map(shards, mesh=mesh, in_specs=in_specs, out_specs=out_specs, check_vma=False)
```

```python
import functools
import math

import jax
import jax.numpy as jnp
import numpy as np
from jax import lax
from jax.experimental import pallas as pl
from jax.experimental.pallas import tpu as pltpu
from jax.sharding import PartitionSpec as P

F32 = jnp.float32
BF16 = jnp.bfloat16
I32 = jnp.int32
FINE = 32
CHUNK = 512
BANDS = 4
EDGES = 2
FIELDS = 8
MESH = pl.DeviceIdType.MESH


def seed_tables(length, fine):
    pixels = np.arange(length, dtype=np.int64)
    rows = np.concatenate([np.arange(fine), fine * np.arange(length // fine)])
    angle = (rows[:, None] * pixels[None, :] % length) * (2.0 * math.pi / length)
    scale = np.where(np.arange(rows.shape[0]) < fine, 1.0 / math.sqrt(length), 1.0)[:, None]
    return np.stack([np.cos(angle) * scale, np.sin(angle) * scale]).astype(np.float32)


def wide(column, width):
    return jnp.concatenate([column] * (width // column.shape[1]), axis=1)


def kernel(
    count_hbm, offset_hbm, width_hbm, bins_hbm, used_hbm, seeds_in, sky_in, weight_in,
    inner_got, edge_got,
    count_in, offset_in, width_in, bins_in, used_in,
    meta_ref, meta_got, meta_all, sky_ref, outer_ref, inner_ref, weight_ref, weight_got,
    seeds_ref, row_tab, flip_tab, col_tab, turn_tab,
    beamed, first, spread, gx_ref, gy_ref, gx_half, gy_half,
    part_send, part_got, totals, raw_send, raw_got, own_send, own_got,
    sum_send, sum_got, back_send, back_got, weights, scaled_own, scaled_par, acc_outer, acc_inner, edge_send, inner_send,
    local_sems, meta_sems, sky_sems, weight_sems, part_sems, raw_sems, own_sems, sum_sems,
    back_sems, par_sems, last_sems,
):
    size = sky_ref.shape[0]
    length = 2 * size
    slots, slots_uv, block = weight_ref.shape[0], weight_ref.shape[1], weight_ref.shape[2]
    half_slots = slots // 2
    ty, tx = lax.axis_index("ty"), lax.axis_index("tx")
    ny, nx = lax.axis_size("ty"), lax.axis_size("tx")
    core = tx % 2
    partner = tx + 1 - 2 * core
    beyond = tx - 1 + 2 * core
    has_up, has_down = ty > 0, ty < ny - 1
    has_beyond = jnp.logical_and(beyond >= 0, beyond < nx)
    has_row = (has_up, has_down)
    row_half = pl.multiple_of((ty % 2) * size, size)
    col_half = pl.multiple_of((1 - core) * size, size)
    to_partner = {"tx": partner}
    to_beyond = {"tx": beyond}
    to_row = ({"ty": ty - 1}, {"ty": ty + 1})
    to_cross = ({"ty": ty - 1, "tx": partner}, {"ty": ty + 1, "tx": partner})
    odd_row = ty % 2
    d_far, d_mate = 2 * odd_row, 2 * (1 - odd_row)
    giving, fed = ty - 2 + 4 * odd_row, ty + 2 - 4 * odd_row
    has_far = jnp.logical_and(giving >= 0, giving < ny)
    has_fed = jnp.logical_and(fed >= 0, fed < ny)
    to_mate, to_giving, to_fed = {"ty": ty + 1 - 2 * odd_row}, {"ty": giving}, {"ty": fed}
    to_far = {"ty": ty - 1 + 2 * odd_row}

    local = [
        pltpu.make_async_copy(source, target, local_sems.at[i])
        for i, (source, target) in enumerate(
            (
                (sky_in, sky_ref),
                (count_hbm, count_in),
                (offset_hbm, offset_in),
                (width_hbm, width_in),
                (bins_hbm, bins_in),
                (used_hbm, used_in),
                (seeds_in, seeds_ref),
                (weight_in, weight_ref),
            )
        )
    ]

    def remote(src, dst, sems, at, target):
        return pltpu.make_async_remote_copy(
            src_ref=src,
            dst_ref=dst,
            send_sem=sems.at[(0,) + at],
            recv_sem=sems.at[(1,) + at],
            device_id=target,
            device_id_type=MESH,
        )

    def meta_copy(slot, target):
        return remote(meta_ref, meta_got[slot], meta_sems, (slot,), target)

    def meta_partner():
        return meta_copy(0, to_partner)

    def meta_send(side):
        return meta_copy(2 - side, to_row[side]), meta_copy(4 - side, to_cross[side])

    def meta_take(side):
        return meta_copy(1 + side, to_row[side]), meta_copy(3 + side, to_cross[side])

    def sky_partner():
        return remote(sky_ref, inner_ref, sky_sems, (0,), to_partner)

    def sky_beyond():
        return remote(sky_ref, outer_ref, sky_sems, (1,), to_beyond)

    def weight_copy():
        return remote(weight_ref, weight_got, weight_sems, (0,), to_partner)

    def part_copy(g, jj):
        return remote(part_send.at[g, jj], part_got.at[g, jj], part_sems, (g, jj), to_partner)

    def raw_copy(target, jj, k):
        return remote(raw_send.at[jj, k], raw_got.at[jj, k], raw_sems, (jj, k), target)

    def own_copy(jj, k):
        return remote(own_send.at[jj, k], own_got.at[jj, k], own_sems, (jj, k), to_mate)

    def sum_copy(jj, k):
        return remote(sum_send.at[jj, k], sum_got.at[jj, k], sum_sems, (jj, k), to_mate)

    def back_copy(target, jj, k):
        return remote(back_send.at[jj, k], back_got.at[jj, k], back_sems, (jj, k), target)

    def weights_mate():
        return remote(weights.at[2], weights.at[1], weight_sems, (1,), to_mate)

    def weights_far():
        return remote(weights.at[2], weights.at[0], weight_sems, (2,), to_far)

    def par_copy(g, jj, k):
        return remote(
            scaled_own.at[g, jj, k], scaled_par.at[g, jj, k], par_sems, (g, jj, k), to_partner
        )

    def last_edge(band):
        rows = slice(band * size // EDGES, (band + 1) * size // EDGES)
        return remote(edge_send.at[rows], edge_got.at[rows], last_sems, (1 + band,), to_beyond)

    def last_inner():
        return remote(inner_send, inner_got, last_sems, (0,), to_partner)

    def no_edge():
        return pltpu.make_async_copy(edge_send, edge_got, local_sems.at[len(local)])

    barrier = pltpu.get_barrier_semaphore()
    pl.semaphore_signal(barrier, inc=1, device_id=to_partner, device_id_type=MESH)

    @pl.when(has_beyond)
    def _():
        pl.semaphore_signal(barrier, inc=1, device_id=to_beyond, device_id_type=MESH)

    for side in range(2):

        @pl.when(has_row[side])
        def _(side=side):
            pl.semaphore_signal(barrier, inc=1, device_id=to_row[side], device_id_type=MESH)
            pl.semaphore_signal(barrier, inc=1, device_id=to_cross[side], device_id_type=MESH)

    for has, target in ((has_far, to_giving), (has_fed, to_fed)):

        @pl.when(has)
        def _(target=target):
            pl.semaphore_signal(barrier, inc=1, device_id=target, device_id_type=MESH)

    for copy in local:
        copy.start()

    for copy in local[1:6]:
        copy.wait()

    lane = lax.broadcasted_iota(I32, (1, slots), 1)
    widths = width_in[...].astype(F32)
    meta_ref[slots, 0] = count_in[0, 0]
    for s in range(slots):
        meta_ref[s, 0] = offset_in[0, s]
        meta_ref[s, 1] = offset_in[1, s]
        meta_ref[s, 2] = jnp.sum(jnp.where(lane == s, widths, 0.0)).astype(I32)
        for k in range(slots_uv):
            for which in range(2):
                meta_ref[s, 3 + 2 * k + which] = bins_in[k, which, s]
        meta_ref[s, 3 + 2 * slots_uv] = used_in[0, s]

    @pl.when(jnp.logical_not(has_beyond))
    def _():
        outer_ref[...] = jnp.zeros_like(outer_ref)
        edge_send[...] = jnp.zeros_like(edge_send)

    with jax.named_scope("barrier"):
        local[0].wait()
        pl.semaphore_wait(
            barrier,
            1 + has_beyond.astype(I32) + 2 * has_up.astype(I32) + 2 * has_down.astype(I32)
            + has_far.astype(I32) + has_fed.astype(I32),
        )

    @pl.when(has_beyond)
    def _():
        sky_beyond().start()

    sky_partner().start()
    meta_partner().start()
    for side in range(2):

        @pl.when(has_row[side])
        def _(side=side):
            for copy in meta_send(side):
                copy.start()

    for copy in local[6:]:
        copy.wait()
    weight_copy().start()

    acc_outer[...] = jnp.zeros_like(acc_outer)
    acc_inner[...] = jnp.zeros_like(acc_inner)

    per_block = block // FINE

    def table(j, carry):
        blk, at = j // per_block, pl.ds(pl.multiple_of((j % per_block) * FINE, FINE), FINE)
        for tab, half in ((row_tab, row_half), (col_tab, col_half)):
            lanes = pl.ds(half, size)
            c, s = seeds_ref[0, pl.ds(FINE + j, 1), lanes], seeds_ref[1, pl.ds(FINE + j, 1), lanes]
            fc, fs = seeds_ref[0, :FINE, lanes], seeds_ref[1, :FINE, lanes]
            tab[blk, at, :] = (fc * c - fs * s).astype(BF16)
            tab[blk, pl.ds(pl.multiple_of(block + (j % per_block) * FINE, FINE), FINE), :] = (fs * c + fc * s).astype(BF16)
        return carry

    with jax.named_scope("tables"):
        lax.fori_loop(0, length // FINE, table, 0)

    def flipped(j, carry):
        at = pl.ds(pl.multiple_of(j * FINE, FINE), FINE)
        for tab, parity in ((flip_tab, odd_row), (turn_tab, 1 - core)):
            row = parity * (size // FINE) + j
            c, s = seeds_ref[0, pl.ds(FINE + row, 1), :], seeds_ref[1, pl.ds(FINE + row, 1), :]
            fc, fs = seeds_ref[0, :FINE, :], seeds_ref[1, :FINE, :]
            cos, sin = (fc * c - fs * s).astype(BF16), (fs * c + fc * s).astype(BF16)
            for blk in range(length // block):
                tab[blk, at, :block] = cos[:, blk * block : (blk + 1) * block]
                tab[blk, at, block:] = sin[:, blk * block : (blk + 1) * block]
        return carry

    with jax.named_scope("flips"):
        lax.fori_loop(0, size // FINE, flipped, 0)

    with jax.named_scope("meta"):
        meta_partner().wait()
        for side in range(2):

            @pl.when(has_row[side])
            def _(side=side):
                for copy in meta_take(side):
                    copy.wait_recv()

            @pl.when(jnp.logical_not(has_row[side]))
            def _(side=side):
                for slot in (1 + side, 3 + side):
                    meta_got[slot][slots, 0] = 0
                    for s in range(slots):
                        for f in range(FIELDS):
                            meta_got[slot][s, f] = 0

    sources = ((meta_got[1], meta_got[3]), (meta_ref, meta_got[0]), (meta_got[2], meta_got[4]))
    even_here = core == 0

    def gather(s, f):
        for d, (same, other) in enumerate(sources):
            a, b = same[s, f], other[s, f]
            meta_all[d, 0, s, f] = jnp.where(even_here, a, b)
            meta_all[d, 1, s, f] = jnp.where(even_here, b, a)

    def gather_slot(s, carry):
        for f in range(FIELDS):
            gather(s, f)
        return carry

    lax.fori_loop(0, slots, gather_slot, 0)
    gather(slots, 0)

    def pointing(d, j):
        even, odd = meta_all[d, 0, slots, 0], meta_all[d, 1, slots, 0]
        from_odd = (j >= even).astype(I32)
        slot = jnp.clip(j - from_odd * even, 0, slots - 1)
        live = j < even + odd
        return from_odd, slot, live

    def bins(d, from_odd, slot, k, which):
        b = meta_all[d, from_odd, slot, 3 + 2 * k + which]
        return jnp.clip(b, 0, length // block - 1)

    def gaussian(shape, axis, shift, decay, live):
        away = lax.broadcasted_iota(I32, shape, axis) + shift
        inside = jnp.logical_and(away >= -size, away < size)
        inside = jnp.logical_and(inside, live)
        away = away.astype(F32)
        if axis == 0:
            fold = away.reshape(shape[0] // 8, 8, shape[1])
            value = jnp.exp(-(fold * fold) * decay[None]).reshape(shape)
        else:
            value = jnp.exp(-(away * away) * wide(decay, shape[1]))
        return jnp.where(inside, value, jnp.zeros(shape, F32))

    def beams(i, carry):
        d, j = i // slots, i % slots
        from_odd, slot, live = pointing(d, j)
        oy, ox = meta_all[d, from_odd, slot, 0], meta_all[d, from_odd, slot, 1]
        width = jnp.full((8, 128), meta_all[d, from_odd, slot, 2], I32).astype(F32)
        decay = 1.0 / (2.0 * width * width)
        gy = gaussian((size, 128), 0, (1 - d) * size - oy, decay, live)
        gy_ref[d, j] = gy
        gy_half[d, j] = gy.astype(BF16)
        outer_at, inner_at = 3 * core - 1, 1 - core
        for i, tile_at in enumerate((outer_at, inner_at)):
            gx = gaussian((8, size), 1, (tile_at - from_odd) * size - ox, decay, live)
            gx_ref[d, j, i] = gx
            gx_half[d, j, i] = jnp.concatenate([gx, gx], axis=0).astype(BF16)
        return carry

    with jax.named_scope("weights"):
        weight_copy().wait_recv()
        for jj in range(half_slots):
            from_odd, slot, live = pointing(1, half_slots * core + jj)
            used = meta_all[1, from_odd, slot, 3 + 2 * slots_uv]
            for k in range(slots_uv):
                weight = jnp.where(from_odd == core, weight_ref[slot, k], weight_got[slot, k])
                weight = weight.astype(F32) * jnp.where(k < used, 1.0, 0.0).astype(F32)
                weights[2, jj, k] = weight.astype(BF16)

        weights_mate().start()

        @pl.when(has_far)
        def _():
            weights_far().start()

    with jax.named_scope("beams"):
        lax.fori_loop(0, 3 * slots, beams, 0)

    def column_table(d, from_odd, slot, k):
        return col_tab[bins(d, from_odd, slot, k, 1)]

    def prepare(d, j, beamed_ref):
        gy = wide(gy_half[d, j], CHUNK)
        for at in range(0, size, CHUNK):
            cols = slice(at, at + CHUNK)
            gx = [jnp.concatenate([gx_half[d, j, i, :, cols]] * (size // 16), axis=0) for i in range(2)]
            value = gx[0] * outer_ref[:, cols] + gx[1] * inner_ref[:, cols]
            beamed_ref[:, cols] = gy * value

    def transform_rows(d, j, beamed_ref, first_ref):
        from_odd, slot, live = pointing(d, j)
        rows = jnp.concatenate(
            [row_tab[bins(d, from_odd, slot, k, 0)] for k in range(slots_uv)], axis=0
        )
        for at in range(0, size, CHUNK):
            cols = slice(at, at + CHUNK)
            first_ref[:, cols] = jnp.dot(
                rows, beamed_ref[:, cols], preferred_element_type=F32
            ).astype(BF16)

    def transform_columns(d, j, first_ref, result_ref):
        from_odd, slot, live = pointing(d, j)
        for k in range(slots_uv):
            both = jnp.dot(
                first_ref[2 * k * block : (2 * k + 2) * block, :],
                turn_tab[bins(d, from_odd, slot, k, 1)],
                preferred_element_type=F32,
            )
            real = both[:block, :block] - both[block:, block:]
            turned = both[:block, block:] + both[block:, :block]
            result_ref[k, :, :block] = real.astype(result_ref.dtype)
            result_ref[k, :, block:] = turned.astype(result_ref.dtype)

    def spread_out(d, j, scaled_ref, spread_ref):
        from_odd, slot, live = pointing(d, j)
        for k in range(slots_uv):
            value = scaled_ref[k]
            real, turned = value[:, :block], value[:, block:]
            square = jnp.concatenate(
                [value, jnp.concatenate([turned, -real], axis=1)], axis=0
            )
            spread_ref[2 * k * block : (2 * k + 2) * block, :] = jnp.dot(
                square, col_tab[bins(d, from_odd, slot, k, 1)], preferred_element_type=F32
            ).astype(BF16)

    def bring_back(d, j, spread_ref, start, stop):
        from_odd, slot, live = pointing(d, j)
        rows = jnp.concatenate(
            [flip_tab[bins(d, from_odd, slot, k, 0), start:stop] for k in range(slots_uv)], axis=1
        )
        gy = wide(gy_ref[d, j, start:stop], CHUNK)
        for at in range(0, size, CHUNK):
            cols = slice(at, at + CHUNK)
            back = gy * jnp.dot(rows, spread_ref[:, cols], preferred_element_type=F32)
            acc_outer[start:stop, cols] += gx_ref[d, j, 0, 0:1, cols] * back
            acc_inner[start:stop, cols] += gx_ref[d, j, 1, 0:1, cols] * back

    mine, theirs = half_slots * core, half_slots * (1 - core)

    with jax.named_scope("sky"):
        sky_partner().wait_recv()

        @pl.when(has_beyond)
        def _():
            sky_beyond().wait_recv()

    def pass_sum(jj, k, value):
        sum_send[jj, k] = value.astype(BF16)
        sum_copy(jj, k).start()

    def row_of(g):
        own = g // 2
        return 2 * (odd_row * (1 - g) + (1 - odd_row) * g) * (1 - own) + own

    def settle(g, jj):
        part_copy(g, jj).wait_recv()
        for k in range(slots_uv):
            totals[g, jj, k] = totals[g, jj, k] + part_got[g, jj, k].astype(F32)

        @pl.when(g == 0)
        def _():
            for k in range(slots_uv):
                raw_send[jj, k] = totals[0, jj, k].astype(BF16)
                raw_copy(to_giving, jj, k).start()

        @pl.when(g == 2)
        def _():
            for k in range(slots_uv):
                own_send[jj, k] = totals[2, jj, k].astype(BF16)
                own_copy(jj, k).start()

        @pl.when(jnp.logical_and(g == 1, jnp.logical_not(has_fed)))
        def _():
            for k in range(slots_uv):
                pass_sum(jj, k, totals[1, jj, k])

    far = has_far.astype(I32)

    def forward_units(s, carry):
        end = s // half_slots
        slot = s * (1 - end)
        units = (
            (2 * (1 - end) * (1 - far) + end, slot),
            ((1 - end) * (1 + far) + end, slot + end),
        )
        for base in (theirs, mine):
            for i, (g, jj) in enumerate(units):
                prepare(row_of(g), base + jj, beamed[i])
            for i, (g, jj) in enumerate(units):
                transform_rows(row_of(g), base + jj, beamed[i], first[i])
            for i, (g, jj) in enumerate(units):
                result = part_send.at[g, jj] if base is theirs else totals.at[g, jj]
                transform_columns(row_of(g), base + jj, first[i], result)
            for g, jj in units:
                if base is theirs:
                    part_copy(g, jj).start()
                else:
                    settle(g, jj)
        return carry

    with jax.named_scope("forward"):
        lax.fori_loop(0, half_slots + far, forward_units, 0)

    def scale(g, jj, k, total):
        weight = weights[g, jj, k].astype(F32)
        scaled_own[g, jj, k] = (total * wide(weight, 2 * block)).astype(BF16)
        par_copy(g, jj, k).start()

    def adjoint_all(g, base, scaled_ref):
        for jj in range(half_slots):
            spread_out(row_of(g), base + jj, scaled_ref.at[g, jj], spread[jj])
        for jj in range(half_slots):
            bring_back(row_of(g), base + jj, spread[jj], 0, size)

    def adjoint_one(g, base, jj, scaled_ref):
        spread_out(row_of(g), base + jj, scaled_ref.at[g, jj], spread[0])
        bring_back(row_of(g), base + jj, spread[0], 0, size)

    def adjoint_theirs(g):
        with jax.named_scope(f"theirs{g}"):
            for jj in range(half_slots):
                for k in range(slots_uv):
                    par_copy(g, jj, k).wait_recv()
            adjoint_all(g, theirs, scaled_par)

    def mate_slot(jj, carry):
        for k in range(slots_uv):
            own_copy(jj, k).wait_recv()
            own_part = own_got[jj, k].astype(F32)

            @pl.when(has_fed)
            def _(k=k):
                back_send[jj, k] = (totals[1, jj, k] + own_got[jj, k].astype(F32)).astype(BF16)
                back_copy(to_fed, jj, k).start()
                raw_copy(to_fed, jj, k).wait_recv()
                both = totals[1, jj, k] + raw_got[jj, k].astype(F32)
                pass_sum(jj, k, both)
                totals[1, jj, k] = both

            scale(1, jj, k, totals[1, jj, k] + own_part)
        adjoint_one(1, mine, jj, scaled_own)
        return carry

    with jax.named_scope("mate"):
        weights_mate().wait_recv()
        lax.fori_loop(0, half_slots, mate_slot, 0)

    def far_slot(jj, carry):
        for k in range(slots_uv):
            back_copy(to_giving, jj, k).wait_recv()
            scale(0, jj, k, totals[0, jj, k] + back_got[jj, k].astype(F32))
        adjoint_one(0, mine, jj, scaled_own)
        return carry

    @pl.when(has_far)
    def _():
        weights_far().wait_recv()

    def mate_theirs(jj, carry):
        for k in range(slots_uv):
            par_copy(1, jj, k).wait_recv()
        adjoint_one(1, theirs, jj, scaled_par)

        @pl.when(has_far)
        def _():
            far_slot(jj, 0)

        return carry

    with jax.named_scope("far"):
        lax.fori_loop(0, half_slots, mate_theirs, 0)

    def own_slot(jj):
        with jax.named_scope(f"own{jj}"):
            for k in range(slots_uv):
                sum_copy(jj, k).wait_recv()
                scale(2, jj, k, totals[2, jj, k] + sum_got[jj, k].astype(F32))
            adjoint_one(2, mine, jj, scaled_own)

    own_slot(0)

    @pl.when(has_far)
    def _():
        adjoint_theirs(0)

    def own_theirs(jj):
        for k in range(slots_uv):
            par_copy(2, jj, k).wait_recv()
        adjoint_one(2, theirs, jj, scaled_par)

    for jj in range(half_slots - 1):

        @pl.when(jnp.logical_not(has_far))
        def _(jj=jj):
            own_theirs(jj)

        own_slot(jj + 1)

        @pl.when(has_far)
        def _(jj=jj):
            own_theirs(jj)

    with jax.named_scope("final"):
        jj = half_slots - 1
        for k in range(slots_uv):
            par_copy(2, jj, k).wait_recv()
        spread_out(1, theirs + jj, scaled_par.at[2, jj], spread[0])
        for band in range(EDGES):
            start, stop = band * size // EDGES, (band + 1) * size // EDGES
            bring_back(1, theirs + jj, spread[0], start, stop)

            @pl.when(has_beyond)
            def _(band=band, start=start, stop=stop):
                edge_send[start:stop] = acc_outer[start:stop].astype(BF16)
                last_edge(band).start()

    inner_send[...] = acc_inner[...].astype(BF16)
    last_inner().start()

    @pl.when(jnp.logical_not(has_beyond))
    def _():
        no_edge().start()

    sky_partner().wait_send()
    weight_copy().wait_send()

    @pl.when(has_beyond)
    def _():
        sky_beyond().wait_send()

    for side in range(2):

        @pl.when(has_row[side])
        def _(side=side):
            for copy in meta_send(side):
                copy.wait_send()

    for jj in range(half_slots):
        for g in (1, 2):
            part_copy(g, jj).wait_send()
            for k in range(slots_uv):
                par_copy(g, jj, k).wait_send()
        for k in range(slots_uv):
            own_copy(jj, k).wait_send()
            sum_copy(jj, k).wait_send()

            @pl.when(has_fed)
            def _(jj=jj, k=k):
                back_copy(to_fed, jj, k).wait_send()

        @pl.when(has_far)
        def _(jj=jj):
            part_copy(0, jj).wait_send()
            for k in range(slots_uv):
                par_copy(0, jj, k).wait_send()
                raw_copy(to_giving, jj, k).wait_send()

    weights_mate().wait_send()

    @pl.when(has_far)
    def _():
        weights_far().wait_send()

    with jax.named_scope("last"):
        last_inner().wait()

        @pl.when(has_beyond)
        def _():
            for band in range(EDGES):
                last_edge(band).wait()

        @pl.when(jnp.logical_not(has_beyond))
        def _():
            no_edge().wait()


def add_kernel(inner_hbm, edge_hbm, out_hbm, inner_ref, edge_ref, out_ref, sems):
    band = out_ref.shape[0] // BANDS
    bands = [slice(i * band, (i + 1) * band) for i in range(BANDS)]
    moves = [
        [
            pltpu.make_async_copy(inner_hbm.at[rows], inner_ref.at[rows], sems.at[0, i]),
            pltpu.make_async_copy(edge_hbm.at[rows], edge_ref.at[rows], sems.at[1, i]),
            pltpu.make_async_copy(out_ref.at[rows], out_hbm.at[rows], sems.at[2, i]),
        ]
        for i, rows in enumerate(bands)
    ]
    for inner, edge, out in moves:
        inner.start()
        edge.start()
    for rows, (inner, edge, out) in zip(bands, moves):
        inner.wait()
        edge.wait()
        out_ref[rows, :] = inner_ref[rows, :].astype(F32) + edge_ref[rows, :].astype(F32)
        out.start()
    for inner, edge, out in moves:
        out.wait()


def shards(sky, point_count, point_offset, beam_width, uv_bins, uv_count, uv_weight):
    size = sky.shape[0]
    length = 2 * size
    slots, slots_uv, block = uv_weight.shape[2], uv_weight.shape[3], uv_weight.shape[4]
    half_slots = slots // 2
    depth = 2 * slots_uv * block
    seeds = seed_tables(length, FINE)
    count = point_count.reshape(1, 1)
    offset = jnp.transpose(point_offset, (0, 1, 3, 2)).reshape(2, slots)
    width = beam_width.reshape(1, slots)
    bins = jnp.transpose(uv_bins, (0, 1, 3, 4, 2)).reshape(slots_uv, 2, slots)
    used = uv_count.reshape(1, slots)
    weight = uv_weight.reshape(slots, slots_uv, block, block)

    dma = pltpu.SemaphoreType.DMA
    meta_shape = (slots + 1, FIELDS)
    tile = pltpu.VMEM((size, size), BF16)
    plane = pltpu.VMEM((size, size), F32)
    patch = (slots_uv, block, 2 * block)
    anywhere = pl.BlockSpec(memory_space=pl.ANY)
    inner, edge = pl.pallas_call(
        kernel,
        out_shape=(jax.ShapeDtypeStruct((size, size), BF16),) * 2,
        in_specs=[anywhere] * 8,
        out_specs=(anywhere, anywhere),
        scratch_shapes=[
            pltpu.SMEM(count.shape, I32),
            pltpu.SMEM(offset.shape, I32),
            pltpu.VMEM(width.shape, BF16),
            pltpu.SMEM(bins.shape, I32),
            pltpu.SMEM(used.shape, I32),
            pltpu.SMEM(meta_shape, I32),
            tuple([pltpu.SMEM(meta_shape, I32)] * 5),
            pltpu.SMEM((3, 2) + meta_shape, I32),
            tile,
            tile,
            tile,
            pltpu.VMEM(weight.shape, BF16),
            pltpu.VMEM(weight.shape, BF16),
            pltpu.VMEM(seeds.shape, F32),
            pltpu.VMEM((length // block, 2 * block, size), BF16),
            pltpu.VMEM((length // block, size, 2 * block), BF16),
            pltpu.VMEM((length // block, 2 * block, size), BF16),
            pltpu.VMEM((length // block, size, 2 * block), BF16),
            (tile, tile),
            (pltpu.VMEM((depth, size), BF16),) * 2,
            (pltpu.VMEM((depth, size), BF16),) * half_slots,
            pltpu.VMEM((3, slots, 2, 8, size), F32),
            pltpu.VMEM((3, slots, size, 128), F32),
            pltpu.VMEM((3, slots, 2, 16, size), BF16),
            pltpu.VMEM((3, slots, size, 128), BF16),
            pltpu.VMEM((3, half_slots) + patch, BF16),
            pltpu.VMEM((3, half_slots) + patch, BF16),
            pltpu.VMEM((3, half_slots) + patch, F32),
            *[pltpu.VMEM((half_slots,) + patch, BF16)] * 8,
            pltpu.VMEM((3, half_slots, slots_uv, block, block), BF16),
            pltpu.VMEM((3, half_slots) + patch, BF16),
            pltpu.VMEM((3, half_slots) + patch, BF16),
            plane,
            plane,
            tile,
            tile,
            dma((9,)),
            dma((2, 5)),
            dma((2, 2)),
            dma((2, 3)),
            dma((2, 3, half_slots)),
            dma((2, half_slots, slots_uv)),
            dma((2, half_slots, slots_uv)),
            dma((2, half_slots, slots_uv)),
            dma((2, half_slots, slots_uv)),
            dma((2, 3, half_slots, slots_uv)),
            dma((2, 1 + EDGES)),
        ],
        compiler_params=pltpu.CompilerParams(
            vmem_limit_bytes=int(56 * 1024 * 1024), collective_id=0, has_side_effects=True
        ),
    )(count, offset, width, bins, used, seeds, sky, weight)
    return pl.pallas_call(
        add_kernel,
        out_shape=jax.ShapeDtypeStruct((size, size), F32),
        in_specs=[anywhere, anywhere],
        out_specs=anywhere,
        scratch_shapes=[tile, tile, plane, dma((3, BANDS))],
        compiler_params=pltpu.CompilerParams(vmem_limit_bytes=56 * 1024 * 1024),
        cost_estimate=pl.CostEstimate(flops=size * size, bytes_accessed=10 * size * size, transcendentals=0),
    )(inner, edge)


def solution(mesh):
    in_specs = (
        P("ty", "tx"),
        P("ty", "tx"),
        P("ty", "tx", None, None),
        P("ty", "tx", None),
        P("ty", "tx", None, None, None),
        P("ty", "tx", None),
        P("ty", "tx", None, None, None, None),
    )
    out_specs = P("ty", "tx")
    return jax.shard_map(shards, mesh=mesh, in_specs=in_specs, out_specs=out_specs, check_vma=False)
```

```python
import functools
import math

import jax
import jax.numpy as jnp
import numpy as np
from jax import lax
from jax.experimental import pallas as pl
from jax.experimental.pallas import tpu as pltpu
from jax.sharding import PartitionSpec as P

F32 = jnp.float32
BF16 = jnp.bfloat16
I32 = jnp.int32
FINE = 32
CHUNK = 512
BANDS = 4
EDGES = 4
FIELDS = 8
MESH = pl.DeviceIdType.MESH


def seed_tables(length, fine):
    pixels = np.arange(length, dtype=np.int64)
    rows = np.concatenate([np.arange(fine), fine * np.arange(length // fine)])
    angle = (rows[:, None] * pixels[None, :] % length) * (2.0 * math.pi / length)
    scale = np.where(np.arange(rows.shape[0]) < fine, 1.0 / math.sqrt(length), 1.0)[:, None]
    return np.stack([np.cos(angle) * scale, np.sin(angle) * scale]).astype(np.float32)


def wide(column, width):
    return jnp.concatenate([column] * (width // column.shape[1]), axis=1)


def kernel(
    count_hbm, offset_hbm, width_hbm, bins_hbm, used_hbm, seeds_in, sky_in, weight_in,
    inner_got, edge_got,
    count_in, offset_in, width_in, bins_in, used_in,
    meta_ref, meta_got, meta_all, sky_ref, outer_ref, inner_ref, weight_ref, weight_got,
    seeds_ref, row_tab, flip_tab, col_tab, turn_tab,
    beamed, first, spread, gx_ref, gy_ref, gx_half, gy_half,
    part_send, part_got, totals, raw_send, raw_got, own_send, own_got,
    sum_send, sum_got, back_send, back_got, weights, scaled_own, scaled_par, acc_outer, acc_inner, edge_send, inner_send,
    local_sems, meta_sems, sky_sems, weight_sems, part_sems, raw_sems, own_sems, sum_sems,
    back_sems, par_sems, last_sems,
):
    size = sky_ref.shape[0]
    length = 2 * size
    slots, slots_uv, block = weight_ref.shape[0], weight_ref.shape[1], weight_ref.shape[2]
    half_slots = slots // 2
    ty, tx = lax.axis_index("ty"), lax.axis_index("tx")
    ny, nx = lax.axis_size("ty"), lax.axis_size("tx")
    core = tx % 2
    partner = tx + 1 - 2 * core
    beyond = tx - 1 + 2 * core
    has_up, has_down = ty > 0, ty < ny - 1
    has_beyond = jnp.logical_and(beyond >= 0, beyond < nx)
    has_row = (has_up, has_down)
    row_half = pl.multiple_of((ty % 2) * size, size)
    col_half = pl.multiple_of((1 - core) * size, size)
    to_partner = {"tx": partner}
    to_beyond = {"tx": beyond}
    to_row = ({"ty": ty - 1}, {"ty": ty + 1})
    to_cross = ({"ty": ty - 1, "tx": partner}, {"ty": ty + 1, "tx": partner})
    odd_row = ty % 2
    d_far, d_mate = 2 * odd_row, 2 * (1 - odd_row)
    giving, fed = ty - 2 + 4 * odd_row, ty + 2 - 4 * odd_row
    has_far = jnp.logical_and(giving >= 0, giving < ny)
    has_fed = jnp.logical_and(fed >= 0, fed < ny)
    to_mate, to_giving, to_fed = {"ty": ty + 1 - 2 * odd_row}, {"ty": giving}, {"ty": fed}
    to_far = {"ty": ty - 1 + 2 * odd_row}

    local = [
        pltpu.make_async_copy(source, target, local_sems.at[i])
        for i, (source, target) in enumerate(
            (
                (sky_in, sky_ref),
                (count_hbm, count_in),
                (offset_hbm, offset_in),
                (width_hbm, width_in),
                (bins_hbm, bins_in),
                (used_hbm, used_in),
                (seeds_in, seeds_ref),
                (weight_in, weight_ref),
            )
        )
    ]

    def remote(src, dst, sems, at, target):
        return pltpu.make_async_remote_copy(
            src_ref=src,
            dst_ref=dst,
            send_sem=sems.at[(0,) + at],
            recv_sem=sems.at[(1,) + at],
            device_id=target,
            device_id_type=MESH,
        )

    def meta_copy(slot, target):
        return remote(meta_ref, meta_got[slot], meta_sems, (slot,), target)

    def meta_partner():
        return meta_copy(0, to_partner)

    def meta_send(side):
        return meta_copy(2 - side, to_row[side]), meta_copy(4 - side, to_cross[side])

    def meta_take(side):
        return meta_copy(1 + side, to_row[side]), meta_copy(3 + side, to_cross[side])

    def sky_partner():
        return remote(sky_ref, inner_ref, sky_sems, (0,), to_partner)

    def sky_beyond():
        return remote(sky_ref, outer_ref, sky_sems, (1,), to_beyond)

    def weight_copy():
        return remote(weight_ref, weight_got, weight_sems, (0,), to_partner)

    def part_copy(g, jj):
        return remote(part_send.at[g, jj], part_got.at[g, jj], part_sems, (g, jj), to_partner)

    def raw_copy(target, jj, k):
        return remote(raw_send.at[jj, k], raw_got.at[jj, k], raw_sems, (jj, k), target)

    def own_copy(jj, k):
        return remote(own_send.at[jj, k], own_got.at[jj, k], own_sems, (jj, k), to_mate)

    def sum_copy(jj, k):
        return remote(sum_send.at[jj, k], sum_got.at[jj, k], sum_sems, (jj, k), to_mate)

    def back_copy(target, jj, k):
        return remote(back_send.at[jj, k], back_got.at[jj, k], back_sems, (jj, k), target)

    def weights_mate():
        return remote(weights.at[2], weights.at[1], weight_sems, (1,), to_mate)

    def weights_far():
        return remote(weights.at[2], weights.at[0], weight_sems, (2,), to_far)

    def par_copy(g, jj, k):
        return remote(
            scaled_own.at[g, jj, k], scaled_par.at[g, jj, k], par_sems, (g, jj, k), to_partner
        )

    def last_edge(band):
        rows = slice(band * size // EDGES, (band + 1) * size // EDGES)
        return remote(edge_send.at[rows], edge_got.at[rows], last_sems, (1 + band,), to_beyond)

    def last_inner():
        return remote(inner_send, inner_got, last_sems, (0,), to_partner)

    def no_edge():
        return pltpu.make_async_copy(edge_send, edge_got, local_sems.at[len(local)])

    barrier = pltpu.get_barrier_semaphore()
    pl.semaphore_signal(barrier, inc=1, device_id=to_partner, device_id_type=MESH)

    @pl.when(has_beyond)
    def _():
        pl.semaphore_signal(barrier, inc=1, device_id=to_beyond, device_id_type=MESH)

    for side in range(2):

        @pl.when(has_row[side])
        def _(side=side):
            pl.semaphore_signal(barrier, inc=1, device_id=to_row[side], device_id_type=MESH)
            pl.semaphore_signal(barrier, inc=1, device_id=to_cross[side], device_id_type=MESH)

    for has, target in ((has_far, to_giving), (has_fed, to_fed)):

        @pl.when(has)
        def _(target=target):
            pl.semaphore_signal(barrier, inc=1, device_id=target, device_id_type=MESH)

    for copy in local:
        copy.start()

    for copy in local[1:6]:
        copy.wait()

    lane = lax.broadcasted_iota(I32, (1, slots), 1)
    widths = width_in[...].astype(F32)
    meta_ref[slots, 0] = count_in[0, 0]
    for s in range(slots):
        meta_ref[s, 0] = offset_in[0, s]
        meta_ref[s, 1] = offset_in[1, s]
        meta_ref[s, 2] = jnp.sum(jnp.where(lane == s, widths, 0.0)).astype(I32)
        for k in range(slots_uv):
            for which in range(2):
                meta_ref[s, 3 + 2 * k + which] = bins_in[k, which, s]
        meta_ref[s, 3 + 2 * slots_uv] = used_in[0, s]

    @pl.when(jnp.logical_not(has_beyond))
    def _():
        outer_ref[...] = jnp.zeros_like(outer_ref)
        edge_send[...] = jnp.zeros_like(edge_send)

    with jax.named_scope("barrier"):
        local[0].wait()
        pl.semaphore_wait(
            barrier,
            1 + has_beyond.astype(I32) + 2 * has_up.astype(I32) + 2 * has_down.astype(I32)
            + has_far.astype(I32) + has_fed.astype(I32),
        )

    @pl.when(has_beyond)
    def _():
        sky_beyond().start()

    sky_partner().start()
    meta_partner().start()
    for side in range(2):

        @pl.when(has_row[side])
        def _(side=side):
            for copy in meta_send(side):
                copy.start()

    for copy in local[6:]:
        copy.wait()
    weight_copy().start()

    acc_outer[...] = jnp.zeros_like(acc_outer)
    acc_inner[...] = jnp.zeros_like(acc_inner)

    per_block = block // FINE

    def table(j, carry):
        blk, at = j // per_block, pl.ds(pl.multiple_of((j % per_block) * FINE, FINE), FINE)
        for tab, half in ((row_tab, row_half), (col_tab, col_half)):
            lanes = pl.ds(half, size)
            c, s = seeds_ref[0, pl.ds(FINE + j, 1), lanes], seeds_ref[1, pl.ds(FINE + j, 1), lanes]
            fc, fs = seeds_ref[0, :FINE, lanes], seeds_ref[1, :FINE, lanes]
            tab[blk, at, :] = (fc * c - fs * s).astype(BF16)
            tab[blk, pl.ds(pl.multiple_of(block + (j % per_block) * FINE, FINE), FINE), :] = (fs * c + fc * s).astype(BF16)
        return carry

    with jax.named_scope("tables"):
        lax.fori_loop(0, length // FINE, table, 0)

    def flipped(j, carry):
        at = pl.ds(pl.multiple_of(j * FINE, FINE), FINE)
        for tab, parity in ((flip_tab, odd_row), (turn_tab, 1 - core)):
            row = parity * (size // FINE) + j
            c, s = seeds_ref[0, pl.ds(FINE + row, 1), :], seeds_ref[1, pl.ds(FINE + row, 1), :]
            fc, fs = seeds_ref[0, :FINE, :], seeds_ref[1, :FINE, :]
            cos, sin = (fc * c - fs * s).astype(BF16), (fs * c + fc * s).astype(BF16)
            for blk in range(length // block):
                tab[blk, at, :block] = cos[:, blk * block : (blk + 1) * block]
                tab[blk, at, block:] = sin[:, blk * block : (blk + 1) * block]
        return carry

    with jax.named_scope("flips"):
        lax.fori_loop(0, size // FINE, flipped, 0)

    with jax.named_scope("meta"):
        meta_partner().wait()
        for side in range(2):

            @pl.when(has_row[side])
            def _(side=side):
                for copy in meta_take(side):
                    copy.wait_recv()

            @pl.when(jnp.logical_not(has_row[side]))
            def _(side=side):
                for slot in (1 + side, 3 + side):
                    meta_got[slot][slots, 0] = 0
                    for s in range(slots):
                        for f in range(FIELDS):
                            meta_got[slot][s, f] = 0

    sources = ((meta_got[1], meta_got[3]), (meta_ref, meta_got[0]), (meta_got[2], meta_got[4]))
    even_here = core == 0

    def gather(s, f):
        for d, (same, other) in enumerate(sources):
            a, b = same[s, f], other[s, f]
            meta_all[d, 0, s, f] = jnp.where(even_here, a, b)
            meta_all[d, 1, s, f] = jnp.where(even_here, b, a)

    def gather_slot(s, carry):
        for f in range(FIELDS):
            gather(s, f)
        return carry

    lax.fori_loop(0, slots, gather_slot, 0)
    gather(slots, 0)

    def pointing(d, j):
        even, odd = meta_all[d, 0, slots, 0], meta_all[d, 1, slots, 0]
        from_odd = (j >= even).astype(I32)
        slot = jnp.clip(j - from_odd * even, 0, slots - 1)
        live = j < even + odd
        return from_odd, slot, live

    def bins(d, from_odd, slot, k, which):
        b = meta_all[d, from_odd, slot, 3 + 2 * k + which]
        return jnp.clip(b, 0, length // block - 1)

    def gaussian(shape, axis, shift, decay, live):
        away = lax.broadcasted_iota(I32, shape, axis) + shift
        inside = jnp.logical_and(away >= -size, away < size)
        inside = jnp.logical_and(inside, live)
        away = away.astype(F32)
        if axis == 0:
            fold = away.reshape(shape[0] // 8, 8, shape[1])
            value = jnp.exp(-(fold * fold) * decay[None]).reshape(shape)
        else:
            value = jnp.exp(-(away * away) * wide(decay, shape[1]))
        return jnp.where(inside, value, jnp.zeros(shape, F32))

    def beams(i, carry):
        d, j = i // slots, i % slots
        from_odd, slot, live = pointing(d, j)
        oy, ox = meta_all[d, from_odd, slot, 0], meta_all[d, from_odd, slot, 1]
        width = jnp.full((8, 128), meta_all[d, from_odd, slot, 2], I32).astype(F32)
        decay = 1.0 / (2.0 * width * width)
        gy = gaussian((size, 128), 0, (1 - d) * size - oy, decay, live)
        gy_ref[d, j] = gy
        gy_half[d, j] = gy.astype(BF16)
        outer_at, inner_at = 3 * core - 1, 1 - core
        for i, tile_at in enumerate((outer_at, inner_at)):
            gx = gaussian((8, size), 1, (tile_at - from_odd) * size - ox, decay, live)
            gx_ref[d, j, i] = gx
            gx_half[d, j, i] = jnp.concatenate([gx, gx], axis=0).astype(BF16)
        return carry

    with jax.named_scope("weights"):
        weight_copy().wait_recv()
        for jj in range(half_slots):
            from_odd, slot, live = pointing(1, half_slots * core + jj)
            used = meta_all[1, from_odd, slot, 3 + 2 * slots_uv]
            for k in range(slots_uv):
                weight = jnp.where(from_odd == core, weight_ref[slot, k], weight_got[slot, k])
                weight = weight.astype(F32) * jnp.where(k < used, 1.0, 0.0).astype(F32)
                weights[2, jj, k] = weight.astype(BF16)

        weights_mate().start()

        @pl.when(has_far)
        def _():
            weights_far().start()

    with jax.named_scope("beams"):
        lax.fori_loop(0, 3 * slots, beams, 0)

    def column_table(d, from_odd, slot, k):
        return col_tab[bins(d, from_odd, slot, k, 1)]

    def prepare(d, j, beamed_ref):
        gy = wide(gy_half[d, j], CHUNK)
        for at in range(0, size, CHUNK):
            cols = slice(at, at + CHUNK)
            gx = [jnp.concatenate([gx_half[d, j, i, :, cols]] * (size // 16), axis=0) for i in range(2)]
            value = gx[0] * outer_ref[:, cols] + gx[1] * inner_ref[:, cols]
            beamed_ref[:, cols] = gy * value

    def transform_rows(d, j, beamed_ref, first_ref):
        from_odd, slot, live = pointing(d, j)
        rows = jnp.concatenate(
            [row_tab[bins(d, from_odd, slot, k, 0)] for k in range(slots_uv)], axis=0
        )
        for at in range(0, size, CHUNK):
            cols = slice(at, at + CHUNK)
            first_ref[:, cols] = jnp.dot(
                rows, beamed_ref[:, cols], preferred_element_type=F32
            ).astype(BF16)

    def transform_columns(d, j, first_ref, result_ref):
        from_odd, slot, live = pointing(d, j)
        for k in range(slots_uv):
            both = jnp.dot(
                first_ref[2 * k * block : (2 * k + 2) * block, :],
                turn_tab[bins(d, from_odd, slot, k, 1)],
                preferred_element_type=F32,
            )
            real = both[:block, :block] - both[block:, block:]
            turned = both[:block, block:] + both[block:, :block]
            result_ref[k, :, :block] = real.astype(result_ref.dtype)
            result_ref[k, :, block:] = turned.astype(result_ref.dtype)

    def spread_out(d, j, scaled_ref, spread_ref):
        from_odd, slot, live = pointing(d, j)
        for k in range(slots_uv):
            value = scaled_ref[k]
            real, turned = value[:, :block], value[:, block:]
            square = jnp.concatenate(
                [value, jnp.concatenate([turned, -real], axis=1)], axis=0
            )
            spread_ref[2 * k * block : (2 * k + 2) * block, :] = jnp.dot(
                square, col_tab[bins(d, from_odd, slot, k, 1)], preferred_element_type=F32
            ).astype(BF16)

    def bring_back(d, j, spread_ref, start, stop):
        from_odd, slot, live = pointing(d, j)
        rows = jnp.concatenate(
            [flip_tab[bins(d, from_odd, slot, k, 0), start:stop] for k in range(slots_uv)], axis=1
        )
        gy = wide(gy_ref[d, j, start:stop], CHUNK)
        for at in range(0, size, CHUNK):
            cols = slice(at, at + CHUNK)
            back = gy * jnp.dot(rows, spread_ref[:, cols], preferred_element_type=F32)
            acc_outer[start:stop, cols] += gx_ref[d, j, 0, 0:1, cols] * back
            acc_inner[start:stop, cols] += gx_ref[d, j, 1, 0:1, cols] * back

    mine, theirs = half_slots * core, half_slots * (1 - core)

    with jax.named_scope("sky"):
        sky_partner().wait_recv()

        @pl.when(has_beyond)
        def _():
            sky_beyond().wait_recv()

    def pass_sum(jj, k, value):
        sum_send[jj, k] = value.astype(BF16)
        sum_copy(jj, k).start()

    def row_of(g):
        own = g // 2
        return 2 * (odd_row * (1 - g) + (1 - odd_row) * g) * (1 - own) + own

    def settle(g, jj):
        part_copy(g, jj).wait_recv()
        for k in range(slots_uv):
            totals[g, jj, k] = totals[g, jj, k] + part_got[g, jj, k].astype(F32)

        @pl.when(g == 0)
        def _():
            for k in range(slots_uv):
                raw_send[jj, k] = totals[0, jj, k].astype(BF16)
                raw_copy(to_giving, jj, k).start()

        @pl.when(g == 2)
        def _():
            for k in range(slots_uv):
                own_send[jj, k] = totals[2, jj, k].astype(BF16)
                own_copy(jj, k).start()

        @pl.when(jnp.logical_and(g == 1, jnp.logical_not(has_fed)))
        def _():
            for k in range(slots_uv):
                pass_sum(jj, k, totals[1, jj, k])

    far = has_far.astype(I32)

    def forward_units(s, carry):
        end = s // half_slots
        slot = s * (1 - end)
        units = (
            (2 * (1 - end) * (1 - far) + end, slot),
            ((1 - end) * (1 + far) + end, slot + end),
        )
        for base in (theirs, mine):
            for i, (g, jj) in enumerate(units):
                prepare(row_of(g), base + jj, beamed[i])
            for i, (g, jj) in enumerate(units):
                transform_rows(row_of(g), base + jj, beamed[i], first[i])
            for i, (g, jj) in enumerate(units):
                result = part_send.at[g, jj] if base is theirs else totals.at[g, jj]
                transform_columns(row_of(g), base + jj, first[i], result)
            for g, jj in units:
                if base is theirs:
                    part_copy(g, jj).start()
                else:
                    settle(g, jj)
        return carry

    with jax.named_scope("forward"):
        lax.fori_loop(0, half_slots + far, forward_units, 0)

    def scale(g, jj, k, total):
        weight = weights[g, jj, k].astype(F32)
        scaled_own[g, jj, k] = (total * wide(weight, 2 * block)).astype(BF16)
        par_copy(g, jj, k).start()

    def adjoint_all(g, base, scaled_ref):
        for jj in range(half_slots):
            spread_out(row_of(g), base + jj, scaled_ref.at[g, jj], spread[jj])
        for jj in range(half_slots):
            bring_back(row_of(g), base + jj, spread[jj], 0, size)

    def adjoint_one(g, base, jj, scaled_ref):
        spread_out(row_of(g), base + jj, scaled_ref.at[g, jj], spread[0])
        bring_back(row_of(g), base + jj, spread[0], 0, size)

    def adjoint_theirs(g):
        with jax.named_scope(f"theirs{g}"):
            for jj in range(half_slots):
                for k in range(slots_uv):
                    par_copy(g, jj, k).wait_recv()
            adjoint_all(g, theirs, scaled_par)

    def mate_slot(jj, carry):
        for k in range(slots_uv):
            own_copy(jj, k).wait_recv()
            own_part = own_got[jj, k].astype(F32)

            @pl.when(has_fed)
            def _(k=k):
                back_send[jj, k] = (totals[1, jj, k] + own_got[jj, k].astype(F32)).astype(BF16)
                back_copy(to_fed, jj, k).start()
                raw_copy(to_fed, jj, k).wait_recv()
                both = totals[1, jj, k] + raw_got[jj, k].astype(F32)
                pass_sum(jj, k, both)
                totals[1, jj, k] = both

            scale(1, jj, k, totals[1, jj, k] + own_part)
        adjoint_one(1, mine, jj, scaled_own)
        return carry

    with jax.named_scope("mate"):
        weights_mate().wait_recv()
        lax.fori_loop(0, half_slots, mate_slot, 0)

    adjoint_theirs(1)

    def far_slot(jj, carry):
        for k in range(slots_uv):
            back_copy(to_giving, jj, k).wait_recv()
            scale(0, jj, k, totals[0, jj, k] + back_got[jj, k].astype(F32))
        adjoint_one(0, mine, jj, scaled_own)
        return carry

    @pl.when(has_far)
    def _():
        with jax.named_scope("far"):
            weights_far().wait_recv()
            lax.fori_loop(0, half_slots, far_slot, 0)

    def own_slot(jj):
        with jax.named_scope(f"own{jj}"):
            for k in range(slots_uv):
                sum_copy(jj, k).wait_recv()
                scale(2, jj, k, totals[2, jj, k] + sum_got[jj, k].astype(F32))
            adjoint_one(2, mine, jj, scaled_own)

    own_slot(0)

    @pl.when(has_far)
    def _():
        adjoint_theirs(0)

    def own_theirs(jj):
        for k in range(slots_uv):
            par_copy(2, jj, k).wait_recv()
        adjoint_one(2, theirs, jj, scaled_par)

    for jj in range(half_slots - 1):

        @pl.when(jnp.logical_not(has_far))
        def _(jj=jj):
            own_theirs(jj)

        own_slot(jj + 1)

        @pl.when(has_far)
        def _(jj=jj):
            own_theirs(jj)

    with jax.named_scope("final"):
        jj = half_slots - 1
        for k in range(slots_uv):
            par_copy(2, jj, k).wait_recv()
        spread_out(1, theirs + jj, scaled_par.at[2, jj], spread[0])
        for band in range(EDGES):
            start, stop = band * size // EDGES, (band + 1) * size // EDGES
            bring_back(1, theirs + jj, spread[0], start, stop)

            @pl.when(has_beyond)
            def _(band=band, start=start, stop=stop):
                edge_send[start:stop] = acc_outer[start:stop].astype(BF16)
                last_edge(band).start()

    inner_send[...] = acc_inner[...].astype(BF16)
    last_inner().start()

    @pl.when(jnp.logical_not(has_beyond))
    def _():
        no_edge().start()

    sky_partner().wait_send()
    weight_copy().wait_send()

    @pl.when(has_beyond)
    def _():
        sky_beyond().wait_send()

    for side in range(2):

        @pl.when(has_row[side])
        def _(side=side):
            for copy in meta_send(side):
                copy.wait_send()

    for jj in range(half_slots):
        for g in (1, 2):
            part_copy(g, jj).wait_send()
            for k in range(slots_uv):
                par_copy(g, jj, k).wait_send()
        for k in range(slots_uv):
            own_copy(jj, k).wait_send()
            sum_copy(jj, k).wait_send()

            @pl.when(has_fed)
            def _(jj=jj, k=k):
                back_copy(to_fed, jj, k).wait_send()

        @pl.when(has_far)
        def _(jj=jj):
            part_copy(0, jj).wait_send()
            for k in range(slots_uv):
                par_copy(0, jj, k).wait_send()
                raw_copy(to_giving, jj, k).wait_send()

    weights_mate().wait_send()

    @pl.when(has_far)
    def _():
        weights_far().wait_send()

    with jax.named_scope("last"):
        last_inner().wait()

        @pl.when(has_beyond)
        def _():
            for band in range(EDGES):
                last_edge(band).wait()

        @pl.when(jnp.logical_not(has_beyond))
        def _():
            no_edge().wait()


def add_kernel(inner_hbm, edge_hbm, out_hbm, inner_ref, edge_ref, out_ref, sems):
    band = out_ref.shape[0] // BANDS
    bands = [slice(i * band, (i + 1) * band) for i in range(BANDS)]
    moves = [
        [
            pltpu.make_async_copy(inner_hbm.at[rows], inner_ref.at[rows], sems.at[0, i]),
            pltpu.make_async_copy(edge_hbm.at[rows], edge_ref.at[rows], sems.at[1, i]),
            pltpu.make_async_copy(out_ref.at[rows], out_hbm.at[rows], sems.at[2, i]),
        ]
        for i, rows in enumerate(bands)
    ]
    for inner, edge, out in moves:
        inner.start()
        edge.start()
    for rows, (inner, edge, out) in zip(bands, moves):
        inner.wait()
        edge.wait()
        out_ref[rows, :] = inner_ref[rows, :].astype(F32) + edge_ref[rows, :].astype(F32)
        out.start()
    for inner, edge, out in moves:
        out.wait()


def shards(sky, point_count, point_offset, beam_width, uv_bins, uv_count, uv_weight):
    size = sky.shape[0]
    length = 2 * size
    slots, slots_uv, block = uv_weight.shape[2], uv_weight.shape[3], uv_weight.shape[4]
    half_slots = slots // 2
    depth = 2 * slots_uv * block
    seeds = seed_tables(length, FINE)
    count = point_count.reshape(1, 1)
    offset = jnp.transpose(point_offset, (0, 1, 3, 2)).reshape(2, slots)
    width = beam_width.reshape(1, slots)
    bins = jnp.transpose(uv_bins, (0, 1, 3, 4, 2)).reshape(slots_uv, 2, slots)
    used = uv_count.reshape(1, slots)
    weight = uv_weight.reshape(slots, slots_uv, block, block)

    dma = pltpu.SemaphoreType.DMA
    meta_shape = (slots + 1, FIELDS)
    tile = pltpu.VMEM((size, size), BF16)
    plane = pltpu.VMEM((size, size), F32)
    patch = (slots_uv, block, 2 * block)
    anywhere = pl.BlockSpec(memory_space=pl.ANY)
    inner, edge = pl.pallas_call(
        kernel,
        out_shape=(jax.ShapeDtypeStruct((size, size), BF16),) * 2,
        in_specs=[anywhere] * 8,
        out_specs=(anywhere, anywhere),
        scratch_shapes=[
            pltpu.SMEM(count.shape, I32),
            pltpu.SMEM(offset.shape, I32),
            pltpu.VMEM(width.shape, BF16),
            pltpu.SMEM(bins.shape, I32),
            pltpu.SMEM(used.shape, I32),
            pltpu.SMEM(meta_shape, I32),
            tuple([pltpu.SMEM(meta_shape, I32)] * 5),
            pltpu.SMEM((3, 2) + meta_shape, I32),
            tile,
            tile,
            tile,
            pltpu.VMEM(weight.shape, BF16),
            pltpu.VMEM(weight.shape, BF16),
            pltpu.VMEM(seeds.shape, F32),
            pltpu.VMEM((length // block, 2 * block, size), BF16),
            pltpu.VMEM((length // block, size, 2 * block), BF16),
            pltpu.VMEM((length // block, 2 * block, size), BF16),
            pltpu.VMEM((length // block, size, 2 * block), BF16),
            (tile, tile),
            (pltpu.VMEM((depth, size), BF16),) * 2,
            (pltpu.VMEM((depth, size), BF16),) * half_slots,
            pltpu.VMEM((3, slots, 2, 8, size), F32),
            pltpu.VMEM((3, slots, size, 128), F32),
            pltpu.VMEM((3, slots, 2, 16, size), BF16),
            pltpu.VMEM((3, slots, size, 128), BF16),
            pltpu.VMEM((3, half_slots) + patch, BF16),
            pltpu.VMEM((3, half_slots) + patch, BF16),
            pltpu.VMEM((3, half_slots) + patch, F32),
            *[pltpu.VMEM((half_slots,) + patch, BF16)] * 8,
            pltpu.VMEM((3, half_slots, slots_uv, block, block), BF16),
            pltpu.VMEM((3, half_slots) + patch, BF16),
            pltpu.VMEM((3, half_slots) + patch, BF16),
            plane,
            plane,
            tile,
            tile,
            dma((9,)),
            dma((2, 5)),
            dma((2, 2)),
            dma((2, 3)),
            dma((2, 3, half_slots)),
            dma((2, half_slots, slots_uv)),
            dma((2, half_slots, slots_uv)),
            dma((2, half_slots, slots_uv)),
            dma((2, half_slots, slots_uv)),
            dma((2, 3, half_slots, slots_uv)),
            dma((2, 1 + EDGES)),
        ],
        compiler_params=pltpu.CompilerParams(
            vmem_limit_bytes=int(56 * 1024 * 1024), collective_id=0, has_side_effects=True
        ),
    )(count, offset, width, bins, used, seeds, sky, weight)
    return pl.pallas_call(
        add_kernel,
        out_shape=jax.ShapeDtypeStruct((size, size), F32),
        in_specs=[anywhere, anywhere],
        out_specs=anywhere,
        scratch_shapes=[tile, tile, plane, dma((3, BANDS))],
        compiler_params=pltpu.CompilerParams(vmem_limit_bytes=56 * 1024 * 1024),
        cost_estimate=pl.CostEstimate(flops=size * size, bytes_accessed=10 * size * size, transcendentals=0),
    )(inner, edge)


def solution(mesh):
    in_specs = (
        P("ty", "tx"),
        P("ty", "tx"),
        P("ty", "tx", None, None),
        P("ty", "tx", None),
        P("ty", "tx", None, None, None),
        P("ty", "tx", None),
        P("ty", "tx", None, None, None, None),
    )
    out_specs = P("ty", "tx")
    return jax.shard_map(shards, mesh=mesh, in_specs=in_specs, out_specs=out_specs, check_vma=False)
```
